32 devices in a mesh: dp: 2 (over x), tp: 16 (over z, y, core).
Axes of the slice: x: 2, y: 2, z: 4, core: 2. Of those that a mesh axis runs over, the one named last changes fastest.
Arguments:
- hidden: bfloat16 [128, 7, 3072], P('dp'), parts along dimension 0
- norm_gain: float32 [3072], replicated
- w_head: bfloat16 [3072, 128256], P(None, 'tp')
- draft_probs: float32 [128, 6, 128256], P('dp', None, 'tp'), parts along dimension 0
- draft_tokens: int32 [128, 6], P('dp'), parts along dimension 0
- temperature: float32 [128], P('dp'), parts along dimension 0
Outputs:
- output 1: float32 [128, 6], P('dp'), parts along dimension 0
- output 2: float32 [128, 6], P('dp'), parts along dimension 0
- output 3: float32 [128, 6, 128256], P('dp', None, 'tp'), parts along dimension 0
- output 4: float32 [128], P('dp'), parts along dimension 0
There are 2 independent parts. The reference program is written for one: setup_inputs(seed, part) draws one part's arguments, and reference() takes and returns one part's arrays. A program takes and returns all parts, laid end to end along the dimension named above; an argument that names none is the same for every part.
All inputs are finite; a program needn't handle non-finite values.
Results may differ from the reference program's by a relative error of at most 0.001.
Values sent between devices are 32-bit elements.
A program may use at most 1 GiB of HBM per device.

```python
import jax
import jax.numpy as jnp
from jax import lax

BATCH_ROWS = 64
DRAFT_LEN = 6
D_MODEL = 3072
VOCAB_SIZE = 128256
CLUSTER_COUNT = 3
WEIGHT_BLOCK = 128
CLUSTER_SPAN = VOCAB_SIZE // 32


def setup_inputs(seed: int = 0, part: int = 0) -> dict:
    part_key = jax.random.fold_in(jax.random.key(seed), part)
    key_h, key_q, key_s, key_t, key_c, key_k, key_o = jax.random.split(part_key, 7)
    key_w, key_g = jax.random.split(jax.random.key(seed + 1), 2)
    hidden = jax.random.normal(key_h, (BATCH_ROWS, DRAFT_LEN + 1, D_MODEL), jnp.float32).astype(jnp.bfloat16)
    norm_gain = jax.random.uniform(key_g, (D_MODEL,), jnp.float32, 0.5, 1.5)

    def weight_block(block_idx):
        gauss_block = jax.random.normal(jax.random.fold_in(key_w, block_idx), (WEIGHT_BLOCK, VOCAB_SIZE), jnp.float32)
        return (gauss_block * D_MODEL ** -0.5).astype(jnp.bfloat16)

    w_head = lax.map(weight_block, jnp.arange(D_MODEL // WEIGHT_BLOCK)).reshape(D_MODEL, VOCAB_SIZE)
    q_scale = jax.random.uniform(key_s, (BATCH_ROWS, DRAFT_LEN, 1), jnp.float32, 0.7, 1.3)
    q_logits = jax.random.normal(key_q, (BATCH_ROWS, DRAFT_LEN, VOCAB_SIZE), jnp.float32) * q_scale
    draft_probs = jax.nn.softmax(q_logits, axis=-1)
    temperature = jax.random.uniform(key_t, (BATCH_ROWS,), jnp.float32, 0.6, 1.4)
    centers = jax.random.randint(key_c, (CLUSTER_COUNT,), 0, VOCAB_SIZE - CLUSTER_SPAN)
    choice = jax.random.randint(key_k, (BATCH_ROWS, DRAFT_LEN), 0, CLUSTER_COUNT)
    offsets = jax.random.randint(key_o, (BATCH_ROWS, DRAFT_LEN), 0, CLUSTER_SPAN)
    draft_tokens = (centers[choice] + offsets).astype(jnp.int32)
    return {'hidden': hidden, 'norm_gain': norm_gain, 'w_head': w_head, 'draft_probs': draft_probs, 'draft_tokens': draft_tokens, 'temperature': temperature}


def reference(hidden, norm_gain, w_head, draft_probs, draft_tokens, temperature):
    def one_row(row_args):
        row_hidden, row_probs, row_tokens, row_temp = row_args
        hidden_f32 = row_hidden.astype(jnp.float32)
        inv_rms = lax.rsqrt(jnp.mean(hidden_f32 * hidden_f32, axis=-1, keepdims=True) + 1e-5)
        normed = (hidden_f32 * inv_rms * norm_gain).astype(jnp.bfloat16)
        logits = jnp.dot(normed, w_head, preferred_element_type=jnp.float32)
        scaled = logits / row_temp
        row_max = jnp.max(scaled, axis=-1, keepdims=True)
        row_lse = row_max + jnp.log(jnp.sum(jnp.exp(scaled - row_max), axis=-1, keepdims=True))
        target = jnp.exp(scaled[:DRAFT_LEN] - row_lse[:DRAFT_LEN])
        tok_target = jnp.take_along_axis(target, row_tokens[:, None], axis=-1)[:, 0]
        tok_draft = jnp.take_along_axis(row_probs, row_tokens[:, None], axis=-1)[:, 0]
        accept = jnp.minimum(1.0, tok_target / tok_draft)
        excess = jnp.maximum(target - row_probs, 0.0)
        norm_sum = jnp.sum(excess, axis=-1)
        residual = excess / norm_sum[:, None]
        return accept, norm_sum, residual, row_lse[DRAFT_LEN, 0]

    accept, norm_sum, residual, bonus_lse = lax.map(one_row, (hidden, draft_probs, draft_tokens, temperature))
    return accept, norm_sum, residual, bonus_lse
```

```python
import functools

import jax
import jax.numpy as jnp
from jax import lax
from jax.experimental import pallas as pl
from jax.experimental.pallas import tpu as pltpu
from jax.sharding import PartitionSpec as P

F32 = jnp.float32
LANES = 128
NEG = -3.0e38
MIB = 1024 * 1024


def eye():
    rows = lax.broadcasted_iota(jnp.int32, (LANES, LANES), 0)
    return rows == lax.broadcasted_iota(jnp.int32, (LANES, LANES), 1)


def to_lanes(column):
    return jnp.sum(jnp.where(eye(), column, 0.0), axis=0, keepdims=True)


def to_column(row):
    col = jnp.sum(jnp.where(eye(), jnp.broadcast_to(row, (LANES, LANES)), 0.0), axis=1, keepdims=True)
    return jnp.broadcast_to(col, (LANES, LANES))


def head_kernel(dims, h_ref, g_ref, w_ref, q_ref, t_ref, s_ref, qv_ref, mrow_ref, lse_ref,
                hbuf, x, wbuf, zs, m, sm, tinv, hsem, wsem, qsem):
    rows, draft_rows, seqs, depth, vocab, chunk, slots, qrows = dims
    n = pl.cdiv(vocab, chunk)
    tail = vocab - (n - 1) * chunk
    zcopy = pltpu.make_async_copy

    def wcopy(i, size=chunk):
        slot = lax.rem(i, slots)
        at = pl.ds(pl.multiple_of(i * chunk, chunk), size)
        return zcopy(w_ref.at[at], wbuf.at[slot, pl.ds(0, size)], wsem.at[slot])

    def qcopy(i):
        at = pl.ds(pl.multiple_of(i * qrows, qrows), qrows)
        return zcopy(q_ref.at[at], qv_ref.at[at], qsem.at[i])

    hcopy = zcopy(h_ref, hbuf, hsem)
    hcopy.start()
    for i in range(slots - 1):
        wcopy(i).start()

    t = t_ref[...]
    spread = jnp.where(eye(), jnp.broadcast_to(jnp.concatenate([t, t], axis=1), (LANES, LANES)), 0.0)
    tcol = jnp.sum(spread, axis=1, keepdims=True)
    tinv[...] = jnp.broadcast_to(1.0 / tcol[:seqs], (seqs, LANES))
    m[...] = jnp.full(m.shape, NEG, F32)
    sm[...] = jnp.zeros(sm.shape, F32)

    hcopy.wait()

    @pl.loop(0, rows // 16)
    def _(i):
        at = pl.ds(pl.multiple_of(i * 16, 16), 16)
        h = hbuf[at, :].astype(F32)
        r = lax.rsqrt(jnp.mean(h * h, axis=1, keepdims=True) + 1e-5)
        x[at, :] = (h * r * g_ref[...]).astype(jnp.bfloat16)

    def matmul(i, z, size=chunk):
        slot = lax.rem(i, slots)
        z[:, 0:size] = lax.dot_general(x[...], wbuf[slot, 0:size, :], (((1,), (1,)), ((), ())),
                                       preferred_element_type=F32)

    def stats(i, z, size=chunk, valid=chunk):
        base = pl.multiple_of(i * chunk, chunk)
        for b in range(rows // 8):
            r8 = slice(b * 8, b * 8 + 8)
            ti = tinv[(b * 8) % seqs:(b * 8) % seqs + 8, :]
            parts = []
            for c in range(0, size, LANES):
                s = z[r8, c:c + LANES] * ti
                if c + LANES > valid:
                    lane = lax.broadcasted_iota(jnp.int32, (8, LANES), 1)
                    s = jnp.where(lane < valid - c, s, NEG)
                parts.append(s)
                if b * 8 < draft_rows:
                    s_ref[r8, pl.ds(base + c, LANES)] = s
            old = m[r8, :]
            new = old
            for s in parts:
                new = jnp.maximum(new, s)
            tot = sm[r8, :] * jnp.exp(old - new)
            for s in parts:
                tot = tot + jnp.exp(s - new)
            m[r8, :] = new
            sm[r8, :] = tot

    nq = draft_rows // qrows

    def step(i, z, zprev):
        nxt = i + slots - 1

        @pl.when(nxt < n - 1)
        def _():
            wcopy(nxt).start()

        @pl.when(nxt == n - 1)
        def _():
            wcopy(n - 1, tail).start()

        @pl.when(i < nq)
        def _():
            qcopy(i).start()

        wcopy(i).wait()
        matmul(i, z)
        if zprev is not None:
            stats(i - 1, zprev)

    za, zb = zs.at[0], zs.at[1]
    step(0, za, None)

    @pl.loop(0, (n - 2) // 2)
    def _(k):
        step(2 * k + 1, zb, za)
        step(2 * k + 2, za, zb)

    last = pl.cdiv(tail, LANES) * LANES
    wcopy(n - 1, tail).wait()
    matmul(n - 1, zb, last)
    stats(n - 2, za)
    stats(n - 1, zb, last, tail)

    lse_ref[...] = jnp.zeros(lse_ref.shape, F32)
    for i in range(pl.cdiv(rows, LANES)):
        size = min(LANES, rows - i * LANES)
        r = slice(i * LANES, i * LANES + size)
        ml = m[r, :]
        mrow = jnp.max(ml, axis=1, keepdims=True)
        srow = jnp.sum(sm[r, :] * jnp.exp(ml - mrow), axis=1, keepdims=True)
        lse = jnp.broadcast_to(mrow + jnp.log(srow), (size, LANES))
        if i * LANES < draft_rows:
            mrow_ref[r, :] = jnp.broadcast_to(mrow, (size, LANES))
        mask = eye()[:size]
        lse_ref[i:i + 1, :] = jnp.sum(jnp.where(mask, lse, 0.0), axis=0, keepdims=True)

    for i in range(nq):
        qcopy(i).wait()


def verify_kernel(dims, s_ref, q_ref, mrow_ref, lse_ref, dt_ref, lcol_ref, ncol_ref, out_ref,
                  e_ref, ccol_ref, g1, g2, msg2, acc, tok, send1, recv1, send2, recv2):
    tp, draft_rows, seqs, vocab = dims
    blocks = draft_rows // LANES
    me = lax.axis_index("tp")
    full = vocab // LANES * LANES
    rest = vocab - full

    barrier = pltpu.get_barrier_semaphore()
    for d in range(1, tp):
        pl.semaphore_signal(barrier, inc=1, device_id={"tp": lax.rem(me + d, tp)},
                            device_id_type=pl.DeviceIdType.MESH)
    pl.semaphore_wait(barrier, tp - 1)

    def exchange(src, gather, send, recv):
        def copy(slot, sem, d):
            return pltpu.make_async_remote_copy(
                src_ref=src, dst_ref=gather.at[slot], send_sem=send.at[d], recv_sem=recv.at[sem],
                device_id={"tp": lax.rem(me + d, tp)}, device_id_type=pl.DeviceIdType.MESH)

        def start():
            for d in range(1, tp):
                copy(me, me, d).start()
            gather[me] = src[...]

        def wait():
            for d in range(1, tp):
                peer = lax.rem(me + d, tp)
                copy(peer, peer, d).wait_recv()

        def drain():
            for d in range(1, tp):
                copy(me, me, d).wait_send()

        return start, wait, drain

    start1, wait1, drain1 = exchange(lse_ref, g1, send1, recv1)
    start2, wait2, drain2 = exchange(msg2, g2, send2, recv2)
    start1()

    offset = me * vocab
    for i in range(blocks):
        ids = jnp.concatenate([dt_ref[2 * i:2 * i + 1, :], dt_ref[2 * i + 1:2 * i + 2, :]], axis=1)
        tok[i * LANES:(i + 1) * LANES, :] = to_column((ids - offset).astype(F32))

    lane = lax.broadcasted_iota(jnp.int32, (8, LANES), 1).astype(F32)

    acc[...] = jnp.zeros(acc.shape, F32)

    @pl.loop(0, draft_rows // 8)
    def _(b):
        r8 = pl.ds(pl.multiple_of(b * 8, 8), 8)
        mr = mrow_ref[r8, :]
        want = tok[r8, :]
        er = jnp.exp(s_ref[r8, full:full + rest] - mr[:, :rest])
        e_ref[r8, full:full + rest] = er
        qr = q_ref[r8, full:full + rest]
        hit = (lane[:, :rest] + float(full)) == want[:, :rest]
        acc[0, r8, 0:rest] = jnp.where(hit, er, 0.0)
        acc[1, r8, 0:rest] = jnp.where(hit, qr, 0.0)
        ae, aq = acc[0, r8, :], acc[1, r8, :]
        for c in range(0, full, LANES):
            e = jnp.exp(s_ref[r8, c:c + LANES] - mr)
            e_ref[r8, c:c + LANES] = e
            hit = (lane + float(c)) == want
            ae = ae + jnp.where(hit, e, 0.0)
            aq = aq + jnp.where(hit, q_ref[r8, c:c + LANES], 0.0)
        acc[0, r8, :] = ae
        acc[1, r8, :] = aq

    wait1()
    parts = g1[...]
    top = jnp.max(parts, axis=0)
    lse = top + jnp.log(jnp.sum(jnp.exp(parts - top[None]), axis=0))
    out_ref[...] = jnp.zeros(out_ref.shape, F32)
    out_ref[0:4, :] = lse
    for i in range(blocks):
        r = slice(i * LANES, (i + 1) * LANES)
        lcol = to_column(lse[i:i + 1, :])
        lcol_ref[r, :] = lcol
        ccol_ref[r, :] = jnp.exp(mrow_ref[r, :] - lcol)

    @pl.loop(0, draft_rows // 8)
    def _(b):
        r8 = pl.ds(pl.multiple_of(b * 8, 8), 8)
        cc = ccol_ref[r8, :]
        er = e_ref[r8, full:full + rest]
        acc[2, r8, 0:rest] = jnp.maximum(er * cc[:, :rest] - q_ref[r8, full:full + rest], 0.0)
        sums = [acc[2, r8, :], jnp.zeros((8, LANES), F32)]
        for k, c in enumerate(range(0, full, LANES)):
            sums[k % 2] += jnp.maximum(e_ref[r8, c:c + LANES] * cc - q_ref[r8, c:c + LANES], 0.0)
        acc[2, r8, :] = sums[0] + sums[1]

    msg2[...] = jnp.zeros(msg2.shape, F32)
    for i in range(blocks):
        r = slice(i * LANES, (i + 1) * LANES)
        total = jnp.sum(acc[2, r, :], axis=1, keepdims=True)
        msg2[i:i + 1, :] = to_lanes(jnp.broadcast_to(total, (LANES, LANES)))
        p = jnp.sum(acc[0, r, :], axis=1, keepdims=True) * ccol_ref[r, 0:1]
        qt = jnp.sum(acc[1, r, :], axis=1, keepdims=True)
        ok = jnp.where(qt > 0.0, jnp.minimum(1.0, p / jnp.where(qt > 0.0, qt, 1.0)), 0.0)
        msg2[4 + i:5 + i, :] = to_lanes(jnp.broadcast_to(ok, (LANES, LANES)))
    start2()
    wait2()
    sums = jnp.sum(g2[...], axis=0)
    out_ref[4:4 + 8, :] = sums
    for i in range(blocks):
        ncol_ref[i * LANES:(i + 1) * LANES, :] = to_column(1.0 / sums[i:i + 1, :])
    drain1()
    drain2()


def residual_kernel(dims, s_ref, q_ref, lcol_ref, ncol_ref, small_ref, res_ref, acc_ref, norm_ref, bonus_ref,
                    stage, sem):
    draft_rows, seqs, vocab, block, slots = dims
    n = draft_rows // block
    full = vocab // LANES * LANES
    rest = vocab - full

    def copy(i):
        slot = lax.rem(i, slots)
        return pltpu.make_async_copy(stage.at[slot], res_ref.at[pl.ds(pl.multiple_of(i * block, block), block)],
                                     sem.at[slot])

    @pl.loop(0, n)
    def _(i):
        slot = lax.rem(i, slots)

        @pl.when(i >= slots)
        def _():
            copy(i - slots).wait()

        for b in range(block // 8):
            src = pl.ds(pl.multiple_of(i * block + b * 8, 8), 8)
            dst = slice(b * 8, b * 8 + 8)
            lc, inv = lcol_ref[src, :], ncol_ref[src, :]
            for c in range(0, full, LANES):
                stage[slot, dst, c:c + LANES] = (
                    jnp.maximum(jnp.exp(s_ref[src, c:c + LANES] - lc) - q_ref[src, c:c + LANES], 0.0) * inv)
            stage[slot, dst, full:full + rest] = (
                jnp.maximum(jnp.exp(s_ref[src, full:full + rest] - lc[:, :rest]) - q_ref[src, full:full + rest], 0.0)
                * inv[:, :rest])
        copy(i).start()

    for j in range(draft_rows // seqs):
        i, off = j // 2, (j % 2) * seqs
        norm_ref[j:j + 1, :] = small_ref[4 + i:5 + i, off:off + seqs]
        acc_ref[j:j + 1, :] = small_ref[8 + i:9 + i, off:off + seqs]
    bonus_ref[...] = small_ref[3:4, 0:seqs]

    for i in range(n - slots, n):
        copy(i).wait()


def solution(mesh):
    tp = mesh.shape["tp"]
    vmem, hbm = pltpu.VMEM, pltpu.HBM

    def spec(space):
        return pl.BlockSpec(memory_space=space)

    def local_step(hidden, norm_gain, w_head, draft_probs, draft_tokens, temperature):
        seqs, positions, depth = hidden.shape
        drafts, vocab = draft_probs.shape[1:]
        rows, draft_rows = seqs * positions, seqs * drafts
        wide = pl.cdiv(vocab, LANES) * LANES
        h = hidden.transpose(1, 0, 2).reshape(rows, depth)
        w = w_head.T
        q = draft_probs.transpose(1, 0, 2).reshape(draft_rows, vocab)
        dt = draft_tokens.T
        chunk, slots, qrows = 512, 4, 32
        dims = (rows, draft_rows, seqs, depth, vocab, chunk, slots, qrows)
        s, qv, mrow, lse = pl.pallas_call(
            functools.partial(head_kernel, dims),
            out_shape=(pltpu.VMEM((draft_rows, wide), F32), pltpu.VMEM((draft_rows, vocab), F32),
                       pltpu.VMEM((draft_rows, LANES), F32), pltpu.VMEM((4, LANES), F32)),
            in_specs=[spec(hbm), spec(vmem), spec(hbm), spec(hbm), spec(vmem)],
            out_specs=(spec(vmem),) * 4,
            scratch_shapes=[
                pltpu.VMEM((rows, depth), jnp.bfloat16), pltpu.VMEM((rows, depth), jnp.bfloat16),
                pltpu.VMEM((slots, chunk, depth), jnp.bfloat16), pltpu.VMEM((2, rows, chunk), F32),
                pltpu.VMEM((rows, LANES), F32), pltpu.VMEM((rows, LANES), F32), pltpu.VMEM((seqs, LANES), F32),
                pltpu.SemaphoreType.DMA, pltpu.SemaphoreType.DMA((slots,)),
                pltpu.SemaphoreType.DMA((draft_rows // qrows,)),
            ],
            compiler_params=pltpu.CompilerParams(vmem_limit_bytes=24 * MIB),
        )(*(pltpu.with_memory_space_constraint(a, hbm) for a in (h,)), norm_gain.reshape(1, depth), w, q,
          temperature.reshape(1, seqs))

        lcol, ncol, small = pl.pallas_call(
            functools.partial(verify_kernel, (tp, draft_rows, seqs, vocab)),
            out_shape=(pltpu.VMEM((draft_rows, LANES), F32), pltpu.VMEM((draft_rows, LANES), F32),
                       pltpu.VMEM((16, LANES), F32)),
            in_specs=[spec(vmem)] * 5,
            out_specs=(spec(vmem),) * 3,
            scratch_shapes=[
                pltpu.VMEM((draft_rows, wide), F32), pltpu.VMEM((draft_rows, LANES), F32),
                pltpu.VMEM((tp, 4, LANES), F32), pltpu.VMEM((tp, 8, LANES), F32), pltpu.VMEM((8, LANES), F32),
                pltpu.VMEM((3, draft_rows, LANES), F32), pltpu.VMEM((draft_rows, LANES), F32),
            ] + [pltpu.SemaphoreType.DMA((tp,))] * 4,
            compiler_params=pltpu.CompilerParams(vmem_limit_bytes=20 * MIB, collective_id=0, has_side_effects=True),
        )(s, qv, mrow, lse, dt)

        block, stages = 32, 3
        res, acc, norm, bonus = pl.pallas_call(
            functools.partial(residual_kernel, (draft_rows, seqs, vocab, block, stages)),
            out_shape=(jax.ShapeDtypeStruct((draft_rows, vocab), F32), jax.ShapeDtypeStruct((drafts, seqs), F32),
                       jax.ShapeDtypeStruct((drafts, seqs), F32), jax.ShapeDtypeStruct((1, seqs), F32)),
            in_specs=[spec(vmem)] * 5,
            out_specs=(spec(hbm), spec(vmem), spec(vmem), spec(vmem)),
            scratch_shapes=[pltpu.VMEM((stages, block, vocab), F32), pltpu.SemaphoreType.DMA((stages,))],
            compiler_params=pltpu.CompilerParams(vmem_limit_bytes=16 * MIB),
        )(s, qv, lcol, ncol, small)
        res = res.reshape(drafts, seqs, vocab).transpose(1, 0, 2)
        return acc.T, norm.T, res, bonus.reshape(seqs)

    return jax.shard_map(
        local_step,
        mesh=mesh,
        in_specs=(P('dp', None, None), P(), P(None, 'tp'), P('dp', None, 'tp'), P('dp', None), P('dp')),
        out_specs=(P('dp', None), P('dp', None), P('dp', None, 'tp'), P('dp')),
        check_vma=False,
    )
```

```python
import functools

import jax
import jax.numpy as jnp
from jax import lax
from jax.experimental import pallas as pl
from jax.experimental.pallas import tpu as pltpu
from jax.sharding import PartitionSpec as P

F32 = jnp.float32
LANES = 128
NEG = -3.0e38
MIB = 1024 * 1024


def eye():
    rows = lax.broadcasted_iota(jnp.int32, (LANES, LANES), 0)
    return rows == lax.broadcasted_iota(jnp.int32, (LANES, LANES), 1)


def to_lanes(column):
    return jnp.sum(jnp.where(eye(), column, 0.0), axis=0, keepdims=True)


def to_column(row):
    col = jnp.sum(jnp.where(eye(), jnp.broadcast_to(row, (LANES, LANES)), 0.0), axis=1, keepdims=True)
    return jnp.broadcast_to(col, (LANES, LANES))


def head_kernel(dims, h_ref, g_ref, w_ref, q_ref, t_ref, s_ref, qv_ref, mrow_ref, lse_ref,
                hbuf, gbuf, tbuf, x, wbuf, m, sm, tinv, rinv, hsem, gsem, wsem, qsem):
    rows, draft_rows, seqs, depth, vocab, chunk, slots, qrows = dims
    n = pl.cdiv(vocab, chunk)
    tail = vocab - (n - 1) * chunk
    half = chunk // 2
    ktiles = depth // half
    groups = rows // 16
    copy = pltpu.make_async_copy

    def wcopy(i, size=chunk):
        slot = lax.rem(i, slots)
        at = pl.ds(pl.multiple_of(i * chunk, chunk), size)
        return copy(w_ref.at[at], wbuf.at[slot, pl.ds(0, size)], wsem.at[slot])

    def qcopy(i):
        at = pl.ds(pl.multiple_of(i * qrows, qrows), qrows)
        return copy(q_ref.at[at], qv_ref.at[at], qsem.at[i])

    def hcopy(i):
        at = pl.ds(pl.multiple_of(i * seqs, seqs), seqs)
        return copy(h_ref.at[at], hbuf.at[at], hsem.at[i])

    gcopy, tcopy = copy(g_ref, gbuf, gsem.at[0]), copy(t_ref, tbuf, gsem.at[1])
    gcopy.start()
    tcopy.start()
    for i in range(rows // seqs):
        hcopy(i).start()
    for i in range(3):
        wcopy(i).start()

    m[...] = jnp.full(m.shape, NEG, F32)
    sm[...] = jnp.zeros(sm.shape, F32)
    gcopy.wait()
    tcopy.wait()
    t = tbuf[...]
    spread = jnp.where(eye(), jnp.broadcast_to(jnp.concatenate([t, t], axis=1), (LANES, LANES)), 0.0)
    tcol = jnp.sum(spread, axis=1, keepdims=True)
    tinv[...] = jnp.broadcast_to(1.0 / tcol[:seqs], (seqs, LANES))

    @pl.loop(0, rows // seqs)
    def _(i):
        hcopy(i).wait()
        for b in range(0, seqs, 16):
            at = pl.ds(pl.multiple_of(i * seqs + b, 16), 16)
            h = hbuf[at, :].astype(F32)
            r = lax.rsqrt(jnp.mean(h * h, axis=1, keepdims=True) + 1e-5)
            rinv[at, :] = jnp.broadcast_to(r, (16, LANES))

    def normalise(k):
        for b in range(0, rows, 16):
            r = rinv[b:b + 16, :]
            for c in range(k * half, (k + 1) * half, LANES):
                h = hbuf[b:b + 16, c:c + LANES].astype(F32)
                x[b:b + 16, c:c + LANES] = (h * r * gbuf[:, c:c + LANES]).astype(jnp.bfloat16)

    def push(i, k):
        slot = lax.rem(i, slots)
        cols = slice(k * half, (k + 1) * half)
        for u in range(2):
            pltpu.matmul_push_rhs(wbuf[slot, u * half:(u + 1) * half, cols], k % 2, u, transpose=True)

    def run(*refs):
        accs = [[refs[(2 * u + v) * groups:(2 * u + v + 1) * groups] for v in range(2)] for u in range(2)]

        def stats(i, side, b, size=chunk, valid=chunk):
            base = pl.multiple_of(i * chunk, chunk)
            z = [pltpu.matmul_pop(accs[u][side][b]) for u in range(2)]
            for o in (0, 8):
                row = b * 16 + o
                r8 = slice(row, row + 8)
                ti = tinv[row % seqs:row % seqs + 8, :]
                parts = []
                for c in range(0, size, LANES):
                    s = z[c // half][o:o + 8, c % half:c % half + LANES] * ti
                    if c + LANES > valid:
                        lane = lax.broadcasted_iota(jnp.int32, (8, LANES), 1)
                        s = jnp.where(lane < valid - c, s, NEG)
                    parts.append(s)
                    if row < draft_rows:
                        s_ref[r8, pl.ds(base + c, LANES)] = s
                old = m[r8, :]
                new = old
                for s in parts:
                    new = jnp.maximum(new, s)
                tot = sm[r8, :] * jnp.exp(old - new)
                for s in parts:
                    tot = tot + jnp.exp(s - new)
                m[r8, :] = new
                sm[r8, :] = tot

        def matmul(i, side, last=False, first=False):
            for k in range(ktiles):
                if first:
                    normalise(k)
                if k + 1 < ktiles:
                    push(i, k + 1)
                elif not last:
                    push(i + 1, 0)
                for b in range(groups):
                    lhs = x[b * 16:(b + 1) * 16, k * half:(k + 1) * half]
                    for u in range(2):
                        pltpu.matmul_acc_lhs(accs[u][side][b], lhs, load_staged_rhs=k % 2 if b == 0 else None)
                    done = k * groups + b
                    if not first and done % ktiles == ktiles - 1:
                        stats(i - 1, 1 - side, done // ktiles)

        nq = draft_rows // qrows
        pairs = (n - 2) // 2
        wcopy(0).wait()
        push(0, 0)
        wcopy(1).wait()
        matmul(0, 0, first=True)

        @pl.loop(0, pairs)
        def _(k):
            i = 2 * k + 1

            @pl.when(k < pairs - 1)
            def _():
                wcopy(i + 2).start()
                wcopy(i + 3).start()
                qcopy(2 * k).start()
                qcopy(2 * k + 1).start()

            @pl.when(k == pairs - 1)
            def _():
                wcopy(n - 1, tail).start()

            wcopy(i + 1).wait()
            matmul(i, 1)

            @pl.when(k < pairs - 1)
            def _():
                wcopy(i + 2).wait()

            @pl.when(k == pairs - 1)
            def _():
                wcopy(n - 1, tail).wait()

            matmul(i + 1, 0)

        matmul(n - 1, 1, True)
        for b in range(groups):
            stats(n - 1, 1, b, pl.cdiv(tail, LANES) * LANES, tail)

    pl.run_scoped(run, *(pltpu.ACC(u)((16, half), F32) for u in range(2) for _ in range(2 * groups)))

    lse_ref[...] = jnp.zeros(lse_ref.shape, F32)
    for i in range(pl.cdiv(rows, LANES)):
        size = min(LANES, rows - i * LANES)
        r = slice(i * LANES, i * LANES + size)
        ml = m[r, :]
        mrow = jnp.max(ml, axis=1, keepdims=True)
        srow = jnp.sum(sm[r, :] * jnp.exp(ml - mrow), axis=1, keepdims=True)
        lse = jnp.broadcast_to(mrow + jnp.log(srow), (size, LANES))
        if i * LANES < draft_rows:
            mrow_ref[r, :] = jnp.broadcast_to(mrow, (size, LANES))
        mask = eye()[:size]
        lse_ref[i:i + 1, :] = jnp.sum(jnp.where(mask, lse, 0.0), axis=0, keepdims=True)

    for i in range(draft_rows // qrows):
        qcopy(i).wait()


def verify_kernel(dims, s_ref, q_ref, mrow_ref, lse_ref, dt_ref, lcol_ref, ncol_ref, out_ref,
                  e_ref, ccol_ref, g1, g2, msg2, acc, tok, send1, recv1, send2, recv2):
    tp, draft_rows, seqs, vocab = dims
    blocks = draft_rows // LANES
    me = lax.axis_index("tp")
    full = vocab // LANES * LANES
    rest = vocab - full

    barrier = pltpu.get_barrier_semaphore()
    for d in range(1, tp):
        pl.semaphore_signal(barrier, inc=1, device_id={"tp": lax.rem(me + d, tp)},
                            device_id_type=pl.DeviceIdType.MESH)
    pl.semaphore_wait(barrier, tp - 1)

    def exchange(src, gather, send, recv):
        def copy(slot, sem, d):
            return pltpu.make_async_remote_copy(
                src_ref=src, dst_ref=gather.at[slot], send_sem=send.at[d], recv_sem=recv.at[sem],
                device_id={"tp": lax.rem(me + d, tp)}, device_id_type=pl.DeviceIdType.MESH)

        def start():
            for d in range(1, tp):
                copy(me, me, d).start()
            gather[me] = src[...]

        def wait():
            for d in range(1, tp):
                peer = lax.rem(me + d, tp)
                copy(peer, peer, d).wait_recv()

        def drain():
            for d in range(1, tp):
                copy(me, me, d).wait_send()

        return start, wait, drain

    start1, wait1, drain1 = exchange(lse_ref, g1, send1, recv1)
    start2, wait2, drain2 = exchange(msg2, g2, send2, recv2)
    start1()

    offset = me * vocab
    for i in range(blocks):
        ids = jnp.concatenate([dt_ref[2 * i:2 * i + 1, :], dt_ref[2 * i + 1:2 * i + 2, :]], axis=1)
        tok[i * LANES:(i + 1) * LANES, :] = to_column((ids - offset).astype(F32))

    lane = lax.broadcasted_iota(jnp.int32, (8, LANES), 1).astype(F32)

    acc[...] = jnp.zeros(acc.shape, F32)

    @pl.loop(0, draft_rows // 8)
    def _(b):
        r8 = pl.ds(pl.multiple_of(b * 8, 8), 8)
        mr = mrow_ref[r8, :]
        want = tok[r8, :]
        er = jnp.exp(s_ref[r8, full:full + rest] - mr[:, :rest])
        e_ref[r8, full:full + rest] = er
        qr = q_ref[r8, full:full + rest]
        hit = (lane[:, :rest] + float(full)) == want[:, :rest]
        acc[0, r8, 0:rest] = jnp.where(hit, er, 0.0)
        acc[1, r8, 0:rest] = jnp.where(hit, qr, 0.0)
        ae, aq = acc[0, r8, :], acc[1, r8, :]
        for c in range(0, full, LANES):
            e = jnp.exp(s_ref[r8, c:c + LANES] - mr)
            e_ref[r8, c:c + LANES] = e
            hit = (lane + float(c)) == want
            ae = ae + jnp.where(hit, e, 0.0)
            aq = aq + jnp.where(hit, q_ref[r8, c:c + LANES], 0.0)
        acc[0, r8, :] = ae
        acc[1, r8, :] = aq

    wait1()
    parts = g1[...]
    top = jnp.max(parts, axis=0)
    lse = top + jnp.log(jnp.sum(jnp.exp(parts - top[None]), axis=0))
    out_ref[...] = jnp.zeros(out_ref.shape, F32)
    out_ref[0:4, :] = lse
    for i in range(blocks):
        r = slice(i * LANES, (i + 1) * LANES)
        lcol = to_column(lse[i:i + 1, :])
        lcol_ref[r, :] = lcol
        ccol_ref[r, :] = jnp.exp(mrow_ref[r, :] - lcol)

    @pl.loop(0, draft_rows // 8)
    def _(b):
        r8 = pl.ds(pl.multiple_of(b * 8, 8), 8)
        cc = ccol_ref[r8, :]
        er = e_ref[r8, full:full + rest]
        acc[2, r8, 0:rest] = jnp.maximum(er * cc[:, :rest] - q_ref[r8, full:full + rest], 0.0)
        sums = [acc[2, r8, :], jnp.zeros((8, LANES), F32)]
        for k, c in enumerate(range(0, full, LANES)):
            sums[k % 2] += jnp.maximum(e_ref[r8, c:c + LANES] * cc - q_ref[r8, c:c + LANES], 0.0)
        acc[2, r8, :] = sums[0] + sums[1]

    msg2[...] = jnp.zeros(msg2.shape, F32)
    for i in range(blocks):
        r = slice(i * LANES, (i + 1) * LANES)
        total = jnp.sum(acc[2, r, :], axis=1, keepdims=True)
        msg2[i:i + 1, :] = to_lanes(jnp.broadcast_to(total, (LANES, LANES)))
        p = jnp.sum(acc[0, r, :], axis=1, keepdims=True) * ccol_ref[r, 0:1]
        qt = jnp.sum(acc[1, r, :], axis=1, keepdims=True)
        ok = jnp.where(qt > 0.0, jnp.minimum(1.0, p / jnp.where(qt > 0.0, qt, 1.0)), 0.0)
        msg2[4 + i:5 + i, :] = to_lanes(jnp.broadcast_to(ok, (LANES, LANES)))
    start2()
    wait2()
    sums = jnp.sum(g2[...], axis=0)
    out_ref[4:4 + 8, :] = sums
    for i in range(blocks):
        ncol_ref[i * LANES:(i + 1) * LANES, :] = to_column(1.0 / sums[i:i + 1, :])
    drain1()
    drain2()


def residual_kernel(dims, s_ref, q_ref, lcol_ref, ncol_ref, small_ref, res_ref, acc_ref, norm_ref, bonus_ref,
                    stage, sem):
    draft_rows, seqs, vocab, block, slots = dims
    n = draft_rows // block
    full = vocab // LANES * LANES
    rest = vocab - full

    def copy(i):
        slot = lax.rem(i, slots)
        return pltpu.make_async_copy(stage.at[slot], res_ref.at[pl.ds(pl.multiple_of(i * block, block), block)],
                                     sem.at[slot])

    @pl.loop(0, n)
    def _(i):
        slot = lax.rem(i, slots)

        @pl.when(i >= slots)
        def _():
            copy(i - slots).wait()

        for b in range(block // 8):
            src = pl.ds(pl.multiple_of(i * block + b * 8, 8), 8)
            dst = slice(b * 8, b * 8 + 8)
            lc, inv = lcol_ref[src, :], ncol_ref[src, :]
            for c in range(0, full, LANES):
                stage[slot, dst, c:c + LANES] = (
                    jnp.maximum(jnp.exp(s_ref[src, c:c + LANES] - lc) - q_ref[src, c:c + LANES], 0.0) * inv)
            stage[slot, dst, full:full + rest] = (
                jnp.maximum(jnp.exp(s_ref[src, full:full + rest] - lc[:, :rest]) - q_ref[src, full:full + rest], 0.0)
                * inv[:, :rest])
        copy(i).start()

    for j in range(draft_rows // seqs):
        i, off = j // 2, (j % 2) * seqs
        norm_ref[j:j + 1, :] = small_ref[4 + i:5 + i, off:off + seqs]
        acc_ref[j:j + 1, :] = small_ref[8 + i:9 + i, off:off + seqs]
    bonus_ref[...] = small_ref[3:4, 0:seqs]

    for i in range(n - slots, n):
        copy(i).wait()


def solution(mesh):
    tp = mesh.shape["tp"]
    vmem, hbm = pltpu.VMEM, pltpu.HBM

    def spec(space):
        return pl.BlockSpec(memory_space=space)

    def local_step(hidden, norm_gain, w_head, draft_probs, draft_tokens, temperature):
        seqs, positions, depth = hidden.shape
        drafts, vocab = draft_probs.shape[1:]
        rows, draft_rows = seqs * positions, seqs * drafts
        wide = pl.cdiv(vocab, LANES) * LANES
        h = hidden.transpose(1, 0, 2).reshape(rows, depth)
        w = w_head.T
        q = draft_probs.transpose(1, 0, 2).reshape(draft_rows, vocab)
        dt = draft_tokens.T
        chunk, slots, qrows = 512, 4, 32
        dims = (rows, draft_rows, seqs, depth, vocab, chunk, slots, qrows)
        s, qv, mrow, lse = pl.pallas_call(
            functools.partial(head_kernel, dims),
            out_shape=(pltpu.VMEM((draft_rows, wide), F32), pltpu.VMEM((draft_rows, vocab), F32),
                       pltpu.VMEM((draft_rows, LANES), F32), pltpu.VMEM((4, LANES), F32)),
            in_specs=[spec(hbm)] * 5,
            out_specs=(spec(vmem),) * 4,
            scratch_shapes=[
                pltpu.VMEM((rows, depth), jnp.bfloat16), pltpu.VMEM((1, depth), F32), pltpu.VMEM((1, seqs), F32),
                pltpu.VMEM((rows, depth), jnp.bfloat16), pltpu.VMEM((slots, chunk, depth), jnp.bfloat16),
                pltpu.VMEM((rows, LANES), F32), pltpu.VMEM((rows, LANES), F32), pltpu.VMEM((seqs, LANES), F32),
                pltpu.VMEM((rows, LANES), F32),
                pltpu.SemaphoreType.DMA((positions,)), pltpu.SemaphoreType.DMA((2,)),
                pltpu.SemaphoreType.DMA((slots,)), pltpu.SemaphoreType.DMA((draft_rows // qrows,)),
            ],
            compiler_params=pltpu.CompilerParams(vmem_limit_bytes=24 * MIB),
        )(*(pltpu.with_memory_space_constraint(a, hbm)
            for a in (h, norm_gain.reshape(1, depth), w, q, temperature.reshape(1, seqs))))

        lcol, ncol, small = pl.pallas_call(
            functools.partial(verify_kernel, (tp, draft_rows, seqs, vocab)),
            out_shape=(pltpu.VMEM((draft_rows, LANES), F32), pltpu.VMEM((draft_rows, LANES), F32),
                       pltpu.VMEM((16, LANES), F32)),
            in_specs=[spec(vmem)] * 5,
            out_specs=(spec(vmem),) * 3,
            scratch_shapes=[
                pltpu.VMEM((draft_rows, wide), F32), pltpu.VMEM((draft_rows, LANES), F32),
                pltpu.VMEM((tp, 4, LANES), F32), pltpu.VMEM((tp, 8, LANES), F32), pltpu.VMEM((8, LANES), F32),
                pltpu.VMEM((3, draft_rows, LANES), F32), pltpu.VMEM((draft_rows, LANES), F32),
            ] + [pltpu.SemaphoreType.DMA((tp,))] * 4,
            compiler_params=pltpu.CompilerParams(vmem_limit_bytes=20 * MIB, collective_id=0, has_side_effects=True),
        )(s, qv, mrow, lse, dt)

        block, stages = 32, 3
        res, acc, norm, bonus = pl.pallas_call(
            functools.partial(residual_kernel, (draft_rows, seqs, vocab, block, stages)),
            out_shape=(jax.ShapeDtypeStruct((draft_rows, vocab), F32), jax.ShapeDtypeStruct((drafts, seqs), F32),
                       jax.ShapeDtypeStruct((drafts, seqs), F32), jax.ShapeDtypeStruct((1, seqs), F32)),
            in_specs=[spec(vmem)] * 5,
            out_specs=(spec(hbm), spec(vmem), spec(vmem), spec(vmem)),
            scratch_shapes=[pltpu.VMEM((stages, block, vocab), F32), pltpu.SemaphoreType.DMA((stages,))],
            compiler_params=pltpu.CompilerParams(vmem_limit_bytes=16 * MIB),
        )(s, qv, lcol, ncol, small)
        res = res.reshape(drafts, seqs, vocab).transpose(1, 0, 2)
        return acc.T, norm.T, res, bonus.reshape(seqs)

    return jax.shard_map(
        local_step,
        mesh=mesh,
        in_specs=(P('dp', None, None), P(), P(None, 'tp'), P('dp', None, 'tp'), P('dp', None), P('dp')),
        out_specs=(P('dp', None), P('dp', None), P('dp', None, 'tp'), P('dp')),
        check_vma=False,
    )
```

```python
import functools

import jax
import jax.numpy as jnp
from jax import lax
from jax.experimental import pallas as pl
from jax.experimental.pallas import tpu as pltpu
from jax.sharding import PartitionSpec as P

F32 = jnp.float32
LANES = 128
NEG = -3.0e38
MIB = 1024 * 1024


def eye():
    rows = lax.broadcasted_iota(jnp.int32, (LANES, LANES), 0)
    return rows == lax.broadcasted_iota(jnp.int32, (LANES, LANES), 1)


def to_lanes(column):
    return jnp.sum(jnp.where(eye(), column, 0.0), axis=0, keepdims=True)


def to_column(row):
    col = jnp.sum(jnp.where(eye(), jnp.broadcast_to(row, (LANES, LANES)), 0.0), axis=1, keepdims=True)
    return jnp.broadcast_to(col, (LANES, LANES))


def head_kernel(dims, h_ref, g_ref, w_ref, q_ref, t_ref, dt_ref, s_ref, qv_ref, mrow_ref, lse_ref, at_ref,
                hbuf, gbuf, tbuf, dbuf, ids, x, wbuf, m, sm, tinv, rinv, tok, hsem, gsem, fsem, wsem, qsem):
    rows, draft_rows, seqs, depth, vocab, chunk, slots, qrows = dims
    n = pl.cdiv(vocab, chunk)
    tail = vocab - (n - 1) * chunk
    half = chunk // 2
    ktiles = depth // half
    groups = rows // 16
    copy = pltpu.make_async_copy

    def wcopy(i):
        slot = lax.rem(i, slots)
        at = pl.ds(pl.multiple_of(i * chunk, chunk), chunk)
        return copy(w_ref.at[at], wbuf.at[slot], wsem.at[slot])

    def wfirst(p):
        cols = slice(p * depth // 4, (p + 1) * depth // 4)
        return copy(w_ref.at[0:chunk, cols], wbuf.at[0, :, cols], fsem.at[p])

    def wlast():
        slot = (n - 1) % slots
        return [copy(w_ref.at[vocab - tail:vocab], wbuf.at[slot, 0:tail], wsem.at[slot]),
                copy(w_ref.at[0:chunk - tail], wbuf.at[slot, tail:chunk], wsem.at[slot])]

    def wwait(i):
        slot = lax.rem(i, slots)
        copy(w_ref.at[0:chunk], wbuf.at[slot], wsem.at[slot]).wait()

    def qcopy(i):
        at = pl.ds(pl.multiple_of(i * qrows, qrows), qrows)
        return copy(q_ref.at[at], qv_ref.at[at], qsem.at[i])

    def hcopy(i):
        at = pl.ds(pl.multiple_of(i * seqs, seqs), seqs)
        return copy(h_ref.at[at], hbuf.at[at], hsem.at[i])

    small = [copy(src, dst, gsem.at[i])
             for i, (src, dst) in enumerate(((g_ref, gbuf), (t_ref, tbuf), (dt_ref, dbuf), (dt_ref, ids)))]
    for c in small:
        c.start()
    for i in range(rows // seqs):
        hcopy(i).start()
    for p in range(4):
        wfirst(p).start()
    for i in range(1, 3):
        wcopy(i).start()

    m[...] = jnp.full(m.shape, NEG, F32)
    sm[...] = jnp.zeros(sm.shape, F32)
    at_ref[...] = jnp.zeros(at_ref.shape, F32)
    for c in small:
        c.wait()
    offset = lax.axis_index("tp") * vocab
    for i in range(draft_rows // LANES):
        row = jnp.concatenate([dbuf[2 * i:2 * i + 1, :], dbuf[2 * i + 1:2 * i + 2, :]], axis=1)
        tok[i * LANES:(i + 1) * LANES, :] = to_column((row - offset).astype(F32))
    lane = lax.broadcasted_iota(jnp.int32, (8, LANES), 1)
    lanef = lane.astype(F32)
    sub = lax.broadcasted_iota(jnp.int32, (8, LANES), 0)
    full = vocab // LANES * LANES
    rest = vocab - full
    t = tbuf[...]
    spread = jnp.where(eye(), jnp.broadcast_to(jnp.concatenate([t, t], axis=1), (LANES, LANES)), 0.0)
    tcol = jnp.sum(spread, axis=1, keepdims=True)
    tinv[...] = jnp.broadcast_to(1.0 / tcol[:seqs], (seqs, LANES))

    @pl.loop(0, rows // seqs)
    def _(i):
        hcopy(i).wait()
        for b in range(0, seqs, 16):
            at = pl.ds(pl.multiple_of(i * seqs + b, 16), 16)
            h = hbuf[at, :].astype(F32)
            r = lax.rsqrt(jnp.mean(h * h, axis=1, keepdims=True) + 1e-5)
            rinv[at, :] = jnp.broadcast_to(r, (16, LANES))

    def normalise(k):
        for b in range(0, rows, 16):
            r = rinv[b:b + 16, :]
            for c in range(k * half, (k + 1) * half, LANES):
                h = hbuf[b:b + 16, c:c + LANES].astype(F32)
                x[b:b + 16, c:c + LANES] = (h * r * gbuf[:, c:c + LANES]).astype(jnp.bfloat16)

    def push(i, k):
        slot = lax.rem(i, slots)
        cols = slice(k * half, (k + 1) * half)
        for u in range(2):
            pltpu.matmul_push_rhs(wbuf[slot, u * half:(u + 1) * half, cols], k % 2, u, transpose=True)

    def run(*refs):
        accs = [[refs[(2 * u + v) * groups:(2 * u + v + 1) * groups] for v in range(2)] for u in range(2)]

        def stats(i, side, b, size=chunk, valid=chunk):
            base = pl.multiple_of(i * chunk, chunk)
            first_id = lax.convert_element_type(base, F32)
            z = [pltpu.matmul_pop(accs[u][side][b]) for u in range(2)]
            for o in (0, 8):
                row = b * 16 + o
                r8 = slice(row, row + 8)
                ti = tinv[row % seqs:row % seqs + 8, :]
                parts = []
                for c in range(0, size, LANES):
                    s = z[c // half][o:o + 8, c % half:c % half + LANES] * ti
                    if c + LANES > valid:
                        s = jnp.where(lane < valid - c, s, NEG)
                    parts.append(s)
                    if row < draft_rows:
                        s_ref[r8, pl.ds(base + c, LANES)] = s
                if row < draft_rows:
                    want = tok[r8, :] - first_id
                    found = at_ref[0, r8, :]
                    for c, s in zip(range(0, size, LANES), parts):
                        found = found + jnp.where(lanef + float(c) == want, s, 0.0)
                    at_ref[0, r8, :] = found
                old = m[r8, :]
                new = old
                for s in parts:
                    new = jnp.maximum(new, s)
                tot = sm[r8, :] * jnp.exp(old - new)
                for s in parts:
                    tot = tot + jnp.exp(s - new)
                m[r8, :] = new
                sm[r8, :] = tot

        def draft(row):
            b = row // 8 * 8
            r8 = slice(b, b + 8)
            if row == b:
                hit = lanef[:, :rest] + float(full) == tok[r8, 0:rest]
                at_ref[1, r8, 0:rest] = jnp.where(hit, qv_ref[r8, full:full + rest], 0.0)
            token = ids[row // seqs, row % seqs] - offset
            tile = jnp.clip(token >> 7, 0, full // LANES - 1) * LANES
            hit = jnp.logical_and(lane == token - tile, sub == row - b)
            at_ref[1, r8, :] += jnp.where(hit, qv_ref[r8, pl.ds(pl.multiple_of(tile, LANES), LANES)], 0.0)

        def matmul(i, side, last=False, first=False):
            for k in range(ktiles):
                if first:
                    normalise(k)
                if k + 1 < ktiles:
                    if first and (k + 1) % (ktiles // 4) == 0:
                        wfirst((k + 1) // (ktiles // 4)).wait()
                    push(i, k + 1)
                elif not last:
                    wwait(i + 1)
                    push(i + 1, 0)
                for b in range(groups):
                    lhs = x[b * 16:(b + 1) * 16, k * half:(k + 1) * half]
                    for u in range(2):
                        pltpu.matmul_acc_lhs(accs[u][side][b], lhs, load_staged_rhs=k % 2 if b == 0 else None)
                    done = k * groups + b
                    if last:
                        steps = ktiles * groups
                        for row in range(draft_rows * done // steps, draft_rows * (done + 1) // steps):
                            draft(row)
                    if not first and done % ktiles == ktiles - 1:
                        stats(i - 1, 1 - side, done // ktiles)

        pairs = (n - 2) // 2
        wfirst(0).wait()
        push(0, 0)
        wcopy(3).start()
        matmul(0, 0, first=True)

        @pl.loop(0, pairs)
        def _(k):
            i = 2 * k + 1

            @pl.when(k < pairs - 1)
            def _():
                wcopy(i + 3).start()
                qcopy(2 * k).start()
                qcopy(2 * k + 1).start()

            matmul(i, 1)

            @pl.when(k < pairs - 2)
            def _():
                wcopy(i + 4).start()

            @pl.when(k == pairs - 2)
            def _():
                for c in wlast():
                    c.start()

            matmul(i + 1, 0)

        for i in range(draft_rows // qrows):
            qcopy(i).wait()
        matmul(n - 1, 1, True)
        for b in range(groups):
            stats(n - 1, 1, b, pl.cdiv(tail, LANES) * LANES, tail)

    pl.run_scoped(run, *(pltpu.ACC(u)((16, half), F32) for u in range(2) for _ in range(2 * groups)))

    lse_ref[...] = jnp.zeros(lse_ref.shape, F32)
    for i in range(pl.cdiv(rows, LANES)):
        size = min(LANES, rows - i * LANES)
        r = slice(i * LANES, i * LANES + size)
        ml = m[r, :]
        mrow = jnp.max(ml, axis=1, keepdims=True)
        srow = jnp.sum(sm[r, :] * jnp.exp(ml - mrow), axis=1, keepdims=True)
        lse = jnp.broadcast_to(mrow + jnp.log(srow), (size, LANES))
        if i * LANES < draft_rows:
            mrow_ref[r, :] = jnp.broadcast_to(mrow, (size, LANES))
        mask = eye()[:size]
        lse_ref[i:i + 1, :] = jnp.sum(jnp.where(mask, lse, 0.0), axis=0, keepdims=True)


def verify_kernel(dims, s_ref, q_ref, mrow_ref, lse_ref, at_ref, lcol_ref, ncol_ref, out_ref,
                  e_ref, ccol_ref, g1, g2, msg2, acc, send1, recv1, send2, recv2):
    tp, draft_rows, seqs, vocab = dims
    blocks = draft_rows // LANES
    me = lax.axis_index("tp")
    full = vocab // LANES * LANES
    rest = vocab - full

    barrier = pltpu.get_barrier_semaphore()
    for d in range(1, tp):
        pl.semaphore_signal(barrier, inc=1, device_id={"tp": lax.rem(me + d, tp)},
                            device_id_type=pl.DeviceIdType.MESH)
    pl.semaphore_wait(barrier, tp - 1)

    def exchange(src, gather, send, recv):
        def copy(slot, sem, d):
            return pltpu.make_async_remote_copy(
                src_ref=src, dst_ref=gather.at[slot], send_sem=send.at[d], recv_sem=recv.at[sem],
                device_id={"tp": lax.rem(me + d, tp)}, device_id_type=pl.DeviceIdType.MESH)

        def start():
            for d in range(1, tp):
                copy(me, me, d).start()
            gather[me] = src[...]

        def wait():
            for d in range(1, tp):
                peer = lax.rem(me + d, tp)
                copy(peer, peer, d).wait_recv()

        def drain():
            for d in range(1, tp):
                copy(me, me, d).wait_send()

        return start, wait, drain

    start1, wait1, drain1 = exchange(lse_ref, g1, send1, recv1)
    start2, wait2, drain2 = exchange(msg2, g2, send2, recv2)
    start1()

    acc[...] = jnp.zeros(acc.shape, F32)

    @pl.loop(0, draft_rows // 8)
    def _(b):
        r8 = pl.ds(pl.multiple_of(b * 8, 8), 8)
        mr = mrow_ref[r8, :]
        e_ref[r8, full:full + rest] = jnp.exp(s_ref[r8, full:full + rest] - mr[:, :rest])
        for c in range(0, full, LANES):
            e_ref[r8, c:c + LANES] = jnp.exp(s_ref[r8, c:c + LANES] - mr)

    wait1()
    parts = g1[...]
    top = jnp.max(parts, axis=0)
    lse = top + jnp.log(jnp.sum(jnp.exp(parts - top[None]), axis=0))
    out_ref[...] = jnp.zeros(out_ref.shape, F32)
    out_ref[0:4, :] = lse
    for i in range(blocks):
        r = slice(i * LANES, (i + 1) * LANES)
        lcol = to_column(lse[i:i + 1, :])
        lcol_ref[r, :] = lcol
        ccol_ref[r, :] = jnp.exp(mrow_ref[r, :] - lcol)

    @pl.loop(0, draft_rows // 8)
    def _(b):
        r8 = pl.ds(pl.multiple_of(b * 8, 8), 8)
        cc = ccol_ref[r8, :]
        er = e_ref[r8, full:full + rest]
        acc[r8, 0:rest] = jnp.maximum(er * cc[:, :rest] - q_ref[r8, full:full + rest], 0.0)
        sums = [acc[r8, :]] + [jnp.zeros((8, LANES), F32)] * 3
        for k, c in enumerate(range(0, full, LANES)):
            sums[k % 4] += jnp.maximum(e_ref[r8, c:c + LANES] * cc - q_ref[r8, c:c + LANES], 0.0)
        acc[r8, :] = (sums[0] + sums[1]) + (sums[2] + sums[3])

    msg2[...] = jnp.zeros(msg2.shape, F32)
    for i in range(blocks):
        r = slice(i * LANES, (i + 1) * LANES)
        total = jnp.sum(acc[r, :], axis=1, keepdims=True)
        msg2[i:i + 1, :] = to_lanes(jnp.broadcast_to(total, (LANES, LANES)))
        p = jnp.exp(jnp.sum(at_ref[0, r, :], axis=1, keepdims=True) - lcol_ref[r, 0:1])
        qt = jnp.sum(at_ref[1, r, :], axis=1, keepdims=True)
        ok = jnp.where(qt > 0.0, jnp.minimum(1.0, p / jnp.where(qt > 0.0, qt, 1.0)), 0.0)
        msg2[4 + i:5 + i, :] = to_lanes(jnp.broadcast_to(ok, (LANES, LANES)))
    start2()
    wait2()
    sums = jnp.sum(g2[...], axis=0)
    out_ref[4:4 + 8, :] = sums
    for i in range(blocks):
        ncol_ref[i * LANES:(i + 1) * LANES, :] = to_column(1.0 / sums[i:i + 1, :])
    drain1()
    drain2()


def residual_kernel(dims, s_ref, q_ref, lcol_ref, ncol_ref, small_ref, res_ref, acc_ref, norm_ref, bonus_ref,
                    stage, sem):
    draft_rows, seqs, vocab, block, slots = dims
    n = draft_rows // block
    full = vocab // LANES * LANES
    rest = vocab - full

    def copy(i):
        slot = lax.rem(i, slots)
        return pltpu.make_async_copy(stage.at[slot], res_ref.at[pl.ds(pl.multiple_of(i * block, block), block)],
                                     sem.at[slot])

    @pl.loop(0, n)
    def _(i):
        slot = lax.rem(i, slots)

        for b in range(block // 8):
            src = pl.ds(pl.multiple_of(i * block + b * 8, 8), 8)
            dst = slice(b * 8, b * 8 + 8)
            lc, inv = lcol_ref[src, :], ncol_ref[src, :]
            for c in range(0, full, LANES):
                stage[slot, dst, c:c + LANES] = (
                    jnp.maximum(jnp.exp(s_ref[src, c:c + LANES] - lc) - q_ref[src, c:c + LANES], 0.0) * inv)
            stage[slot, dst, full:full + rest] = (
                jnp.maximum(jnp.exp(s_ref[src, full:full + rest] - lc[:, :rest]) - q_ref[src, full:full + rest], 0.0)
                * inv[:, :rest])
        copy(i).start()

    for j in range(draft_rows // seqs):
        i, off = j // 2, (j % 2) * seqs
        norm_ref[j:j + 1, :] = small_ref[4 + i:5 + i, off:off + seqs]
        acc_ref[j:j + 1, :] = small_ref[8 + i:9 + i, off:off + seqs]
    bonus_ref[...] = small_ref[3:4, 0:seqs]

    for i in range(n - slots, n):
        copy(i).wait()


def solution(mesh):
    tp = mesh.shape["tp"]
    vmem, hbm = pltpu.VMEM, pltpu.HBM

    def spec(space):
        return pl.BlockSpec(memory_space=space)

    def local_step(hidden, norm_gain, w_head, draft_probs, draft_tokens, temperature):
        seqs, positions, depth = hidden.shape
        drafts, vocab = draft_probs.shape[1:]
        rows, draft_rows = seqs * positions, seqs * drafts
        wide = pl.cdiv(vocab, LANES) * LANES
        h = hidden.transpose(1, 0, 2).reshape(rows, depth)
        w = w_head.T
        q = draft_probs.transpose(1, 0, 2).reshape(draft_rows, vocab)
        dt = draft_tokens.T
        chunk, slots, qrows = 512, 4, 32
        dims = (rows, draft_rows, seqs, depth, vocab, chunk, slots, qrows)
        s, qv, mrow, lse, at = pl.pallas_call(
            functools.partial(head_kernel, dims),
            out_shape=(pltpu.VMEM((draft_rows, wide), F32), pltpu.VMEM((draft_rows, vocab), F32),
                       pltpu.VMEM((draft_rows, LANES), F32), pltpu.VMEM((4, LANES), F32),
                       pltpu.VMEM((2, draft_rows, LANES), F32)),
            in_specs=[spec(hbm)] * 6,
            out_specs=(spec(vmem),) * 5,
            scratch_shapes=[
                pltpu.VMEM((rows, depth), jnp.bfloat16), pltpu.VMEM((1, depth), F32), pltpu.VMEM((1, seqs), F32),
                pltpu.VMEM((drafts, seqs), jnp.int32), pltpu.SMEM((drafts, seqs), jnp.int32),
                pltpu.VMEM((rows, depth), jnp.bfloat16), pltpu.VMEM((slots, chunk, depth), jnp.bfloat16),
                pltpu.VMEM((rows, LANES), F32), pltpu.VMEM((rows, LANES), F32), pltpu.VMEM((seqs, LANES), F32),
                pltpu.VMEM((rows, LANES), F32), pltpu.VMEM((draft_rows, LANES), F32),
                pltpu.SemaphoreType.DMA((positions,)), pltpu.SemaphoreType.DMA((4,)), pltpu.SemaphoreType.DMA((4,)),
                pltpu.SemaphoreType.DMA((slots,)), pltpu.SemaphoreType.DMA((draft_rows // qrows,)),
            ],
            compiler_params=pltpu.CompilerParams(vmem_limit_bytes=24 * MIB),
        )(*(pltpu.with_memory_space_constraint(a, hbm)
            for a in (h, norm_gain.reshape(1, depth), w, q, temperature.reshape(1, seqs), dt)))

        lcol, ncol, small = pl.pallas_call(
            functools.partial(verify_kernel, (tp, draft_rows, seqs, vocab)),
            out_shape=(pltpu.VMEM((draft_rows, LANES), F32), pltpu.VMEM((draft_rows, LANES), F32),
                       pltpu.VMEM((16, LANES), F32)),
            in_specs=[spec(vmem)] * 5,
            out_specs=(spec(vmem),) * 3,
            scratch_shapes=[
                pltpu.VMEM((draft_rows, wide), F32), pltpu.VMEM((draft_rows, LANES), F32),
                pltpu.VMEM((tp, 4, LANES), F32), pltpu.VMEM((tp, 8, LANES), F32), pltpu.VMEM((8, LANES), F32),
                pltpu.VMEM((draft_rows, LANES), F32),
            ] + [pltpu.SemaphoreType.DMA((tp,))] * 4,
            compiler_params=pltpu.CompilerParams(vmem_limit_bytes=20 * MIB, collective_id=0, has_side_effects=True),
        )(s, qv, mrow, lse, at)

        block = 16
        stages = draft_rows // block
        res, acc, norm, bonus = pl.pallas_call(
            functools.partial(residual_kernel, (draft_rows, seqs, vocab, block, stages)),
            out_shape=(jax.ShapeDtypeStruct((draft_rows, vocab), F32), jax.ShapeDtypeStruct((drafts, seqs), F32),
                       jax.ShapeDtypeStruct((drafts, seqs), F32), jax.ShapeDtypeStruct((1, seqs), F32)),
            in_specs=[spec(vmem)] * 5,
            out_specs=(spec(hbm), spec(vmem), spec(vmem), spec(vmem)),
            scratch_shapes=[pltpu.VMEM((stages, block, vocab), F32), pltpu.SemaphoreType.DMA((stages,))],
            compiler_params=pltpu.CompilerParams(vmem_limit_bytes=16 * MIB),
        )(s, qv, lcol, ncol, small)
        res = res.reshape(drafts, seqs, vocab).transpose(1, 0, 2)
        return acc.T, norm.T, res, bonus.reshape(seqs)

    return jax.shard_map(
        local_step,
        mesh=mesh,
        in_specs=(P('dp', None, None), P(), P(None, 'tp'), P('dp', None, 'tp'), P('dp', None), P('dp')),
        out_specs=(P('dp', None), P('dp', None), P('dp', None, 'tp'), P('dp')),
        check_vma=False,
    )
```

```python
import functools

import jax
import jax.numpy as jnp
from jax import lax
from jax.experimental import pallas as pl
from jax.experimental.pallas import tpu as pltpu
from jax.sharding import PartitionSpec as P

F32 = jnp.float32
LANES = 128
NEG = -3.0e38
LOG2E = 1.4426950408889634
MIB = 1024 * 1024


def eye():
    rows = lax.broadcasted_iota(jnp.int32, (LANES, LANES), 0)
    return rows == lax.broadcasted_iota(jnp.int32, (LANES, LANES), 1)


def to_lanes(column):
    return jnp.sum(jnp.where(eye(), column, 0.0), axis=0, keepdims=True)


def to_column(row):
    col = jnp.sum(jnp.where(eye(), jnp.broadcast_to(row, (LANES, LANES)), 0.0), axis=1, keepdims=True)
    return jnp.broadcast_to(col, (LANES, LANES))


def head_kernel(dims, h_ref, g_ref, w_ref, q_ref, t_ref, s_ref, qv_ref, mrow_ref, lse_ref, scale_ref,
                hbuf, gbuf, tbuf, x, wbuf, m, sm, rinv, hsem, gsem, fsem, wsem, qsem):
    rows, draft_rows, seqs, depth, vocab, chunk, slots, qrows = dims
    n = pl.cdiv(vocab, chunk)
    tail = vocab - (n - 1) * chunk
    half = chunk // 2
    ktiles = depth // half
    groups = rows // 16
    copy = pltpu.make_async_copy

    def wcopy(i):
        slot = lax.rem(i, slots)
        at = pl.ds(pl.multiple_of(i * chunk, chunk), chunk)
        return copy(w_ref.at[at], wbuf.at[slot], wsem.at[slot])

    def wfirst(p):
        cols = slice(p * depth // 4, (p + 1) * depth // 4)
        return copy(w_ref.at[0:chunk, cols], wbuf.at[0, :, cols], fsem.at[p])

    def wlast():
        slot = (n - 1) % slots
        return [copy(w_ref.at[vocab - tail:vocab], wbuf.at[slot, 0:tail], wsem.at[slot]),
                copy(w_ref.at[0:chunk - tail], wbuf.at[slot, tail:chunk], wsem.at[slot])]

    def wwait(i):
        slot = lax.rem(i, slots)
        copy(w_ref.at[0:chunk], wbuf.at[slot], wsem.at[slot]).wait()

    def qcopy(i):
        at = pl.ds(pl.multiple_of(i * qrows, qrows), qrows)
        return copy(q_ref.at[at], qv_ref.at[at], qsem.at[i])

    def hcopy(i):
        at = pl.ds(pl.multiple_of(i * seqs, seqs), seqs)
        return copy(h_ref.at[at], hbuf.at[at], hsem.at[i])

    small = [copy(src, dst, gsem.at[i])
             for i, (src, dst) in enumerate(((g_ref, gbuf), (t_ref, tbuf)))]
    for c in small:
        c.start()
    for i in range(rows // seqs):
        hcopy(i).start()
    for p in range(4):
        wfirst(p).start()
    for i in range(1, 3):
        wcopy(i).start()

    m[...] = jnp.full(m.shape, NEG, F32)
    sm[...] = jnp.zeros(sm.shape, F32)
    for c in small:
        c.wait()
    lane = lax.broadcasted_iota(jnp.int32, (8, LANES), 1)
    t = tbuf[...]
    spread = jnp.where(eye(), jnp.broadcast_to(jnp.concatenate([t, t], axis=1), (LANES, LANES)), 0.0)
    tcol = jnp.sum(spread, axis=1, keepdims=True)
    scale_ref[...] = jnp.broadcast_to(LOG2E / tcol[:seqs], (seqs, LANES))

    @pl.loop(0, rows // seqs)
    def _(i):
        hcopy(i).wait()
        for b in range(0, seqs, 16):
            at = pl.ds(pl.multiple_of(i * seqs + b, 16), 16)
            h = hbuf[at, :].astype(F32)
            r = lax.rsqrt(jnp.mean(h * h, axis=1, keepdims=True) + 1e-5)
            rinv[at, :] = jnp.broadcast_to(r, (16, LANES))

    def normalise(k):
        for b in range(0, rows, 16):
            r = rinv[b:b + 16, :]
            for c in range(k * half, (k + 1) * half, LANES):
                h = hbuf[b:b + 16, c:c + LANES].astype(F32)
                x[b // 16, c // LANES] = (h * r * gbuf[:, c:c + LANES]).astype(jnp.bfloat16)

    def push(i, k):
        slot = lax.rem(i, slots)
        cols = slice(k * half, (k + 1) * half)
        for u in range(2):
            pltpu.matmul_push_rhs(wbuf[slot, u * half:(u + 1) * half, cols], k % 2, u, transpose=True)

    def run(*refs):
        accs = [[refs[(2 * u + v) * groups:(2 * u + v + 1) * groups] for v in range(2)] for u in range(2)]

        def stats(i, side, b, size=chunk, valid=chunk):
            base = pl.multiple_of(i * chunk, chunk)
            zs = [pltpu.matmul_pop(accs[u][side][b]) for u in range(2)]
            for o in (0, 8):
                row = b * 16 + o
                r8 = slice(row, row + 8)
                scale = scale_ref[row % seqs:row % seqs + 8, :]
                parts = []
                for c in range(0, size, LANES):
                    z = zs[c // half][o:o + 8, c % half:c % half + LANES]
                    if c + LANES > valid:
                        z = jnp.where(lane < valid - c, z, NEG)
                    parts.append(z)
                    if row < draft_rows:
                        s_ref[r8, pl.ds(base + c, LANES)] = z
                old = m[r8, :]
                new = old
                for z in parts:
                    new = jnp.maximum(new, z)
                tot = sm[r8, :] * jnp.exp2((old - new) * scale)
                for z in parts:
                    tot = tot + jnp.exp2((z - new) * scale)
                m[r8, :] = new
                sm[r8, :] = tot

        def matmul(i, side, last=False, first=False):
            for k in range(ktiles):
                if first:
                    normalise(k)
                if k + 1 < ktiles:
                    if first and (k + 1) % (ktiles // 4) == 0:
                        wfirst((k + 1) // (ktiles // 4)).wait()
                    push(i, k + 1)
                elif not last:
                    wwait(i + 1)
                    push(i + 1, 0)
                for b in range(groups):
                    lhs = jnp.concatenate([x[b, k * half // LANES + c] for c in range(half // LANES)], axis=1)
                    for u in range(2):
                        pltpu.matmul_acc_lhs(accs[u][side][b], lhs, load_staged_rhs=k % 2 if b == 0 else None)
                    done = k * groups + b
                    if not first and done % ktiles == ktiles - 1:
                        stats(i - 1, 1 - side, done // ktiles)

        pairs = (n - 2) // 2
        wfirst(0).wait()
        push(0, 0)
        wcopy(3).start()
        matmul(0, 0, first=True)

        @pl.loop(0, pairs)
        def _(k):
            i = 2 * k + 1

            @pl.when(k < pairs - 1)
            def _():
                wcopy(i + 3).start()
                qcopy(2 * k).start()
                qcopy(2 * k + 1).start()

            matmul(i, 1)

            @pl.when(k < pairs - 2)
            def _():
                wcopy(i + 4).start()

            @pl.when(k == pairs - 2)
            def _():
                for c in wlast():
                    c.start()

            matmul(i + 1, 0)

        for i in range(draft_rows // qrows):
            qcopy(i).wait()
        matmul(n - 1, 1, True)
        for b in range(groups):
            stats(n - 1, 1, b, pl.cdiv(tail, LANES) * LANES, tail)

    pl.run_scoped(run, *(pltpu.ACC(u)((16, half), F32) for u in range(2) for _ in range(2 * groups)))

    lse_ref[...] = jnp.zeros(lse_ref.shape, F32)
    for i in range(pl.cdiv(rows, LANES)):
        size = min(LANES, rows - i * LANES)
        r = slice(i * LANES, i * LANES + size)
        ml = m[r, :]
        mrow = jnp.max(ml, axis=1, keepdims=True)
        scale = jnp.concatenate([scale_ref[...]] * (size // seqs), axis=0)
        srow = jnp.sum(sm[r, :] * jnp.exp2((ml - mrow) * scale), axis=1, keepdims=True)
        lse = mrow * (scale * (1.0 / LOG2E)) + jnp.log(srow)
        if i * LANES < draft_rows:
            mrow_ref[r, :] = jnp.broadcast_to(mrow, (size, LANES))
        mask = eye()[:size]
        lse_ref[i:i + 1, :] = jnp.sum(jnp.where(mask, lse, 0.0), axis=0, keepdims=True)


def verify_kernel(dims, s_ref, q_ref, mrow_ref, lse_ref, scale_ref, dt_ref, lcol_ref, ncol_ref, out_ref,
                  e_ref, ccol_ref, g1, g2, msg2, acc, at_ref, tok, send1, recv1, send2, recv2):
    tp, draft_rows, seqs, vocab = dims
    blocks = draft_rows // LANES
    me = lax.axis_index("tp")
    full = vocab // LANES * LANES
    rest = vocab - full

    barrier = pltpu.get_barrier_semaphore()
    for d in range(1, tp):
        pl.semaphore_signal(barrier, inc=1, device_id={"tp": lax.rem(me + d, tp)},
                            device_id_type=pl.DeviceIdType.MESH)
    pl.semaphore_wait(barrier, tp - 1)

    def exchange(src, gather, send, recv):
        def copy(slot, sem, d):
            return pltpu.make_async_remote_copy(
                src_ref=src, dst_ref=gather.at[slot], send_sem=send.at[d], recv_sem=recv.at[sem],
                device_id={"tp": lax.rem(me + d, tp)}, device_id_type=pl.DeviceIdType.MESH)

        def start():
            for d in range(1, tp):
                copy(me, me, d).start()
            gather[me] = src[...]

        def wait():
            for d in range(1, tp):
                peer = lax.rem(me + d, tp)
                copy(peer, peer, d).wait_recv()

        def drain():
            for d in range(1, tp):
                copy(me, me, d).wait_send()

        return start, wait, drain

    start1, wait1, drain1 = exchange(lse_ref, g1, send1, recv1)
    start2, wait2, drain2 = exchange(msg2, g2, send2, recv2)
    start1()

    offset = me * vocab
    for i in range(blocks):
        ids = jnp.concatenate([dt_ref[2 * i:2 * i + 1, :], dt_ref[2 * i + 1:2 * i + 2, :]], axis=1)
        tok[i * LANES:(i + 1) * LANES, :] = to_column((ids - offset).astype(F32))
    lane = lax.broadcasted_iota(jnp.int32, (8, LANES), 1).astype(F32)
    acc[...] = jnp.zeros(acc.shape, F32)
    at_ref[...] = jnp.zeros(at_ref.shape, F32)

    @pl.loop(0, draft_rows // 8)
    def _(b):
        r8 = pl.ds(pl.multiple_of(b * 8, 8), 8)
        mr = mrow_ref[r8, :]
        scale = scale_ref[pl.ds(pl.multiple_of(lax.rem(b * 8, seqs), 8), 8), :]
        away = tok[r8, :] - lane
        zr = s_ref[r8, full:full + rest]
        e_ref[r8, full:full + rest] = jnp.exp2((zr - mr[:, :rest]) * scale[:, :rest])
        hit = away[:, :rest] == float(full)
        at_ref[0, r8, 0:rest] = jnp.where(hit, zr, 0.0)
        at_ref[1, r8, 0:rest] = jnp.where(hit, q_ref[r8, full:full + rest], 0.0)
        az, aq = at_ref[0, r8, :], at_ref[1, r8, :]
        for c in range(0, full, LANES):
            z = s_ref[r8, c:c + LANES]
            e_ref[r8, c:c + LANES] = jnp.exp2((z - mr) * scale)
            hit = away == float(c)
            az = jnp.where(hit, z, az)
            aq = jnp.where(hit, q_ref[r8, c:c + LANES], aq)
        at_ref[0, r8, :] = az
        at_ref[1, r8, :] = aq

    wait1()
    parts = g1[...]
    top = jnp.max(parts, axis=0)
    lse = top + jnp.log(jnp.sum(jnp.exp(parts - top[None]), axis=0))
    out_ref[...] = jnp.zeros(out_ref.shape, F32)
    out_ref[0:4, :] = lse
    for i in range(blocks):
        r = slice(i * LANES, (i + 1) * LANES)
        scale = jnp.concatenate([scale_ref[...]] * (LANES // seqs), axis=0)
        lcol = to_column(lse[i:i + 1, :]) * (LOG2E / scale)
        lcol_ref[r, :] = lcol
        ccol_ref[r, :] = jnp.exp2((mrow_ref[r, :] - lcol) * scale)

    @pl.loop(0, draft_rows // 8)
    def _(b):
        r8 = pl.ds(pl.multiple_of(b * 8, 8), 8)
        cc = ccol_ref[r8, :]
        er = e_ref[r8, full:full + rest]
        acc[r8, 0:rest] = jnp.maximum(er * cc[:, :rest] - q_ref[r8, full:full + rest], 0.0)
        sums = [acc[r8, :]] + [jnp.zeros((8, LANES), F32)] * 3
        for k, c in enumerate(range(0, full, LANES)):
            sums[k % 4] += jnp.maximum(e_ref[r8, c:c + LANES] * cc - q_ref[r8, c:c + LANES], 0.0)
        acc[r8, :] = (sums[0] + sums[1]) + (sums[2] + sums[3])

    msg2[...] = jnp.zeros(msg2.shape, F32)
    for i in range(blocks):
        r = slice(i * LANES, (i + 1) * LANES)
        total = jnp.sum(acc[r, :], axis=1, keepdims=True)
        msg2[i:i + 1, :] = to_lanes(jnp.broadcast_to(total, (LANES, LANES)))
        scale = jnp.concatenate([scale_ref[:, 0:1]] * (LANES // seqs), axis=0)
        p = jnp.exp2((jnp.sum(at_ref[0, r, :], axis=1, keepdims=True) - lcol_ref[r, 0:1]) * scale)
        qt = jnp.sum(at_ref[1, r, :], axis=1, keepdims=True)
        ok = jnp.where(qt > 0.0, jnp.minimum(1.0, p / jnp.where(qt > 0.0, qt, 1.0)), 0.0)
        msg2[4 + i:5 + i, :] = to_lanes(jnp.broadcast_to(ok, (LANES, LANES)))
    start2()
    wait2()
    sums = jnp.sum(g2[...], axis=0)
    out_ref[4:4 + 8, :] = sums
    for i in range(blocks):
        ncol_ref[i * LANES:(i + 1) * LANES, :] = to_column(1.0 / sums[i:i + 1, :])
    drain1()
    drain2()


def residual_kernel(dims, s_ref, q_ref, lcol_ref, ncol_ref, scale_ref, small_ref, res_ref, acc_ref, norm_ref, bonus_ref,
                    stage, sem):
    draft_rows, seqs, vocab, block, slots = dims
    n = draft_rows // block
    full = vocab // LANES * LANES
    rest = vocab - full

    def copy(i):
        slot = lax.rem(i, slots)
        return pltpu.make_async_copy(stage.at[slot], res_ref.at[pl.ds(pl.multiple_of(i * block, block), block)],
                                     sem.at[slot])

    @pl.loop(0, n)
    def _(i):
        slot = lax.rem(i, slots)

        for b in range(block // 8):
            src = pl.ds(pl.multiple_of(i * block + b * 8, 8), 8)
            dst = slice(b * 8, b * 8 + 8)
            lc, inv = lcol_ref[src, :], ncol_ref[src, :]
            scale = scale_ref[pl.ds(pl.multiple_of(lax.rem(i * block + b * 8, seqs), 8), 8), :]
            for c in range(0, full, LANES):
                stage[slot, dst, c:c + LANES] = (
                    jnp.maximum(jnp.exp2((s_ref[src, c:c + LANES] - lc) * scale) - q_ref[src, c:c + LANES], 0.0) * inv)
            stage[slot, dst, full:full + rest] = (
                jnp.maximum(jnp.exp2((s_ref[src, full:full + rest] - lc[:, :rest]) * scale[:, :rest])
                            - q_ref[src, full:full + rest], 0.0)
                * inv[:, :rest])
        copy(i).start()

    for j in range(draft_rows // seqs):
        i, off = j // 2, (j % 2) * seqs
        norm_ref[j:j + 1, :] = small_ref[4 + i:5 + i, off:off + seqs]
        acc_ref[j:j + 1, :] = small_ref[8 + i:9 + i, off:off + seqs]
    bonus_ref[...] = small_ref[3:4, 0:seqs]

    for i in range(n - slots, n):
        copy(i).wait()


def solution(mesh):
    tp = mesh.shape["tp"]
    vmem, hbm = pltpu.VMEM, pltpu.HBM

    def spec(space):
        return pl.BlockSpec(memory_space=space)

    def local_step(hidden, norm_gain, w_head, draft_probs, draft_tokens, temperature):
        seqs, positions, depth = hidden.shape
        drafts, vocab = draft_probs.shape[1:]
        rows, draft_rows = seqs * positions, seqs * drafts
        wide = pl.cdiv(vocab, LANES) * LANES
        h = hidden.transpose(1, 0, 2).reshape(rows, depth)
        w = w_head.T
        q = draft_probs.transpose(1, 0, 2).reshape(draft_rows, vocab)
        dt = draft_tokens.T
        chunk, slots, qrows = 512, 4, 32
        dims = (rows, draft_rows, seqs, depth, vocab, chunk, slots, qrows)
        s, qv, mrow, lse, scale = pl.pallas_call(
            functools.partial(head_kernel, dims),
            out_shape=(pltpu.VMEM((draft_rows, wide), F32), pltpu.VMEM((draft_rows, vocab), F32),
                       pltpu.VMEM((draft_rows, LANES), F32), pltpu.VMEM((4, LANES), F32),
                       pltpu.VMEM((seqs, LANES), F32)),
            in_specs=[spec(hbm)] * 5,
            out_specs=(spec(vmem),) * 5,
            scratch_shapes=[
                pltpu.VMEM((rows, depth), jnp.bfloat16), pltpu.VMEM((1, depth), F32), pltpu.VMEM((1, seqs), F32),
                pltpu.VMEM((rows // 16, depth // LANES, 16, LANES), jnp.bfloat16),
                pltpu.VMEM((slots, chunk, depth), jnp.bfloat16),
                pltpu.VMEM((rows, LANES), F32), pltpu.VMEM((rows, LANES), F32),
                pltpu.VMEM((rows, LANES), F32),
                pltpu.SemaphoreType.DMA((positions,)), pltpu.SemaphoreType.DMA((2,)), pltpu.SemaphoreType.DMA((4,)),
                pltpu.SemaphoreType.DMA((slots,)), pltpu.SemaphoreType.DMA((draft_rows // qrows,)),
            ],
            compiler_params=pltpu.CompilerParams(vmem_limit_bytes=24 * MIB),
        )(*(pltpu.with_memory_space_constraint(a, hbm)
            for a in (h, norm_gain.reshape(1, depth), w, q, temperature.reshape(1, seqs))))

        lcol, ncol, small = pl.pallas_call(
            functools.partial(verify_kernel, (tp, draft_rows, seqs, vocab)),
            out_shape=(pltpu.VMEM((draft_rows, LANES), F32), pltpu.VMEM((draft_rows, LANES), F32),
                       pltpu.VMEM((16, LANES), F32)),
            in_specs=[spec(vmem)] * 6,
            out_specs=(spec(vmem),) * 3,
            scratch_shapes=[
                pltpu.VMEM((draft_rows, wide), F32), pltpu.VMEM((draft_rows, LANES), F32),
                pltpu.VMEM((tp, 4, LANES), F32), pltpu.VMEM((tp, 8, LANES), F32), pltpu.VMEM((8, LANES), F32),
                pltpu.VMEM((draft_rows, LANES), F32), pltpu.VMEM((2, draft_rows, LANES), F32),
                pltpu.VMEM((draft_rows, LANES), F32),
            ] + [pltpu.SemaphoreType.DMA((tp,))] * 4,
            compiler_params=pltpu.CompilerParams(vmem_limit_bytes=20 * MIB, collective_id=0, has_side_effects=True),
        )(s, qv, mrow, lse, scale, dt)

        block = 16
        stages = draft_rows // block
        res, acc, norm, bonus = pl.pallas_call(
            functools.partial(residual_kernel, (draft_rows, seqs, vocab, block, stages)),
            out_shape=(jax.ShapeDtypeStruct((draft_rows, vocab), F32), jax.ShapeDtypeStruct((drafts, seqs), F32),
                       jax.ShapeDtypeStruct((drafts, seqs), F32), jax.ShapeDtypeStruct((1, seqs), F32)),
            in_specs=[spec(vmem)] * 6,
            out_specs=(spec(hbm), spec(vmem), spec(vmem), spec(vmem)),
            scratch_shapes=[pltpu.VMEM((stages, block, vocab), F32), pltpu.SemaphoreType.DMA((stages,))],
            compiler_params=pltpu.CompilerParams(vmem_limit_bytes=16 * MIB),
        )(s, qv, lcol, ncol, scale, small)
        res = res.reshape(drafts, seqs, vocab).transpose(1, 0, 2)
        return acc.T, norm.T, res, bonus.reshape(seqs)

    return jax.shard_map(
        local_step,
        mesh=mesh,
        in_specs=(P('dp', None, None), P(), P(None, 'tp'), P('dp', None, 'tp'), P('dp', None), P('dp')),
        out_specs=(P('dp', None), P('dp', None), P('dp', None, 'tp'), P('dp')),
        check_vma=False,
    )
```

```python
import functools

import jax
import jax.numpy as jnp
from jax import lax
from jax.experimental import pallas as pl
from jax.experimental.pallas import tpu as pltpu
from jax.sharding import PartitionSpec as P

F32 = jnp.float32
LANES = 128
NEG = -3.0e38
LOG2E = 1.4426950408889634
MIB = 1024 * 1024


def eye():
    rows = lax.broadcasted_iota(jnp.int32, (LANES, LANES), 0)
    return rows == lax.broadcasted_iota(jnp.int32, (LANES, LANES), 1)


def to_lanes(column):
    return jnp.sum(jnp.where(eye(), column, 0.0), axis=0, keepdims=True)


def to_column(row):
    col = jnp.sum(jnp.where(eye(), jnp.broadcast_to(row, (LANES, LANES)), 0.0), axis=1, keepdims=True)
    return jnp.broadcast_to(col, (LANES, LANES))


def head_kernel(dims, h_ref, g_ref, w_ref, q_ref, t_ref, s_ref, qv_ref, mrow_ref, lse_ref, scale_ref,
                hbuf, gbuf, tbuf, x, wbuf, m, sm, rinv, hsem, gsem, fsem, wsem, qsem):
    rows, draft_rows, seqs, depth, vocab, chunk, slots, qrows = dims
    n = pl.cdiv(vocab, chunk)
    tail = vocab - (n - 1) * chunk
    half = chunk // 2
    ktiles = depth // half
    groups = rows // 16
    copy = pltpu.make_async_copy

    def wcopy(i):
        slot = lax.rem(i, slots)
        at = pl.ds(pl.multiple_of(i * chunk, chunk), chunk)
        return copy(w_ref.at[at], wbuf.at[slot], wsem.at[slot])

    def wfirst(p):
        cols = slice(p * depth // 4, (p + 1) * depth // 4)
        return copy(w_ref.at[0:chunk, cols], wbuf.at[0, :, cols], fsem.at[p])

    def wlast():
        slot = (n - 1) % slots
        return [copy(w_ref.at[vocab - tail:vocab], wbuf.at[slot, 0:tail], wsem.at[slot]),
                copy(w_ref.at[0:chunk - tail], wbuf.at[slot, tail:chunk], wsem.at[slot])]

    def wwait(i):
        slot = lax.rem(i, slots)
        copy(w_ref.at[0:chunk], wbuf.at[slot], wsem.at[slot]).wait()

    def qcopy(i):
        at = pl.ds(pl.multiple_of(i * qrows, qrows), qrows)
        return copy(q_ref.at[at], qv_ref.at[at], qsem.at[i])

    def hcopy(i):
        at = pl.ds(pl.multiple_of(i * seqs, seqs), seqs)
        return copy(h_ref.at[at], hbuf.at[at], hsem.at[i])

    small = [copy(src, dst, gsem.at[i])
             for i, (src, dst) in enumerate(((g_ref, gbuf), (t_ref, tbuf)))]
    for c in small:
        c.start()
    for i in range(rows // seqs):
        hcopy(i).start()
    wfirst(0).start()

    m[...] = jnp.full(m.shape, NEG, F32)
    sm[...] = jnp.zeros(sm.shape, F32)
    for c in small:
        c.wait()
    lane = lax.broadcasted_iota(jnp.int32, (8, LANES), 1)
    t = tbuf[...]
    spread = jnp.where(eye(), jnp.broadcast_to(jnp.concatenate([t, t], axis=1), (LANES, LANES)), 0.0)
    tcol = jnp.sum(spread, axis=1, keepdims=True)
    scale_ref[...] = jnp.broadcast_to(LOG2E / tcol[:seqs], (seqs, LANES))

    for i in range(rows // seqs):
        hcopy(i).wait()
        if i % 2 == 0 and i > 0:
            wfirst(i // 2).start()
        for b in range(i * seqs, (i + 1) * seqs, 16):
            h = hbuf[b:b + 16, :].astype(F32)
            r = lax.rsqrt(jnp.mean(h * h, axis=1, keepdims=True) + 1e-5)
            rinv[b:b + 16, :] = jnp.broadcast_to(r, (16, LANES))

    def normalise(k):
        for b in range(0, rows, 16):
            r = rinv[b:b + 16, :]
            for c in range(k * half, (k + 1) * half, LANES):
                h = hbuf[b:b + 16, c:c + LANES].astype(F32)
                x[b // 16, c // LANES] = (h * r * gbuf[:, c:c + LANES]).astype(jnp.bfloat16)

    def push(i, k):
        slot = lax.rem(i, slots)
        cols = slice(k * half, (k + 1) * half)
        for u in range(2):
            pltpu.matmul_push_rhs(wbuf[slot, u * half:(u + 1) * half, cols], k % 2, u, transpose=True)

    def run(*refs):
        accs = [[refs[(2 * u + v) * groups:(2 * u + v + 1) * groups] for v in range(2)] for u in range(2)]

        def stats(i, side, b, size=chunk, valid=chunk):
            base = pl.multiple_of(i * chunk, chunk)
            zs = [pltpu.matmul_pop(accs[u][side][b]) for u in range(2)]
            for o in (0, 8):
                row = b * 16 + o
                r8 = slice(row, row + 8)
                scale = scale_ref[row % seqs:row % seqs + 8, :]
                parts = []
                for c in range(0, size, LANES):
                    z = zs[c // half][o:o + 8, c % half:c % half + LANES]
                    if c + LANES > valid:
                        z = jnp.where(lane < valid - c, z, NEG)
                    parts.append(z)
                    if row < draft_rows:
                        s_ref[r8, pl.ds(base + c, LANES)] = z
                old = m[r8, :]
                new = old
                for z in parts:
                    new = jnp.maximum(new, z)
                tot = sm[r8, :] * jnp.exp2((old - new) * scale)
                for z in parts:
                    tot = tot + jnp.exp2((z - new) * scale)
                m[r8, :] = new
                sm[r8, :] = tot

        def matmul(i, side, last=False, first=False):
            for k in range(ktiles):
                if first:
                    normalise(k)
                    if k in (4, 8):
                        wcopy(1 + k // 4).start()
                if k + 1 < ktiles:
                    if first and (k + 1) % (ktiles // 4) == 0:
                        wfirst((k + 1) // (ktiles // 4)).wait()
                    push(i, k + 1)
                elif not last:
                    wwait(i + 1)
                    push(i + 1, 0)
                for b in range(groups):
                    lhs = jnp.concatenate([x[b, k * half // LANES + c] for c in range(half // LANES)], axis=1)
                    for u in range(2):
                        pltpu.matmul_acc_lhs(accs[u][side][b], lhs, load_staged_rhs=k % 2 if b == 0 else None)
                    done = k * groups + b
                    if not first and done % ktiles == ktiles - 1:
                        stats(i - 1, 1 - side, done // ktiles)

        pairs = (n - 2) // 2
        wfirst(0).wait()
        push(0, 0)
        wcopy(1).start()
        matmul(0, 0, first=True)

        @pl.loop(0, pairs)
        def _(k):
            i = 2 * k + 1

            @pl.when(k < pairs - 1)
            def _():
                wcopy(i + 3).start()
                qcopy(2 * k).start()
                qcopy(2 * k + 1).start()

            matmul(i, 1)

            @pl.when(k < pairs - 2)
            def _():
                wcopy(i + 4).start()

            @pl.when(k == pairs - 2)
            def _():
                for c in wlast():
                    c.start()

            matmul(i + 1, 0)

        for i in range(draft_rows // qrows):
            qcopy(i).wait()
        matmul(n - 1, 1, True)
        for b in range(groups):
            stats(n - 1, 1, b, pl.cdiv(tail, LANES) * LANES, tail)

    pl.run_scoped(run, *(pltpu.ACC(u)((16, half), F32) for u in range(2) for _ in range(2 * groups)))

    lse_ref[...] = jnp.zeros(lse_ref.shape, F32)
    for i in range(pl.cdiv(rows, LANES)):
        size = min(LANES, rows - i * LANES)
        r = slice(i * LANES, i * LANES + size)
        ml = m[r, :]
        mrow = jnp.max(ml, axis=1, keepdims=True)
        scale = jnp.concatenate([scale_ref[...]] * (size // seqs), axis=0)
        srow = jnp.sum(sm[r, :] * jnp.exp2((ml - mrow) * scale), axis=1, keepdims=True)
        lse = mrow * (scale * (1.0 / LOG2E)) + jnp.log(srow)
        if i * LANES < draft_rows:
            mrow_ref[r, :] = jnp.broadcast_to(mrow, (size, LANES))
        mask = eye()[:size]
        lse_ref[i:i + 1, :] = jnp.sum(jnp.where(mask, lse, 0.0), axis=0, keepdims=True)


def verify_kernel(dims, s_ref, q_ref, mrow_ref, lse_ref, scale_ref, dt_ref, lcol_ref, ncol_ref, out_ref,
                  e_ref, ccol_ref, g1, g2, g3, msg2, msg3, acc, at_ref, tok, send1, recv1, send2, recv2, send3, recv3):
    tp, draft_rows, seqs, vocab = dims
    blocks = draft_rows // LANES
    me = lax.axis_index("tp")
    full = vocab // LANES * LANES
    rest = vocab - full

    barrier = pltpu.get_barrier_semaphore()
    for d in range(1, tp):
        pl.semaphore_signal(barrier, inc=1, device_id={"tp": lax.rem(me + d, tp)},
                            device_id_type=pl.DeviceIdType.MESH)
    pl.semaphore_wait(barrier, tp - 1)

    def exchange(src, gather, send, recv):
        def copy(slot, sem, d):
            return pltpu.make_async_remote_copy(
                src_ref=src, dst_ref=gather.at[slot], send_sem=send.at[d], recv_sem=recv.at[sem],
                device_id={"tp": lax.rem(me + d, tp)}, device_id_type=pl.DeviceIdType.MESH)

        def start():
            for d in range(1, tp):
                copy(me, me, d).start()
            gather[me] = src[...]

        def wait():
            for d in range(1, tp):
                peer = lax.rem(me + d, tp)
                copy(peer, peer, d).wait_recv()

        def drain():
            for d in range(1, tp):
                copy(me, me, d).wait_send()

        return start, wait, drain

    start1, wait1, drain1 = exchange(lse_ref, g1, send1, recv1)
    start2, wait2, drain2 = exchange(msg2, g2, send2, recv2)
    start3, wait3, drain3 = exchange(msg3, g3, send3, recv3)
    start1()

    offset = me * vocab
    for i in range(blocks):
        ids = jnp.concatenate([dt_ref[2 * i:2 * i + 1, :], dt_ref[2 * i + 1:2 * i + 2, :]], axis=1)
        tok[i * LANES:(i + 1) * LANES, :] = to_column((ids - offset).astype(F32))
    lane = lax.broadcasted_iota(jnp.int32, (8, LANES), 1).astype(F32)
    acc[...] = jnp.zeros(acc.shape, F32)
    at_ref[...] = jnp.zeros(at_ref.shape, F32)

    @pl.loop(0, draft_rows // 8)
    def _(b):
        r8 = pl.ds(pl.multiple_of(b * 8, 8), 8)
        mr = mrow_ref[r8, :]
        scale = scale_ref[pl.ds(pl.multiple_of(lax.rem(b * 8, seqs), 8), 8), :]
        away = tok[r8, :] - lane
        zr = s_ref[r8, full:full + rest]
        e_ref[r8, full:full + rest] = jnp.exp2((zr - mr[:, :rest]) * scale[:, :rest])
        hit = away[:, :rest] == float(full)
        at_ref[0, r8, 0:rest] = jnp.where(hit, zr, 0.0)
        at_ref[1, r8, 0:rest] = jnp.where(hit, q_ref[r8, full:full + rest], 0.0)
        az, aq = at_ref[0, r8, :], at_ref[1, r8, :]
        for c in range(0, full, LANES):
            z = s_ref[r8, c:c + LANES]
            e_ref[r8, c:c + LANES] = jnp.exp2((z - mr) * scale)
            hit = away == float(c)
            az = jnp.where(hit, z, az)
            aq = jnp.where(hit, q_ref[r8, c:c + LANES], aq)
        at_ref[0, r8, :] = az
        at_ref[1, r8, :] = aq

    msg3[...] = jnp.zeros(msg3.shape, F32)
    for i in range(blocks):
        r = slice(i * LANES, (i + 1) * LANES)
        for part in range(2):
            value = jnp.sum(at_ref[part, r, :], axis=1, keepdims=True)
            msg3[4 * part + i:4 * part + i + 1, :] = to_lanes(jnp.broadcast_to(value, (LANES, LANES)))
    start3()
    wait1()
    parts = g1[...]
    top = jnp.max(parts, axis=0)
    lse = top + jnp.log(jnp.sum(jnp.exp(parts - top[None]), axis=0))
    out_ref[...] = jnp.zeros(out_ref.shape, F32)
    out_ref[0:4, :] = lse
    for i in range(blocks):
        r = slice(i * LANES, (i + 1) * LANES)
        scale = jnp.concatenate([scale_ref[...]] * (LANES // seqs), axis=0)
        lcol = to_column(lse[i:i + 1, :]) * (LOG2E / scale)
        lcol_ref[r, :] = lcol
        ccol_ref[r, :] = jnp.exp2((mrow_ref[r, :] - lcol) * scale)

    @pl.loop(0, draft_rows // 8)
    def _(b):
        r8 = pl.ds(pl.multiple_of(b * 8, 8), 8)
        cc = ccol_ref[r8, :]
        er = e_ref[r8, full:full + rest]
        acc[r8, 0:rest] = jnp.maximum(er * cc[:, :rest] - q_ref[r8, full:full + rest], 0.0)
        sums = [acc[r8, :]] + [jnp.zeros((8, LANES), F32)] * 3
        for k, c in enumerate(range(0, full, LANES)):
            sums[k % 4] += jnp.maximum(e_ref[r8, c:c + LANES] * cc - q_ref[r8, c:c + LANES], 0.0)
        acc[r8, :] = (sums[0] + sums[1]) + (sums[2] + sums[3])

    msg2[...] = jnp.zeros(msg2.shape, F32)
    for i in range(blocks):
        total = jnp.sum(acc[i * LANES:(i + 1) * LANES, :], axis=1, keepdims=True)
        msg2[i:i + 1, :] = to_lanes(jnp.broadcast_to(total, (LANES, LANES)))
    start2()
    wait3()
    at = jnp.sum(g3[...], axis=0)
    column = jnp.concatenate([scale_ref[...]] * (LANES // seqs), axis=0)
    scale = to_lanes(column)
    p = jnp.exp2((at[0:4] - lse * (LOG2E / scale)) * scale)
    out_ref[8:12, :] = jnp.minimum(1.0, p / at[4:8])
    wait2()
    sums = jnp.sum(g2[...], axis=0)
    out_ref[4:8, :] = sums
    for i in range(blocks):
        ncol_ref[i * LANES:(i + 1) * LANES, :] = to_column(1.0 / sums[i:i + 1, :])
    drain1()
    drain2()
    drain3()


def residual_kernel(dims, s_ref, q_ref, lcol_ref, ncol_ref, scale_ref, small_ref, res_ref, acc_ref, norm_ref, bonus_ref,
                    stage, sem):
    draft_rows, seqs, vocab, block, slots = dims
    n = draft_rows // block
    full = vocab // LANES * LANES
    rest = vocab - full

    def copy(i):
        slot = lax.rem(i, slots)
        return pltpu.make_async_copy(stage.at[slot], res_ref.at[pl.ds(pl.multiple_of(i * block, block), block)],
                                     sem.at[slot])

    @pl.loop(0, n)
    def _(i):
        slot = lax.rem(i, slots)

        for b in range(block // 8):
            src = pl.ds(pl.multiple_of(i * block + b * 8, 8), 8)
            dst = slice(b * 8, b * 8 + 8)
            lc, inv = lcol_ref[src, :], ncol_ref[src, :]
            scale = scale_ref[pl.ds(pl.multiple_of(lax.rem(i * block + b * 8, seqs), 8), 8), :]
            for c in range(0, full, LANES):
                stage[slot, dst, c:c + LANES] = (
                    jnp.maximum(jnp.exp2((s_ref[src, c:c + LANES] - lc) * scale) - q_ref[src, c:c + LANES], 0.0) * inv)
            stage[slot, dst, full:full + rest] = (
                jnp.maximum(jnp.exp2((s_ref[src, full:full + rest] - lc[:, :rest]) * scale[:, :rest])
                            - q_ref[src, full:full + rest], 0.0)
                * inv[:, :rest])
        copy(i).start()

    for j in range(draft_rows // seqs):
        i, off = j // 2, (j % 2) * seqs
        norm_ref[j:j + 1, :] = small_ref[4 + i:5 + i, off:off + seqs]
        acc_ref[j:j + 1, :] = small_ref[8 + i:9 + i, off:off + seqs]
    bonus_ref[...] = small_ref[3:4, 0:seqs]

    for i in range(n - slots, n):
        copy(i).wait()


def solution(mesh):
    tp = mesh.shape["tp"]
    vmem, hbm = pltpu.VMEM, pltpu.HBM

    def spec(space):
        return pl.BlockSpec(memory_space=space)

    def local_step(hidden, norm_gain, w_head, draft_probs, draft_tokens, temperature):
        seqs, positions, depth = hidden.shape
        drafts, vocab = draft_probs.shape[1:]
        rows, draft_rows = seqs * positions, seqs * drafts
        wide = pl.cdiv(vocab, LANES) * LANES
        h = hidden.transpose(1, 0, 2).reshape(rows, depth)
        w = w_head.T
        q = draft_probs.transpose(1, 0, 2).reshape(draft_rows, vocab)
        dt = draft_tokens.T
        chunk, slots, qrows = 512, 4, 32
        dims = (rows, draft_rows, seqs, depth, vocab, chunk, slots, qrows)
        s, qv, mrow, lse, scale = pl.pallas_call(
            functools.partial(head_kernel, dims),
            out_shape=(pltpu.VMEM((draft_rows, wide), F32), pltpu.VMEM((draft_rows, vocab), F32),
                       pltpu.VMEM((draft_rows, LANES), F32), pltpu.VMEM((4, LANES), F32),
                       pltpu.VMEM((seqs, LANES), F32)),
            in_specs=[spec(hbm)] * 5,
            out_specs=(spec(vmem),) * 5,
            scratch_shapes=[
                pltpu.VMEM((rows, depth), jnp.bfloat16), pltpu.VMEM((1, depth), F32), pltpu.VMEM((1, seqs), F32),
                pltpu.VMEM((rows // 16, depth // LANES, 16, LANES), jnp.bfloat16),
                pltpu.VMEM((slots, chunk, depth), jnp.bfloat16),
                pltpu.VMEM((rows, LANES), F32), pltpu.VMEM((rows, LANES), F32),
                pltpu.VMEM((rows, LANES), F32),
                pltpu.SemaphoreType.DMA((positions,)), pltpu.SemaphoreType.DMA((2,)), pltpu.SemaphoreType.DMA((4,)),
                pltpu.SemaphoreType.DMA((slots,)), pltpu.SemaphoreType.DMA((draft_rows // qrows,)),
            ],
            compiler_params=pltpu.CompilerParams(vmem_limit_bytes=24 * MIB),
        )(*(pltpu.with_memory_space_constraint(a, hbm)
            for a in (h, norm_gain.reshape(1, depth), w, q, temperature.reshape(1, seqs))))

        lcol, ncol, small = pl.pallas_call(
            functools.partial(verify_kernel, (tp, draft_rows, seqs, vocab)),
            out_shape=(pltpu.VMEM((draft_rows, LANES), F32), pltpu.VMEM((draft_rows, LANES), F32),
                       pltpu.VMEM((16, LANES), F32)),
            in_specs=[spec(vmem)] * 6,
            out_specs=(spec(vmem),) * 3,
            scratch_shapes=[
                pltpu.VMEM((draft_rows, wide), F32), pltpu.VMEM((draft_rows, LANES), F32),
                pltpu.VMEM((tp, 4, LANES), F32), pltpu.VMEM((tp, 4, LANES), F32), pltpu.VMEM((tp, 8, LANES), F32),
                pltpu.VMEM((4, LANES), F32), pltpu.VMEM((8, LANES), F32),
                pltpu.VMEM((draft_rows, LANES), F32), pltpu.VMEM((2, draft_rows, LANES), F32),
                pltpu.VMEM((draft_rows, LANES), F32),
            ] + [pltpu.SemaphoreType.DMA((tp,))] * 6,
            compiler_params=pltpu.CompilerParams(vmem_limit_bytes=20 * MIB, collective_id=0, has_side_effects=True),
        )(s, qv, mrow, lse, scale, dt)

        block = 16
        stages = draft_rows // block
        res, acc, norm, bonus = pl.pallas_call(
            functools.partial(residual_kernel, (draft_rows, seqs, vocab, block, stages)),
            out_shape=(jax.ShapeDtypeStruct((draft_rows, vocab), F32), jax.ShapeDtypeStruct((drafts, seqs), F32),
                       jax.ShapeDtypeStruct((drafts, seqs), F32), jax.ShapeDtypeStruct((1, seqs), F32)),
            in_specs=[spec(vmem)] * 6,
            out_specs=(spec(hbm), spec(vmem), spec(vmem), spec(vmem)),
            scratch_shapes=[pltpu.VMEM((stages, block, vocab), F32), pltpu.SemaphoreType.DMA((stages,))],
            compiler_params=pltpu.CompilerParams(vmem_limit_bytes=16 * MIB),
        )(s, qv, lcol, ncol, scale, small)
        res = res.reshape(drafts, seqs, vocab).transpose(1, 0, 2)
        return acc.T, norm.T, res, bonus.reshape(seqs)

    return jax.shard_map(
        local_step,
        mesh=mesh,
        in_specs=(P('dp', None, None), P(), P(None, 'tp'), P('dp', None, 'tp'), P('dp', None), P('dp')),
        out_specs=(P('dp', None), P('dp', None), P('dp', None, 'tp'), P('dp')),
        check_vma=False,
    )
```

```python
import functools

import jax
import jax.numpy as jnp
from jax import lax
from jax.experimental import pallas as pl
from jax.experimental.pallas import tpu as pltpu
from jax.sharding import PartitionSpec as P

F32 = jnp.float32
LANES = 128
NEG = -3.0e38
LOG2E = 1.4426950408889634
MIB = 1024 * 1024


def eye():
    rows = lax.broadcasted_iota(jnp.int32, (LANES, LANES), 0)
    return rows == lax.broadcasted_iota(jnp.int32, (LANES, LANES), 1)


def to_lanes(column):
    return jnp.sum(jnp.where(eye(), column, 0.0), axis=0, keepdims=True)


def to_column(row):
    col = jnp.sum(jnp.where(eye(), jnp.broadcast_to(row, (LANES, LANES)), 0.0), axis=1, keepdims=True)
    return jnp.broadcast_to(col, (LANES, LANES))


def head_kernel(dims, h_ref, g_ref, w_ref, q_ref, t_ref, s_ref, qv_ref, scale_ref, x, wend, m, sm,
                hbuf, gbuf, tbuf, wbuf, rinv, hsem, gsem, fsem, wsem, qsem, esem):
    rows, draft_rows, seqs, depth, vocab, chunk, slots, qrows = dims
    n = pl.cdiv(vocab, chunk)
    tail = vocab - (n - 1) * chunk
    half = chunk // 2
    ktiles = depth // half
    groups = rows // 16
    copy = pltpu.make_async_copy

    def wcopy(i):
        slot = lax.rem(i, slots)
        at = pl.ds(pl.multiple_of(i * chunk, chunk), chunk)
        return copy(w_ref.at[at], wbuf.at[slot], wsem.at[slot])

    def wfirst(p):
        cols = slice(p * depth // 4, (p + 1) * depth // 4)
        return copy(w_ref.at[0:chunk, cols], wbuf.at[0, :, cols], fsem.at[p])

    def wlast():
        fill = wend.shape[0] - tail
        return [copy(w_ref.at[vocab - tail:vocab], wend.at[0:tail], esem.at[0]),
                copy(w_ref.at[0:fill], wend.at[tail:tail + fill], esem.at[1])]

    def wwait(i):
        slot = lax.rem(i, slots)
        copy(w_ref.at[0:chunk], wbuf.at[slot], wsem.at[slot]).wait()

    def qcopy(i):
        at = pl.ds(pl.multiple_of(i * qrows, qrows), qrows)
        return copy(q_ref.at[at], qv_ref.at[at], qsem.at[i])

    def hcopy(i):
        at = pl.ds(pl.multiple_of(i * seqs, seqs), seqs)
        return copy(h_ref.at[at], hbuf.at[at], hsem.at[i])

    small = [copy(src, dst, gsem.at[i])
             for i, (src, dst) in enumerate(((g_ref, gbuf), (t_ref, tbuf)))]
    for c in small:
        c.start()
    for i in range(rows // seqs):
        hcopy(i).start()
    wfirst(0).start()

    m[...] = jnp.full(m.shape, NEG, F32)
    sm[...] = jnp.zeros(sm.shape, F32)
    for c in small:
        c.wait()
    lane = lax.broadcasted_iota(jnp.int32, (8, LANES), 1)
    t = tbuf[...]
    spread = jnp.where(eye(), jnp.broadcast_to(jnp.concatenate([t, t], axis=1), (LANES, LANES)), 0.0)
    tcol = jnp.sum(spread, axis=1, keepdims=True)
    scale_ref[...] = jnp.broadcast_to(LOG2E / tcol[:seqs], (seqs, LANES))

    for i in range(rows // seqs):
        hcopy(i).wait()
        if i % 2 == 0 and i > 0:
            wfirst(i // 2).start()
        for b in range(i * seqs, (i + 1) * seqs, 16):
            h = hbuf[b:b + 16, :].astype(F32)
            r = lax.rsqrt(jnp.mean(h * h, axis=1, keepdims=True) + 1e-5)
            rinv[b:b + 16, :] = jnp.broadcast_to(r, (16, LANES))

    def normalise(k):
        for b in range(0, rows, 16):
            r = rinv[b:b + 16, :]
            for c in range(k * half, (k + 1) * half, LANES):
                h = hbuf[b:b + 16, c:c + LANES].astype(F32)
                x[b // 16, c // LANES] = (h * r * gbuf[:, c:c + LANES]).astype(jnp.bfloat16)

    def push(i, k):
        slot = lax.rem(i, slots)
        cols = slice(k * half, (k + 1) * half)
        for u in range(2):
            pltpu.matmul_push_rhs(wbuf[slot, u * half:(u + 1) * half, cols], k % 2, u, transpose=True)

    def run(*refs):
        accs = [[refs[(2 * u + v) * groups:(2 * u + v + 1) * groups] for v in range(2)] for u in range(2)]

        def stats(i, side, b, size=chunk, valid=chunk):
            base = pl.multiple_of(i * chunk, chunk)
            zs = [pltpu.matmul_pop(accs[u][side][b]) for u in range(2)]
            for o in (0, 8):
                row = b * 16 + o
                r8 = slice(row, row + 8)
                scale = scale_ref[row % seqs:row % seqs + 8, :]
                parts = []
                for c in range(0, size, LANES):
                    z = zs[c // half][o:o + 8, c % half:c % half + LANES]
                    if c + LANES > valid:
                        z = jnp.where(lane < valid - c, z, NEG)
                    parts.append(z)
                    if row < draft_rows:
                        s_ref[r8, pl.ds(base + c, LANES)] = z
                old = m[r8, :]
                new = old
                for z in parts:
                    new = jnp.maximum(new, z)
                tot = sm[r8, :] * jnp.exp2((old - new) * scale)
                for z in parts:
                    tot = tot + jnp.exp2((z - new) * scale)
                m[r8, :] = new
                sm[r8, :] = tot

        def matmul(i, side, last=False, first=False):
            for k in range(ktiles):
                if first:
                    normalise(k)
                    if k in (4, 8):
                        wcopy(1 + k // 4).start()
                if k + 1 < ktiles:
                    if first and (k + 1) % (ktiles // 4) == 0:
                        wfirst((k + 1) // (ktiles // 4)).wait()
                    push(i, k + 1)
                elif not last:
                    wwait(i + 1)
                    push(i + 1, 0)
                for b in range(groups):
                    lhs = jnp.concatenate([x[b, k * half // LANES + c] for c in range(half // LANES)], axis=1)
                    for u in range(2):
                        pltpu.matmul_acc_lhs(accs[u][side][b], lhs, load_staged_rhs=k % 2 if b == 0 else None)
                    done = k * groups + b
                    if not first and done % ktiles == ktiles - 1:
                        stats(i - 1, 1 - side, done // ktiles)

        pairs = (n - 2) // 2
        wfirst(0).wait()
        push(0, 0)
        wcopy(1).start()
        matmul(0, 0, first=True)

        @pl.loop(0, pairs - 1)
        def _(k):
            i = 2 * k + 1
            wcopy(i + 3).start()
            qcopy(2 * k).start()
            qcopy(2 * k + 1).start()
            matmul(i, 1)

            @pl.when(k < pairs - 2)
            def _():
                wcopy(i + 4).start()

            @pl.when(k == pairs - 2)
            def _():
                for c in wlast():
                    c.start()

            matmul(i + 1, 0)

        matmul(n - 3, 1)
        matmul(n - 2, 0, True)
        for b in range(groups):
            stats(n - 2, 0, b)
        for i in range(draft_rows // qrows):
            qcopy(i).wait()
        for c in wlast():
            c.wait()

    pl.run_scoped(run, *(pltpu.ACC(u)((16, half), F32) for u in range(2) for _ in range(2 * groups)))


def verify_kernel(dims, s_ref, q_ref, scale_ref, x_ref, wend_ref, m_ref, sm_ref, dt_ref, lcol_ref, ncol_ref, out_ref, zend,
                  mrow_ref, lse_ref, e_ref, ccol_ref, g1, g2, g3, msg2, msg3, acc, at_ref, tok, send1, recv1, send2, recv2, send3, recv3):
    tp, rows, draft_rows, seqs, vocab, start = dims
    blocks = draft_rows // LANES
    me = lax.axis_index("tp")
    full = vocab // LANES * LANES
    rest = vocab - full

    barrier = pltpu.get_barrier_semaphore()
    for d in range(1, tp):
        pl.semaphore_signal(barrier, inc=1, device_id={"tp": lax.rem(me + d, tp)},
                            device_id_type=pl.DeviceIdType.MESH)
    width = wend_ref.shape[0]
    pieces = x_ref.shape[1]

    lhs = jnp.concatenate([
        jnp.concatenate([x_ref[b, p] for p in range(pieces)], axis=1) for b in range(rows // 16)], axis=0)
    zend[...] = lax.dot_general(lhs, wend_ref[...], (((1,), (1,)), ((), ())), preferred_element_type=F32)

    lse_ref[...] = jnp.zeros(lse_ref.shape, F32)
    for i in range(pl.cdiv(rows, LANES)):
        size = min(LANES, rows - i * LANES)
        r = slice(i * LANES, i * LANES + size)
        scale = jnp.concatenate([scale_ref[...]] * (size // seqs), axis=0)
        parts = [zend[r, c:c + LANES] for c in range(0, width, LANES)]
        lanes = lax.broadcasted_iota(jnp.int32, (size, LANES), 1)
        parts[-1] = jnp.where(lanes < vocab - start - width + LANES, parts[-1], NEG)
        ml = m_ref[r, :]
        top = ml
        for z in parts:
            top = jnp.maximum(top, z)
        mrow = jnp.max(top, axis=1, keepdims=True)
        tot = sm_ref[r, :] * jnp.exp2((ml - mrow) * scale)
        for z in parts:
            tot = tot + jnp.exp2((z - mrow) * scale)
        srow = jnp.sum(tot, axis=1, keepdims=True)
        lse = mrow * (scale * (1.0 / LOG2E)) + jnp.log(srow)
        if i * LANES < draft_rows:
            mrow_ref[r, :] = jnp.broadcast_to(mrow, (size, LANES))
        mask = eye()[:size]
        lse_ref[i:i + 1, :] = jnp.sum(jnp.where(mask, lse, 0.0), axis=0, keepdims=True)

    pl.semaphore_wait(barrier, tp - 1)

    def exchange(src, gather, send, recv):
        def copy(slot, sem, d):
            return pltpu.make_async_remote_copy(
                src_ref=src, dst_ref=gather.at[slot], send_sem=send.at[d], recv_sem=recv.at[sem],
                device_id={"tp": lax.rem(me + d, tp)}, device_id_type=pl.DeviceIdType.MESH)

        def start():
            for d in range(1, tp):
                copy(me, me, d).start()
            gather[me] = src[...]

        def wait():
            for d in range(1, tp):
                peer = lax.rem(me + d, tp)
                copy(peer, peer, d).wait_recv()

        def drain():
            for d in range(1, tp):
                copy(me, me, d).wait_send()

        return start, wait, drain

    start1, wait1, drain1 = exchange(lse_ref, g1, send1, recv1)
    start2, wait2, drain2 = exchange(msg2, g2, send2, recv2)
    start3, wait3, drain3 = exchange(msg3, g3, send3, recv3)
    start1()

    offset = me * vocab
    for i in range(blocks):
        ids = jnp.concatenate([dt_ref[2 * i:2 * i + 1, :], dt_ref[2 * i + 1:2 * i + 2, :]], axis=1)
        tok[i * LANES:(i + 1) * LANES, :] = to_column((ids - offset).astype(F32))
    lane = lax.broadcasted_iota(jnp.int32, (8, LANES), 1).astype(F32)
    acc[...] = jnp.zeros(acc.shape, F32)
    at_ref[...] = jnp.zeros(at_ref.shape, F32)

    @pl.loop(0, draft_rows // 8)
    def _(b):
        r8 = pl.ds(pl.multiple_of(b * 8, 8), 8)
        mr = mrow_ref[r8, :]
        scale = scale_ref[pl.ds(pl.multiple_of(lax.rem(b * 8, seqs), 8), 8), :]
        away = tok[r8, :] - lane
        zr = zend[r8, full - start:full - start + rest]
        e_ref[r8, full:full + rest] = jnp.exp2((zr - mr[:, :rest]) * scale[:, :rest])
        hit = away[:, :rest] == float(full)
        at_ref[0, r8, 0:rest] = jnp.where(hit, zr, 0.0)
        at_ref[1, r8, 0:rest] = jnp.where(hit, q_ref[r8, full:full + rest], 0.0)
        az, aq = at_ref[0, r8, :], at_ref[1, r8, :]
        for c in range(0, full, LANES):
            z = s_ref[r8, c:c + LANES] if c < start else zend[r8, c - start:c - start + LANES]
            e_ref[r8, c:c + LANES] = jnp.exp2((z - mr) * scale)
            hit = away == float(c)
            az = jnp.where(hit, z, az)
            aq = jnp.where(hit, q_ref[r8, c:c + LANES], aq)
        at_ref[0, r8, :] = az
        at_ref[1, r8, :] = aq

    msg3[...] = jnp.zeros(msg3.shape, F32)
    for i in range(blocks):
        r = slice(i * LANES, (i + 1) * LANES)
        for part in range(2):
            value = jnp.sum(at_ref[part, r, :], axis=1, keepdims=True)
            msg3[4 * part + i:4 * part + i + 1, :] = to_lanes(jnp.broadcast_to(value, (LANES, LANES)))
    start3()
    wait1()
    parts = g1[...]
    top = jnp.max(parts, axis=0)
    lse = top + jnp.log(jnp.sum(jnp.exp(parts - top[None]), axis=0))
    out_ref[...] = jnp.zeros(out_ref.shape, F32)
    out_ref[0:4, :] = lse
    for i in range(blocks):
        r = slice(i * LANES, (i + 1) * LANES)
        scale = jnp.concatenate([scale_ref[...]] * (LANES // seqs), axis=0)
        lcol = to_column(lse[i:i + 1, :]) * (LOG2E / scale)
        lcol_ref[r, :] = lcol
        ccol_ref[r, :] = jnp.exp2((mrow_ref[r, :] - lcol) * scale)

    @pl.loop(0, draft_rows // 8)
    def _(b):
        r8 = pl.ds(pl.multiple_of(b * 8, 8), 8)
        cc = ccol_ref[r8, :]
        er = e_ref[r8, full:full + rest]
        acc[r8, 0:rest] = jnp.maximum(er * cc[:, :rest] - q_ref[r8, full:full + rest], 0.0)
        sums = [acc[r8, :]] + [jnp.zeros((8, LANES), F32)] * 3
        for k, c in enumerate(range(0, full, LANES)):
            sums[k % 4] += jnp.maximum(e_ref[r8, c:c + LANES] * cc - q_ref[r8, c:c + LANES], 0.0)
        acc[r8, :] = (sums[0] + sums[1]) + (sums[2] + sums[3])

    msg2[...] = jnp.zeros(msg2.shape, F32)
    for i in range(blocks):
        total = jnp.sum(acc[i * LANES:(i + 1) * LANES, :], axis=1, keepdims=True)
        msg2[i:i + 1, :] = to_lanes(jnp.broadcast_to(total, (LANES, LANES)))
    start2()
    wait3()
    at = jnp.sum(g3[...], axis=0)
    column = jnp.concatenate([scale_ref[...]] * (LANES // seqs), axis=0)
    scale = to_lanes(column)
    p = jnp.exp2((at[0:4] - lse * (LOG2E / scale)) * scale)
    out_ref[8:12, :] = jnp.minimum(1.0, p / at[4:8])
    wait2()
    sums = jnp.sum(g2[...], axis=0)
    out_ref[4:8, :] = sums
    for i in range(blocks):
        ncol_ref[i * LANES:(i + 1) * LANES, :] = to_column(1.0 / sums[i:i + 1, :])
    drain1()
    drain2()
    drain3()


def residual_kernel(dims, s_ref, zend_ref, q_ref, lcol_ref, ncol_ref, scale_ref, small_ref, res_ref, acc_ref, norm_ref, bonus_ref,
                    stage, sem):
    draft_rows, seqs, vocab, block, slots, start = dims
    n = draft_rows // block
    full = vocab // LANES * LANES
    rest = vocab - full

    def copy(i):
        slot = lax.rem(i, slots)
        return pltpu.make_async_copy(stage.at[slot], res_ref.at[pl.ds(pl.multiple_of(i * block, block), block)],
                                     sem.at[slot])

    @pl.loop(0, n)
    def _(i):
        slot = lax.rem(i, slots)

        for b in range(block // 8):
            src = pl.ds(pl.multiple_of(i * block + b * 8, 8), 8)
            dst = slice(b * 8, b * 8 + 8)
            lc, inv = lcol_ref[src, :], ncol_ref[src, :]
            scale = scale_ref[pl.ds(pl.multiple_of(lax.rem(i * block + b * 8, seqs), 8), 8), :]
            for c in range(0, full, LANES):
                z = s_ref[src, c:c + LANES] if c < start else zend_ref[src, c - start:c - start + LANES]
                stage[slot, dst, c:c + LANES] = (
                    jnp.maximum(jnp.exp2((z - lc) * scale) - q_ref[src, c:c + LANES], 0.0) * inv)
            stage[slot, dst, full:full + rest] = (
                jnp.maximum(jnp.exp2((zend_ref[src, full - start:full - start + rest] - lc[:, :rest]) * scale[:, :rest])
                            - q_ref[src, full:full + rest], 0.0)
                * inv[:, :rest])
        copy(i).start()

    for j in range(draft_rows // seqs):
        i, off = j // 2, (j % 2) * seqs
        norm_ref[j:j + 1, :] = small_ref[4 + i:5 + i, off:off + seqs]
        acc_ref[j:j + 1, :] = small_ref[8 + i:9 + i, off:off + seqs]
    bonus_ref[...] = small_ref[3:4, 0:seqs]

    for i in range(n - slots, n):
        copy(i).wait()


def solution(mesh):
    tp = mesh.shape["tp"]
    vmem, hbm = pltpu.VMEM, pltpu.HBM

    def spec(space):
        return pl.BlockSpec(memory_space=space)

    def local_step(hidden, norm_gain, w_head, draft_probs, draft_tokens, temperature):
        seqs, positions, depth = hidden.shape
        drafts, vocab = draft_probs.shape[1:]
        rows, draft_rows = seqs * positions, seqs * drafts
        h = hidden.transpose(1, 0, 2).reshape(rows, depth)
        w = w_head.T
        q = draft_probs.transpose(1, 0, 2).reshape(draft_rows, vocab)
        dt = draft_tokens.T
        chunk, slots, qrows = 512, 4, 32
        start = (pl.cdiv(vocab, chunk) - 1) * chunk
        width = pl.cdiv(vocab - start, LANES) * LANES
        stat = pltpu.VMEM((rows, LANES), F32)
        dims = (rows, draft_rows, seqs, depth, vocab, chunk, slots, qrows)
        s, qv, scale, x, wend, m, sm = pl.pallas_call(
            functools.partial(head_kernel, dims),
            out_shape=(pltpu.VMEM((draft_rows, start), F32), pltpu.VMEM((draft_rows, vocab), F32),
                       pltpu.VMEM((seqs, LANES), F32), pltpu.VMEM((rows // 16, depth // LANES, 16, LANES), jnp.bfloat16),
                       pltpu.VMEM((width, depth), jnp.bfloat16), stat, stat),
            in_specs=[spec(hbm)] * 5,
            out_specs=(spec(vmem),) * 7,
            scratch_shapes=[
                pltpu.VMEM((rows, depth), jnp.bfloat16), pltpu.VMEM((1, depth), F32), pltpu.VMEM((1, seqs), F32),
                pltpu.VMEM((slots, chunk, depth), jnp.bfloat16),
                pltpu.VMEM((rows, LANES), F32),
                pltpu.SemaphoreType.DMA((positions,)), pltpu.SemaphoreType.DMA((2,)), pltpu.SemaphoreType.DMA((4,)),
                pltpu.SemaphoreType.DMA((slots,)), pltpu.SemaphoreType.DMA((draft_rows // qrows,)),
                pltpu.SemaphoreType.DMA((2,)),
            ],
            compiler_params=pltpu.CompilerParams(vmem_limit_bytes=18 * MIB),
        )(*(pltpu.with_memory_space_constraint(a, hbm)
            for a in (h, norm_gain.reshape(1, depth), w, q, temperature.reshape(1, seqs))))

        lcol, ncol, small, zend = pl.pallas_call(
            functools.partial(verify_kernel, (tp, rows, draft_rows, seqs, vocab, start)),
            out_shape=(pltpu.VMEM((draft_rows, LANES), F32), pltpu.VMEM((draft_rows, LANES), F32),
                       pltpu.VMEM((16, LANES), F32), pltpu.VMEM((rows, width), F32)),
            in_specs=[spec(vmem)] * 8,
            out_specs=(spec(vmem),) * 4,
            scratch_shapes=[
                pltpu.VMEM((draft_rows, LANES), F32), pltpu.VMEM((4, LANES), F32),
                pltpu.VMEM((draft_rows, start + width), F32), pltpu.VMEM((draft_rows, LANES), F32),
                pltpu.VMEM((tp, 4, LANES), F32), pltpu.VMEM((tp, 4, LANES), F32), pltpu.VMEM((tp, 8, LANES), F32),
                pltpu.VMEM((4, LANES), F32), pltpu.VMEM((8, LANES), F32),
                pltpu.VMEM((draft_rows, LANES), F32), pltpu.VMEM((2, draft_rows, LANES), F32),
                pltpu.VMEM((draft_rows, LANES), F32),
            ] + [pltpu.SemaphoreType.DMA((tp,))] * 6,
            compiler_params=pltpu.CompilerParams(vmem_limit_bytes=17 * MIB, collective_id=0, has_side_effects=True),
        )(s, qv, scale, x, wend, m, sm, dt)

        block = 16
        stages = draft_rows // block
        res, acc, norm, bonus = pl.pallas_call(
            functools.partial(residual_kernel, (draft_rows, seqs, vocab, block, stages, start)),
            out_shape=(jax.ShapeDtypeStruct((draft_rows, vocab), F32), jax.ShapeDtypeStruct((drafts, seqs), F32),
                       jax.ShapeDtypeStruct((drafts, seqs), F32), jax.ShapeDtypeStruct((1, seqs), F32)),
            in_specs=[spec(vmem)] * 7,
            out_specs=(spec(hbm), spec(vmem), spec(vmem), spec(vmem)),
            scratch_shapes=[pltpu.VMEM((stages, block, vocab), F32), pltpu.SemaphoreType.DMA((stages,))],
            compiler_params=pltpu.CompilerParams(vmem_limit_bytes=16 * MIB),
        )(s, zend, qv, lcol, ncol, scale, small)
        res = res.reshape(drafts, seqs, vocab).transpose(1, 0, 2)
        return acc.T, norm.T, res, bonus.reshape(seqs)

    return jax.shard_map(
        local_step,
        mesh=mesh,
        in_specs=(P('dp', None, None), P(), P(None, 'tp'), P('dp', None, 'tp'), P('dp', None), P('dp')),
        out_specs=(P('dp', None), P('dp', None), P('dp', None, 'tp'), P('dp')),
        check_vma=False,
    )
```

```python
import functools

import jax
import jax.numpy as jnp
from jax import lax
from jax.experimental import pallas as pl
from jax.experimental.pallas import tpu as pltpu
from jax.sharding import PartitionSpec as P

F32 = jnp.float32
LANES = 128
NEG = -3.0e38
LOG2E = 1.4426950408889634
MIB = 1024 * 1024


def eye():
    rows = lax.broadcasted_iota(jnp.int32, (LANES, LANES), 0)
    return rows == lax.broadcasted_iota(jnp.int32, (LANES, LANES), 1)


def to_lanes(column):
    return jnp.sum(jnp.where(eye(), column, 0.0), axis=0, keepdims=True)


def to_column(row):
    col = jnp.sum(jnp.where(eye(), jnp.broadcast_to(row, (LANES, LANES)), 0.0), axis=1, keepdims=True)
    return jnp.broadcast_to(col, (LANES, LANES))


def head_kernel(dims, h_ref, g_ref, w_ref, q_ref, t_ref, s_ref, qv_ref, scale_ref, x, wend, m, sm, bonus,
                hbuf, gbuf, tbuf, wbuf, rinv, hsem, gsem, fsem, wsem, qsem, esem):
    rows, draft_rows, seqs, depth, vocab, chunk, slots, qrows = dims
    n = pl.cdiv(vocab, chunk)
    tail = vocab - (n - 1) * chunk
    half = chunk // 2
    ktiles = depth // half
    groups = rows // 16
    copy = pltpu.make_async_copy

    def wcopy(i):
        slot = lax.rem(i, slots)
        at = pl.ds(pl.multiple_of(i * chunk, chunk), chunk)
        return copy(w_ref.at[at], wbuf.at[slot], wsem.at[slot])

    def wfirst(p):
        cols = slice(p * depth // 4, (p + 1) * depth // 4)
        return copy(w_ref.at[0:chunk, cols], wbuf.at[0, :, cols], fsem.at[p])

    def wlast():
        fill = wend.shape[0] - tail
        return [copy(w_ref.at[vocab - tail:vocab], wend.at[0:tail], esem.at[0]),
                copy(w_ref.at[0:fill], wend.at[tail:tail + fill], esem.at[1])]

    def wwait(i):
        slot = lax.rem(i, slots)
        copy(w_ref.at[0:chunk], wbuf.at[slot], wsem.at[slot]).wait()

    def qcopy(i):
        at = pl.ds(pl.multiple_of(i * qrows, qrows), qrows)
        return copy(q_ref.at[at], qv_ref.at[at], qsem.at[i])

    def hcopy(i):
        at = pl.ds(pl.multiple_of(i * seqs, seqs), seqs)
        return copy(h_ref.at[at], hbuf.at[at], hsem.at[i])

    small = [copy(src, dst, gsem.at[i])
             for i, (src, dst) in enumerate(((g_ref, gbuf), (t_ref, tbuf)))]
    for c in small:
        c.start()
    for i in range(rows // seqs):
        hcopy(i).start()
    wfirst(0).start()
    wfirst(1).start()

    m[...] = jnp.full(m.shape, NEG, F32)
    sm[...] = jnp.zeros(sm.shape, F32)
    for c in small:
        c.wait()
    lane = lax.broadcasted_iota(jnp.int32, (8, LANES), 1)
    t = tbuf[...]
    spread = jnp.where(eye(), jnp.broadcast_to(jnp.concatenate([t, t], axis=1), (LANES, LANES)), 0.0)
    tcol = jnp.sum(spread, axis=1, keepdims=True)
    scale_ref[...] = jnp.broadcast_to(LOG2E / tcol[:seqs], (seqs, LANES))

    for i in range(rows // seqs):
        hcopy(i).wait()
        if i == 0:
            wfirst(2).start()
            wfirst(3).start()
        if i == 3:
            wcopy(1).start()
        for b in range(i * seqs, (i + 1) * seqs, 16):
            h = hbuf[b:b + 16, :].astype(F32)
            r = lax.rsqrt(jnp.mean(h * h, axis=1, keepdims=True) + 1e-5)
            rinv[b:b + 16, :] = jnp.broadcast_to(r, (16, LANES))

    def normalise(k):
        for b in range(0, rows, 16):
            r = rinv[b:b + 16, :]
            for c in range(k * half, (k + 1) * half, LANES):
                h = hbuf[b:b + 16, c:c + LANES].astype(F32)
                x[b // 16, c // LANES] = (h * r * gbuf[:, c:c + LANES]).astype(jnp.bfloat16)

    def push(i, k):
        slot = lax.rem(i, slots)
        cols = slice(k * half, (k + 1) * half)
        for u in range(2):
            pltpu.matmul_push_rhs(wbuf[slot, u * half:(u + 1) * half, cols], k % 2, u, transpose=True)

    def run(*refs):
        accs = [[refs[(2 * u + v) * groups:(2 * u + v + 1) * groups] for v in range(2)] for u in range(2)]

        def stats(i, side, b, size=chunk, valid=chunk):
            base = pl.multiple_of(i * chunk, chunk)
            zs = [pltpu.matmul_pop(accs[u][side][b]) for u in range(2)]
            for o in (0, 8):
                row = b * 16 + o
                r8 = slice(row, row + 8)
                scale = scale_ref[row % seqs:row % seqs + 8, :]
                parts = []
                for c in range(0, size, LANES):
                    z = zs[c // half][o:o + 8, c % half:c % half + LANES]
                    if c + LANES > valid:
                        z = jnp.where(lane < valid - c, z, NEG)
                    parts.append(z)
                    if row < draft_rows:
                        s_ref[r8, pl.ds(base + c, LANES)] = z
                old = m[r8, :]
                new = old
                for z in parts:
                    new = jnp.maximum(new, z)
                tot = sm[r8, :] * jnp.exp2((old - new) * scale)
                for z in parts:
                    tot = tot + jnp.exp2((z - new) * scale)
                m[r8, :] = new
                sm[r8, :] = tot

        def matmul(i, side, last=False, first=False):
            for k in range(ktiles):
                if first:
                    normalise(k)
                    if k == 6:
                        wcopy(3).start()
                if k + 1 < ktiles:
                    if first and (k + 1) % (ktiles // 4) == 0:
                        wfirst((k + 1) // (ktiles // 4)).wait()
                    push(i, k + 1)
                elif not last:
                    wwait(i + 1)
                    push(i + 1, 0)
                for b in range(groups):
                    lhs = jnp.concatenate([x[b, k * half // LANES + c] for c in range(half // LANES)], axis=1)
                    for u in range(2):
                        pltpu.matmul_acc_lhs(accs[u][side][b], lhs, load_staged_rhs=k % 2 if b == 0 else None)
                    done = k * groups + b
                    if not first and done % ktiles == ktiles - 1:
                        stats(i - 1, 1 - side, done // ktiles)

        pairs = (n - 2) // 2
        wfirst(0).wait()
        push(0, 0)
        wcopy(2).start()
        matmul(0, 0, first=True)

        @pl.loop(0, pairs - 1)
        def _(k):
            i = 2 * k + 1
            wcopy(i + 3).start()
            qcopy(2 * k).start()
            qcopy(2 * k + 1).start()
            matmul(i, 1)

            @pl.when(k < pairs - 2)
            def _():
                wcopy(i + 4).start()

            @pl.when(k == pairs - 2)
            def _():
                for c in wlast():
                    c.start()

            matmul(i + 1, 0)

        matmul(n - 3, 1)
        matmul(n - 2, 0, True)
        for b in range(groups):
            zs = [pltpu.matmul_pop(accs[u][0][b]) for u in range(2)]
            for u in range(2):
                if b * 16 < draft_rows:
                    s_ref[b * 16:b * 16 + 16, (n - 2) * chunk + u * half:(n - 2) * chunk + (u + 1) * half] = zs[u]
                else:
                    bonus[b * 16 - draft_rows:b * 16 - draft_rows + 16, u * half:(u + 1) * half] = zs[u]
        for i in range(draft_rows // qrows):
            qcopy(i).wait()
        for c in wlast():
            c.wait()

    pl.run_scoped(run, *(pltpu.ACC(u)((16, half), F32) for u in range(2) for _ in range(2 * groups)))


def verify_kernel(dims, s_ref, q_ref, scale_ref, x_ref, wend_ref, m_ref, sm_ref, bonus_ref, dt_ref, lcol_ref, ncol_ref, out_ref, zend,
                  mrow_ref, lse_ref, e_ref, ccol_ref, g1, g2, g3, msg2, msg3, acc, at_ref, tok, send1, recv1, send2, recv2, send3, recv3):
    tp, rows, draft_rows, seqs, vocab, start = dims
    blocks = draft_rows // LANES
    me = lax.axis_index("tp")
    full = vocab // LANES * LANES
    rest = vocab - full

    barrier = pltpu.get_barrier_semaphore()
    for d in range(1, tp):
        pl.semaphore_signal(barrier, inc=1, device_id={"tp": lax.rem(me + d, tp)},
                            device_id_type=pl.DeviceIdType.MESH)
    width = wend_ref.shape[0]
    pieces = x_ref.shape[1]

    lhs = jnp.concatenate([
        jnp.concatenate([x_ref[b, p] for p in range(pieces)], axis=1) for b in range(rows // 16)], axis=0)
    zend[...] = lax.dot_general(lhs, wend_ref[...], (((1,), (1,)), ((), ())), preferred_element_type=F32)

    lse_ref[...] = jnp.zeros(lse_ref.shape, F32)
    for i in range(pl.cdiv(rows, LANES)):
        size = min(LANES, rows - i * LANES)
        r = slice(i * LANES, i * LANES + size)
        scale = jnp.concatenate([scale_ref[...]] * (size // seqs), axis=0)
        parts = [zend[r, c:c + LANES] for c in range(0, width, LANES)]
        lanes = lax.broadcasted_iota(jnp.int32, (size, LANES), 1)
        parts[-1] = jnp.where(lanes < vocab - start - width + LANES, parts[-1], NEG)
        for c in range(0, bonus_ref.shape[1], LANES):
            if i * LANES < draft_rows:
                at = start - bonus_ref.shape[1] + c
                parts.append(s_ref[r, at:at + LANES])
            else:
                parts.append(bonus_ref[:, c:c + LANES])
        ml = m_ref[r, :]
        top = ml
        for z in parts:
            top = jnp.maximum(top, z)
        mrow = jnp.max(top, axis=1, keepdims=True)
        tot = sm_ref[r, :] * jnp.exp2((ml - mrow) * scale)
        for z in parts:
            tot = tot + jnp.exp2((z - mrow) * scale)
        srow = jnp.sum(tot, axis=1, keepdims=True)
        lse = mrow * (scale * (1.0 / LOG2E)) + jnp.log(srow)
        if i * LANES < draft_rows:
            mrow_ref[r, :] = jnp.broadcast_to(mrow, (size, LANES))
        mask = eye()[:size]
        lse_ref[i:i + 1, :] = jnp.sum(jnp.where(mask, lse, 0.0), axis=0, keepdims=True)

    pl.semaphore_wait(barrier, tp - 1)

    def exchange(src, gather, send, recv):
        def copy(slot, sem, d):
            return pltpu.make_async_remote_copy(
                src_ref=src, dst_ref=gather.at[slot], send_sem=send.at[d], recv_sem=recv.at[sem],
                device_id={"tp": lax.rem(me + d, tp)}, device_id_type=pl.DeviceIdType.MESH)

        def start():
            for d in range(1, tp):
                copy(me, me, d).start()
            gather[me] = src[...]

        def wait():
            for d in range(1, tp):
                peer = lax.rem(me + d, tp)
                copy(peer, peer, d).wait_recv()

        def drain():
            for d in range(1, tp):
                copy(me, me, d).wait_send()

        return start, wait, drain

    start1, wait1, drain1 = exchange(lse_ref, g1, send1, recv1)
    start2, wait2, drain2 = exchange(msg2, g2, send2, recv2)
    start3, wait3, drain3 = exchange(msg3, g3, send3, recv3)
    start1()

    offset = me * vocab
    for i in range(blocks):
        ids = jnp.concatenate([dt_ref[2 * i:2 * i + 1, :], dt_ref[2 * i + 1:2 * i + 2, :]], axis=1)
        tok[i * LANES:(i + 1) * LANES, :] = to_column((ids - offset).astype(F32))
    lane = lax.broadcasted_iota(jnp.int32, (8, LANES), 1).astype(F32)
    acc[...] = jnp.zeros(acc.shape, F32)
    at_ref[...] = jnp.zeros(at_ref.shape, F32)

    @pl.loop(0, draft_rows // 8)
    def _(b):
        r8 = pl.ds(pl.multiple_of(b * 8, 8), 8)
        mr = mrow_ref[r8, :]
        scale = scale_ref[pl.ds(pl.multiple_of(lax.rem(b * 8, seqs), 8), 8), :]
        away = tok[r8, :] - lane
        zr = zend[r8, full - start:full - start + rest]
        e_ref[r8, full:full + rest] = jnp.exp2((zr - mr[:, :rest]) * scale[:, :rest])
        hit = away[:, :rest] == float(full)
        at_ref[0, r8, 0:rest] = jnp.where(hit, zr, 0.0)
        at_ref[1, r8, 0:rest] = jnp.where(hit, q_ref[r8, full:full + rest], 0.0)
        az, aq = at_ref[0, r8, :], at_ref[1, r8, :]
        for c in range(0, full, LANES):
            z = s_ref[r8, c:c + LANES] if c < start else zend[r8, c - start:c - start + LANES]
            e_ref[r8, c:c + LANES] = jnp.exp2((z - mr) * scale)
            hit = away == float(c)
            az = jnp.where(hit, z, az)
            aq = jnp.where(hit, q_ref[r8, c:c + LANES], aq)
        at_ref[0, r8, :] = az
        at_ref[1, r8, :] = aq

    msg3[...] = jnp.zeros(msg3.shape, F32)
    for i in range(blocks):
        r = slice(i * LANES, (i + 1) * LANES)
        for part in range(2):
            value = jnp.sum(at_ref[part, r, :], axis=1, keepdims=True)
            msg3[4 * part + i:4 * part + i + 1, :] = to_lanes(jnp.broadcast_to(value, (LANES, LANES)))
    start3()
    wait1()
    parts = g1[...]
    top = jnp.max(parts, axis=0)
    lse = top + jnp.log(jnp.sum(jnp.exp(parts - top[None]), axis=0))
    out_ref[...] = jnp.zeros(out_ref.shape, F32)
    out_ref[0:4, :] = lse
    for i in range(blocks):
        r = slice(i * LANES, (i + 1) * LANES)
        scale = jnp.concatenate([scale_ref[...]] * (LANES // seqs), axis=0)
        lcol = to_column(lse[i:i + 1, :]) * (LOG2E / scale)
        lcol_ref[r, :] = lcol
        ccol_ref[r, :] = jnp.exp2((mrow_ref[r, :] - lcol) * scale)

    @pl.loop(0, draft_rows // 8)
    def _(b):
        r8 = pl.ds(pl.multiple_of(b * 8, 8), 8)
        cc = ccol_ref[r8, :]
        er = e_ref[r8, full:full + rest]
        acc[r8, 0:rest] = jnp.maximum(er * cc[:, :rest] - q_ref[r8, full:full + rest], 0.0)
        sums = [acc[r8, :]] + [jnp.zeros((8, LANES), F32)] * 3
        for k, c in enumerate(range(0, full, LANES)):
            sums[k % 4] += jnp.maximum(e_ref[r8, c:c + LANES] * cc - q_ref[r8, c:c + LANES], 0.0)
        acc[r8, :] = (sums[0] + sums[1]) + (sums[2] + sums[3])

    msg2[...] = jnp.zeros(msg2.shape, F32)
    for i in range(blocks):
        total = jnp.sum(acc[i * LANES:(i + 1) * LANES, :], axis=1, keepdims=True)
        msg2[i:i + 1, :] = to_lanes(jnp.broadcast_to(total, (LANES, LANES)))
    start2()
    wait3()
    at = jnp.sum(g3[...], axis=0)
    column = jnp.concatenate([scale_ref[...]] * (LANES // seqs), axis=0)
    scale = to_lanes(column)
    p = jnp.exp2((at[0:4] - lse * (LOG2E / scale)) * scale)
    out_ref[8:12, :] = jnp.minimum(1.0, p / at[4:8])
    drain1()
    drain3()
    drain2()
    wait2()
    sums = jnp.sum(g2[...], axis=0)
    out_ref[4:8, :] = sums
    for i in range(blocks):
        ncol_ref[i * LANES:(i + 1) * LANES, :] = to_column(1.0 / sums[i:i + 1, :])


def residual_kernel(dims, s_ref, zend_ref, q_ref, lcol_ref, ncol_ref, scale_ref, small_ref, res_ref, *refs):
    draft_rows, seqs, vocab, block, slots, start = dims
    outs, (acc_ref, norm_ref, bonus_ref, stage, sem, small_sem) = refs[:3], refs[3:]
    n = draft_rows // block
    full = vocab // LANES * LANES
    rest = vocab - full

    def copy(i):
        slot = lax.rem(i, slots)
        return pltpu.make_async_copy(stage.at[slot], res_ref.at[pl.ds(pl.multiple_of(i * block, block), block)],
                                     sem.at[slot])

    for j in range(draft_rows // seqs):
        i, off = j // 2, (j % 2) * seqs
        norm_ref[j:j + 1, :] = small_ref[4 + i:5 + i, off:off + seqs]
        acc_ref[j:j + 1, :] = small_ref[8 + i:9 + i, off:off + seqs]
    bonus_ref[...] = small_ref[3:4, 0:seqs]
    small_copies = [pltpu.make_async_copy(src, dst, small_sem.at[i])
                    for i, (src, dst) in enumerate(zip((acc_ref, norm_ref, bonus_ref), outs))]
    for c in small_copies:
        c.start()

    @pl.loop(0, n)
    def _(i):
        slot = lax.rem(i, slots)

        for b in range(block // 8):
            src = pl.ds(pl.multiple_of(i * block + b * 8, 8), 8)
            dst = slice(b * 8, b * 8 + 8)
            lc, inv = lcol_ref[src, :], ncol_ref[src, :]
            scale = scale_ref[pl.ds(pl.multiple_of(lax.rem(i * block + b * 8, seqs), 8), 8), :]
            for c in range(0, full, LANES):
                z = s_ref[src, c:c + LANES] if c < start else zend_ref[src, c - start:c - start + LANES]
                stage[slot, dst, c:c + LANES] = (
                    jnp.maximum(jnp.exp2((z - lc) * scale) - q_ref[src, c:c + LANES], 0.0) * inv)
            stage[slot, dst, full:full + rest] = (
                jnp.maximum(jnp.exp2((zend_ref[src, full - start:full - start + rest] - lc[:, :rest]) * scale[:, :rest])
                            - q_ref[src, full:full + rest], 0.0)
                * inv[:, :rest])
        copy(i).start()

    for c in small_copies:
        c.wait()
    for i in range(n - slots, n):
        copy(i).wait()


def solution(mesh):
    tp = mesh.shape["tp"]
    vmem, hbm = pltpu.VMEM, pltpu.HBM

    def spec(space):
        return pl.BlockSpec(memory_space=space)

    def local_step(hidden, norm_gain, w_head, draft_probs, draft_tokens, temperature):
        seqs, positions, depth = hidden.shape
        drafts, vocab = draft_probs.shape[1:]
        rows, draft_rows = seqs * positions, seqs * drafts
        h = hidden.transpose(1, 0, 2).reshape(rows, depth)
        w = w_head.T
        q = draft_probs.transpose(1, 0, 2).reshape(draft_rows, vocab)
        dt = draft_tokens.T
        chunk, slots, qrows = 512, 4, 32
        start = (pl.cdiv(vocab, chunk) - 1) * chunk
        width = pl.cdiv(vocab - start, LANES) * LANES
        stat = pltpu.VMEM((rows, LANES), F32)
        dims = (rows, draft_rows, seqs, depth, vocab, chunk, slots, qrows)
        s, qv, scale, x, wend, m, sm, bonus = pl.pallas_call(
            functools.partial(head_kernel, dims),
            out_shape=(pltpu.VMEM((draft_rows, start), F32), pltpu.VMEM((draft_rows, vocab), F32),
                       pltpu.VMEM((seqs, LANES), F32), pltpu.VMEM((rows // 16, depth // LANES, 16, LANES), jnp.bfloat16),
                       pltpu.VMEM((width, depth), jnp.bfloat16), stat, stat,
                       pltpu.VMEM((rows - draft_rows, chunk), F32)),
            in_specs=[spec(hbm)] * 5,
            out_specs=(spec(vmem),) * 8,
            scratch_shapes=[
                pltpu.VMEM((rows, depth), jnp.bfloat16), pltpu.VMEM((1, depth), F32), pltpu.VMEM((1, seqs), F32),
                pltpu.VMEM((slots, chunk, depth), jnp.bfloat16),
                pltpu.VMEM((rows, LANES), F32),
                pltpu.SemaphoreType.DMA((positions,)), pltpu.SemaphoreType.DMA((2,)), pltpu.SemaphoreType.DMA((4,)),
                pltpu.SemaphoreType.DMA((slots,)), pltpu.SemaphoreType.DMA((draft_rows // qrows,)),
                pltpu.SemaphoreType.DMA((2,)),
            ],
            compiler_params=pltpu.CompilerParams(vmem_limit_bytes=18 * MIB),
        )(*(pltpu.with_memory_space_constraint(a, hbm)
            for a in (h, norm_gain.reshape(1, depth), w, q, temperature.reshape(1, seqs))))

        lcol, ncol, small, zend = pl.pallas_call(
            functools.partial(verify_kernel, (tp, rows, draft_rows, seqs, vocab, start)),
            out_shape=(pltpu.VMEM((draft_rows, LANES), F32), pltpu.VMEM((draft_rows, LANES), F32),
                       pltpu.VMEM((16, LANES), F32), pltpu.VMEM((rows, width), F32)),
            in_specs=[spec(vmem)] * 9,
            out_specs=(spec(vmem),) * 4,
            scratch_shapes=[
                pltpu.VMEM((draft_rows, LANES), F32), pltpu.VMEM((4, LANES), F32),
                pltpu.VMEM((draft_rows, start + width), F32), pltpu.VMEM((draft_rows, LANES), F32),
                pltpu.VMEM((tp, 4, LANES), F32), pltpu.VMEM((tp, 4, LANES), F32), pltpu.VMEM((tp, 8, LANES), F32),
                pltpu.VMEM((4, LANES), F32), pltpu.VMEM((8, LANES), F32),
                pltpu.VMEM((draft_rows, LANES), F32), pltpu.VMEM((2, draft_rows, LANES), F32),
                pltpu.VMEM((draft_rows, LANES), F32),
            ] + [pltpu.SemaphoreType.DMA((tp,))] * 6,
            compiler_params=pltpu.CompilerParams(vmem_limit_bytes=17 * MIB, collective_id=0, has_side_effects=True),
        )(s, qv, scale, x, wend, m, sm, bonus, dt)

        block = 16
        stages = draft_rows // block
        res, acc, norm, bonus = pl.pallas_call(
            functools.partial(residual_kernel, (draft_rows, seqs, vocab, block, stages, start)),
            out_shape=(jax.ShapeDtypeStruct((draft_rows, vocab), F32), jax.ShapeDtypeStruct((drafts, seqs), F32),
                       jax.ShapeDtypeStruct((drafts, seqs), F32), jax.ShapeDtypeStruct((1, seqs), F32)),
            in_specs=[spec(vmem)] * 7,
            out_specs=(spec(hbm),) * 4,
            scratch_shapes=[
                pltpu.VMEM((drafts, seqs), F32), pltpu.VMEM((drafts, seqs), F32), pltpu.VMEM((1, seqs), F32),
                pltpu.VMEM((stages, block, vocab), F32), pltpu.SemaphoreType.DMA((stages,)),
                pltpu.SemaphoreType.DMA((3,)),
            ],
            compiler_params=pltpu.CompilerParams(vmem_limit_bytes=16 * MIB),
        )(s, zend, qv, lcol, ncol, scale, small)
        res = res.reshape(drafts, seqs, vocab).transpose(1, 0, 2)
        return acc.T, norm.T, res, bonus.reshape(seqs)

    return jax.shard_map(
        local_step,
        mesh=mesh,
        in_specs=(P('dp', None, None), P(), P(None, 'tp'), P('dp', None, 'tp'), P('dp', None), P('dp')),
        out_specs=(P('dp', None), P('dp', None), P('dp', None, 'tp'), P('dp')),
        check_vma=False,
    )
```

```python
import functools

import jax
import jax.numpy as jnp
from jax import lax
from jax.experimental import pallas as pl
from jax.experimental.pallas import tpu as pltpu
from jax.sharding import PartitionSpec as P

F32 = jnp.float32
LANES = 128
NEG = -3.0e38
LOG2E = 1.4426950408889634
MIB = 1024 * 1024


def eye():
    rows = lax.broadcasted_iota(jnp.int32, (LANES, LANES), 0)
    return rows == lax.broadcasted_iota(jnp.int32, (LANES, LANES), 1)


def to_lanes(column):
    return jnp.sum(jnp.where(eye(), column, 0.0), axis=0, keepdims=True)


def to_column(row):
    col = jnp.sum(jnp.where(eye(), jnp.broadcast_to(row, (LANES, LANES)), 0.0), axis=1, keepdims=True)
    return jnp.broadcast_to(col, (LANES, LANES))


def head_kernel(dims, h_ref, g_ref, w_ref, q_ref, t_ref, s_ref, qv_ref, scale_ref, x, wend, m, sm, bonus,
                hbuf, gbuf, tbuf, wbuf, rinv, hsem, gsem, fsem, wsem, qsem, esem):
    rows, draft_rows, seqs, depth, vocab, chunk, slots, qrows = dims
    n = pl.cdiv(vocab, chunk)
    tail = vocab - (n - 1) * chunk
    half = chunk // 2
    ktiles = depth // half
    groups = rows // 16
    copy = pltpu.make_async_copy

    def wcopy(i):
        slot = lax.rem(i, slots)
        at = pl.ds(pl.multiple_of(i * chunk, chunk), chunk)
        return copy(w_ref.at[at], wbuf.at[slot], wsem.at[slot])

    def wfirst(p):
        cols = slice(p * depth // 4, (p + 1) * depth // 4)
        return copy(w_ref.at[0:chunk, cols], wbuf.at[0, :, cols], fsem.at[p])

    def wlast():
        fill = wend.shape[0] - tail
        return [copy(w_ref.at[vocab - tail:vocab], wend.at[0:tail], esem.at[0]),
                copy(w_ref.at[0:fill], wend.at[tail:tail + fill], esem.at[1])]

    def wwait(i):
        slot = lax.rem(i, slots)
        copy(w_ref.at[0:chunk], wbuf.at[slot], wsem.at[slot]).wait()

    def qcopy(i):
        at = pl.ds(pl.multiple_of(i * qrows, qrows), qrows)
        return copy(q_ref.at[at], qv_ref.at[at], qsem.at[i])

    def hcopy(i):
        at = pl.ds(pl.multiple_of(i * seqs, seqs), seqs)
        return copy(h_ref.at[at], hbuf.at[at], hsem.at[i])

    small = [copy(src, dst, gsem.at[i])
             for i, (src, dst) in enumerate(((g_ref, gbuf), (t_ref, tbuf)))]
    for c in small:
        c.start()
    for i in range(rows // seqs):
        hcopy(i).start()
    wfirst(0).start()
    wfirst(1).start()

    m[...] = jnp.full(m.shape, NEG, F32)
    sm[...] = jnp.zeros(sm.shape, F32)
    for c in small:
        c.wait()
    lane = lax.broadcasted_iota(jnp.int32, (8, LANES), 1)
    t = tbuf[...]
    spread = jnp.where(eye(), jnp.broadcast_to(jnp.concatenate([t, t], axis=1), (LANES, LANES)), 0.0)
    tcol = jnp.sum(spread, axis=1, keepdims=True)
    scale_ref[...] = jnp.broadcast_to(LOG2E / tcol[:seqs], (seqs, LANES))

    def inverse_rms(i):
        hcopy(i).wait()
        for b in range(i * seqs, (i + 1) * seqs, 16):
            h = hbuf[b:b + 16, :].astype(F32)
            r = lax.rsqrt(jnp.mean(h * h, axis=1, keepdims=True) + 1e-5)
            rinv[b:b + 16, :] = jnp.broadcast_to(r, (16, LANES))

    early = 4
    for i in range(early):
        inverse_rms(i)
        if i == 0:
            wfirst(2).start()
            wfirst(3).start()
    wcopy(1).start()

    def normalise(k, blocks):
        for b in blocks:
            r = rinv[b * 16:b * 16 + 16, :]
            for c in range(k * half, (k + 1) * half, LANES):
                h = hbuf[b * 16:b * 16 + 16, c:c + LANES].astype(F32)
                x[b, c // LANES] = (h * r * gbuf[:, c:c + LANES]).astype(jnp.bfloat16)

    def push(i, k):
        slot = lax.rem(i, slots)
        cols = slice(k * half, (k + 1) * half)
        for u in range(2):
            pltpu.matmul_push_rhs(wbuf[slot, u * half:(u + 1) * half, cols], k % 2, u, transpose=True)

    def run(*refs):
        accs = [[refs[(2 * u + v) * groups:(2 * u + v + 1) * groups] for v in range(2)] for u in range(2)]

        def stats(i, side, b, size=chunk, valid=chunk):
            base = pl.multiple_of(i * chunk, chunk)
            zs = [pltpu.matmul_pop(accs[u][side][b]) for u in range(2)]
            for o in (0, 8):
                row = b * 16 + o
                r8 = slice(row, row + 8)
                scale = scale_ref[row % seqs:row % seqs + 8, :]
                parts = []
                for c in range(0, size, LANES):
                    z = zs[c // half][o:o + 8, c % half:c % half + LANES]
                    if c + LANES > valid:
                        z = jnp.where(lane < valid - c, z, NEG)
                    parts.append(z)
                    if row < draft_rows:
                        s_ref[r8, pl.ds(base + c, LANES)] = z
                old = m[r8, :]
                new = old
                for z in parts:
                    new = jnp.maximum(new, z)
                tot = sm[r8, :] * jnp.exp2((old - new) * scale)
                for z in parts:
                    tot = tot + jnp.exp2((z - new) * scale)
                m[r8, :] = new
                sm[r8, :] = tot

        def accumulate(side, k, b, load):
            lhs = jnp.concatenate([x[b, k * half // LANES + c] for c in range(half // LANES)], axis=1)
            for u in range(2):
                pltpu.matmul_acc_lhs(accs[u][side][b], lhs, load_staged_rhs=k % 2 if load else None)

        def first_chunk():
            cut = early * seqs // 16
            for part, blocks in enumerate((range(cut), range(cut, groups))):
                for k in range(ktiles):
                    if part == 1 and k == 0:
                        wcopy(3).start()
                    normalise(k, blocks)
                    if k + 1 < ktiles:
                        if part == 0 and (k + 1) % (ktiles // 4) == 0:
                            wfirst((k + 1) // (ktiles // 4)).wait()
                            inverse_rms(early - 1 + (k + 1) // (ktiles // 4))
                        push(0, k + 1)
                    elif part == 0:
                        push(0, 0)
                    else:
                        wwait(1)
                        push(1, 0)
                    for b in blocks:
                        accumulate(0, k, b, b == blocks[0])

        def matmul(i, side, last=False):
            for k in range(ktiles):
                if k + 1 < ktiles:
                    push(i, k + 1)
                elif not last:
                    wwait(i + 1)
                    push(i + 1, 0)
                for b in range(groups):
                    accumulate(side, k, b, b == 0)
                    done = k * groups + b
                    if done % ktiles == ktiles - 1:
                        stats(i - 1, 1 - side, done // ktiles)

        pairs = (n - 2) // 2
        wfirst(0).wait()
        push(0, 0)
        wcopy(2).start()
        first_chunk()

        @pl.loop(0, pairs - 1)
        def _(k):
            i = 2 * k + 1
            wcopy(i + 3).start()
            qcopy(2 * k).start()
            qcopy(2 * k + 1).start()
            matmul(i, 1)

            @pl.when(k < pairs - 2)
            def _():
                wcopy(i + 4).start()

            @pl.when(k == pairs - 2)
            def _():
                for c in wlast():
                    c.start()

            matmul(i + 1, 0)

        matmul(n - 3, 1)
        matmul(n - 2, 0, True)
        for b in range(groups):
            zs = [pltpu.matmul_pop(accs[u][0][b]) for u in range(2)]
            for u in range(2):
                if b * 16 < draft_rows:
                    s_ref[b * 16:b * 16 + 16, (n - 2) * chunk + u * half:(n - 2) * chunk + (u + 1) * half] = zs[u]
                else:
                    bonus[b * 16 - draft_rows:b * 16 - draft_rows + 16, u * half:(u + 1) * half] = zs[u]
        for i in range(draft_rows // qrows):
            qcopy(i).wait()
        for c in wlast():
            c.wait()

    pl.run_scoped(run, *(pltpu.ACC(u)((16, half), F32) for u in range(2) for _ in range(2 * groups)))


def verify_kernel(dims, s_ref, q_ref, scale_ref, x_ref, wend_ref, m_ref, sm_ref, bonus_ref, dt_ref, lcol_ref, ncol_ref, out_ref, zend,
                  mrow_ref, lse_ref, e_ref, ccol_ref, g1, g2, g3, msg2, msg3, acc, at_ref, tok, send1, recv1, send2, recv2, send3, recv3):
    tp, rows, draft_rows, seqs, vocab, start = dims
    blocks = draft_rows // LANES
    me = lax.axis_index("tp")
    full = vocab // LANES * LANES
    rest = vocab - full

    barrier = pltpu.get_barrier_semaphore()
    for d in range(1, tp):
        pl.semaphore_signal(barrier, inc=1, device_id={"tp": lax.rem(me + d, tp)},
                            device_id_type=pl.DeviceIdType.MESH)
    width = wend_ref.shape[0]
    pieces = x_ref.shape[1]

    lhs = jnp.concatenate([
        jnp.concatenate([x_ref[b, p] for p in range(pieces)], axis=1) for b in range(rows // 16)], axis=0)
    zend[...] = lax.dot_general(lhs, wend_ref[...], (((1,), (1,)), ((), ())), preferred_element_type=F32)

    lse_ref[...] = jnp.zeros(lse_ref.shape, F32)
    for i in range(pl.cdiv(rows, LANES)):
        size = min(LANES, rows - i * LANES)
        r = slice(i * LANES, i * LANES + size)
        scale = jnp.concatenate([scale_ref[...]] * (size // seqs), axis=0)
        parts = [zend[r, c:c + LANES] for c in range(0, width, LANES)]
        lanes = lax.broadcasted_iota(jnp.int32, (size, LANES), 1)
        parts[-1] = jnp.where(lanes < vocab - start - width + LANES, parts[-1], NEG)
        for c in range(0, bonus_ref.shape[1], LANES):
            if i * LANES < draft_rows:
                at = start - bonus_ref.shape[1] + c
                parts.append(s_ref[r, at:at + LANES])
            else:
                parts.append(bonus_ref[:, c:c + LANES])
        ml = m_ref[r, :]
        top = ml
        for z in parts:
            top = jnp.maximum(top, z)
        mrow = jnp.max(top, axis=1, keepdims=True)
        tot = sm_ref[r, :] * jnp.exp2((ml - mrow) * scale)
        for z in parts:
            tot = tot + jnp.exp2((z - mrow) * scale)
        srow = jnp.sum(tot, axis=1, keepdims=True)
        lse = mrow * (scale * (1.0 / LOG2E)) + jnp.log(srow)
        if i * LANES < draft_rows:
            mrow_ref[r, :] = jnp.broadcast_to(mrow, (size, LANES))
        mask = eye()[:size]
        lse_ref[i:i + 1, :] = jnp.sum(jnp.where(mask, lse, 0.0), axis=0, keepdims=True)

    pl.semaphore_wait(barrier, tp - 1)

    def exchange(src, gather, send, recv):
        def copy(slot, sem, d):
            return pltpu.make_async_remote_copy(
                src_ref=src, dst_ref=gather.at[slot], send_sem=send.at[d], recv_sem=recv.at[sem],
                device_id={"tp": lax.rem(me + d, tp)}, device_id_type=pl.DeviceIdType.MESH)

        def start():
            for d in range(1, tp):
                copy(me, me, d).start()
            gather[me] = src[...]

        def wait():
            for d in range(1, tp):
                peer = lax.rem(me + d, tp)
                copy(peer, peer, d).wait_recv()

        def drain():
            for d in range(1, tp):
                copy(me, me, d).wait_send()

        return start, wait, drain

    start1, wait1, drain1 = exchange(lse_ref, g1, send1, recv1)
    start2, wait2, drain2 = exchange(msg2, g2, send2, recv2)
    start3, wait3, drain3 = exchange(msg3, g3, send3, recv3)
    start1()

    offset = me * vocab
    for i in range(blocks):
        ids = jnp.concatenate([dt_ref[2 * i:2 * i + 1, :], dt_ref[2 * i + 1:2 * i + 2, :]], axis=1)
        tok[i * LANES:(i + 1) * LANES, :] = to_column((ids - offset).astype(F32))
    lane = lax.broadcasted_iota(jnp.int32, (8, LANES), 1).astype(F32)
    acc[...] = jnp.zeros(acc.shape, F32)
    at_ref[...] = jnp.zeros(at_ref.shape, F32)

    @pl.loop(0, draft_rows // 8)
    def _(b):
        r8 = pl.ds(pl.multiple_of(b * 8, 8), 8)
        mr = mrow_ref[r8, :]
        scale = scale_ref[pl.ds(pl.multiple_of(lax.rem(b * 8, seqs), 8), 8), :]
        away = tok[r8, :] - lane
        zr = zend[r8, full - start:full - start + rest]
        e_ref[r8, full:full + rest] = jnp.exp2((zr - mr[:, :rest]) * scale[:, :rest])
        hit = away[:, :rest] == float(full)
        at_ref[0, r8, 0:rest] = jnp.where(hit, zr, 0.0)
        at_ref[1, r8, 0:rest] = jnp.where(hit, q_ref[r8, full:full + rest], 0.0)
        az, aq = at_ref[0, r8, :], at_ref[1, r8, :]
        for c in range(0, full, LANES):
            z = s_ref[r8, c:c + LANES] if c < start else zend[r8, c - start:c - start + LANES]
            e_ref[r8, c:c + LANES] = jnp.exp2((z - mr) * scale)
            hit = away == float(c)
            az = jnp.where(hit, z, az)
            aq = jnp.where(hit, q_ref[r8, c:c + LANES], aq)
        at_ref[0, r8, :] = az
        at_ref[1, r8, :] = aq

    msg3[...] = jnp.zeros(msg3.shape, F32)
    for i in range(blocks):
        r = slice(i * LANES, (i + 1) * LANES)
        for part in range(2):
            value = jnp.sum(at_ref[part, r, :], axis=1, keepdims=True)
            msg3[4 * part + i:4 * part + i + 1, :] = to_lanes(jnp.broadcast_to(value, (LANES, LANES)))
    start3()
    wait1()
    parts = g1[...]
    top = jnp.max(parts, axis=0)
    lse = top + jnp.log(jnp.sum(jnp.exp(parts - top[None]), axis=0))
    out_ref[...] = jnp.zeros(out_ref.shape, F32)
    out_ref[0:4, :] = lse
    for i in range(blocks):
        r = slice(i * LANES, (i + 1) * LANES)
        scale = jnp.concatenate([scale_ref[...]] * (LANES // seqs), axis=0)
        lcol = to_column(lse[i:i + 1, :]) * (LOG2E / scale)
        lcol_ref[r, :] = lcol
        ccol_ref[r, :] = jnp.exp2((mrow_ref[r, :] - lcol) * scale)

    @pl.loop(0, draft_rows // 8)
    def _(b):
        r8 = pl.ds(pl.multiple_of(b * 8, 8), 8)
        cc = ccol_ref[r8, :]
        er = e_ref[r8, full:full + rest]
        acc[r8, 0:rest] = jnp.maximum(er * cc[:, :rest] - q_ref[r8, full:full + rest], 0.0)
        sums = [acc[r8, :]] + [jnp.zeros((8, LANES), F32)] * 3
        for k, c in enumerate(range(0, full, LANES)):
            sums[k % 4] += jnp.maximum(e_ref[r8, c:c + LANES] * cc - q_ref[r8, c:c + LANES], 0.0)
        acc[r8, :] = (sums[0] + sums[1]) + (sums[2] + sums[3])

    msg2[...] = jnp.zeros(msg2.shape, F32)
    for i in range(blocks):
        total = jnp.sum(acc[i * LANES:(i + 1) * LANES, :], axis=1, keepdims=True)
        msg2[i:i + 1, :] = to_lanes(jnp.broadcast_to(total, (LANES, LANES)))
    start2()
    wait3()
    at = jnp.sum(g3[...], axis=0)
    column = jnp.concatenate([scale_ref[...]] * (LANES // seqs), axis=0)
    scale = to_lanes(column)
    p = jnp.exp2((at[0:4] - lse * (LOG2E / scale)) * scale)
    out_ref[8:12, :] = jnp.minimum(1.0, p / at[4:8])
    drain1()
    drain3()
    drain2()
    wait2()
    sums = jnp.sum(g2[...], axis=0)
    out_ref[4:8, :] = sums
    for i in range(blocks):
        ncol_ref[i * LANES:(i + 1) * LANES, :] = to_column(1.0 / sums[i:i + 1, :])


def residual_kernel(dims, s_ref, zend_ref, q_ref, lcol_ref, ncol_ref, scale_ref, small_ref, res_ref, *refs):
    draft_rows, seqs, vocab, block, slots, start = dims
    outs, (acc_ref, norm_ref, bonus_ref, stage, sem, small_sem) = refs[:3], refs[3:]
    n = draft_rows // block
    full = vocab // LANES * LANES
    rest = vocab - full

    def copy(i):
        slot = lax.rem(i, slots)
        return pltpu.make_async_copy(stage.at[slot], res_ref.at[pl.ds(pl.multiple_of(i * block, block), block)],
                                     sem.at[slot])

    for j in range(draft_rows // seqs):
        i, off = j // 2, (j % 2) * seqs
        norm_ref[j:j + 1, :] = small_ref[4 + i:5 + i, off:off + seqs]
        acc_ref[j:j + 1, :] = small_ref[8 + i:9 + i, off:off + seqs]
    bonus_ref[...] = small_ref[3:4, 0:seqs]
    small_copies = [pltpu.make_async_copy(src, dst, small_sem.at[i])
                    for i, (src, dst) in enumerate(zip((acc_ref, norm_ref, bonus_ref), outs))]
    for c in small_copies:
        c.start()

    @pl.loop(0, n)
    def _(i):
        slot = lax.rem(i, slots)

        for b in range(block // 8):
            src = pl.ds(pl.multiple_of(i * block + b * 8, 8), 8)
            dst = slice(b * 8, b * 8 + 8)
            lc, inv = lcol_ref[src, :], ncol_ref[src, :]
            scale = scale_ref[pl.ds(pl.multiple_of(lax.rem(i * block + b * 8, seqs), 8), 8), :]
            for c in range(0, full, LANES):
                z = s_ref[src, c:c + LANES] if c < start else zend_ref[src, c - start:c - start + LANES]
                stage[slot, dst, c:c + LANES] = (
                    jnp.maximum(jnp.exp2((z - lc) * scale) - q_ref[src, c:c + LANES], 0.0) * inv)
            stage[slot, dst, full:full + rest] = (
                jnp.maximum(jnp.exp2((zend_ref[src, full - start:full - start + rest] - lc[:, :rest]) * scale[:, :rest])
                            - q_ref[src, full:full + rest], 0.0)
                * inv[:, :rest])
        copy(i).start()

    for c in small_copies:
        c.wait()
    for i in range(n - slots, n):
        copy(i).wait()


def solution(mesh):
    tp = mesh.shape["tp"]
    vmem, hbm = pltpu.VMEM, pltpu.HBM

    def spec(space):
        return pl.BlockSpec(memory_space=space)

    def local_step(hidden, norm_gain, w_head, draft_probs, draft_tokens, temperature):
        seqs, positions, depth = hidden.shape
        drafts, vocab = draft_probs.shape[1:]
        rows, draft_rows = seqs * positions, seqs * drafts
        h = hidden.transpose(1, 0, 2).reshape(rows, depth)
        w = w_head.T
        q = draft_probs.transpose(1, 0, 2).reshape(draft_rows, vocab)
        dt = draft_tokens.T
        chunk, slots, qrows = 512, 4, 32
        start = (pl.cdiv(vocab, chunk) - 1) * chunk
        width = pl.cdiv(vocab - start, LANES) * LANES
        stat = pltpu.VMEM((rows, LANES), F32)
        dims = (rows, draft_rows, seqs, depth, vocab, chunk, slots, qrows)
        s, qv, scale, x, wend, m, sm, bonus = pl.pallas_call(
            functools.partial(head_kernel, dims),
            out_shape=(pltpu.VMEM((draft_rows, start), F32), pltpu.VMEM((draft_rows, vocab), F32),
                       pltpu.VMEM((seqs, LANES), F32), pltpu.VMEM((rows // 16, depth // LANES, 16, LANES), jnp.bfloat16),
                       pltpu.VMEM((width, depth), jnp.bfloat16), stat, stat,
                       pltpu.VMEM((rows - draft_rows, chunk), F32)),
            in_specs=[spec(hbm)] * 5,
            out_specs=(spec(vmem),) * 8,
            scratch_shapes=[
                pltpu.VMEM((rows, depth), jnp.bfloat16), pltpu.VMEM((1, depth), F32), pltpu.VMEM((1, seqs), F32),
                pltpu.VMEM((slots, chunk, depth), jnp.bfloat16),
                pltpu.VMEM((rows, LANES), F32),
                pltpu.SemaphoreType.DMA((positions,)), pltpu.SemaphoreType.DMA((2,)), pltpu.SemaphoreType.DMA((4,)),
                pltpu.SemaphoreType.DMA((slots,)), pltpu.SemaphoreType.DMA((draft_rows // qrows,)),
                pltpu.SemaphoreType.DMA((2,)),
            ],
            compiler_params=pltpu.CompilerParams(vmem_limit_bytes=18 * MIB),
        )(*(pltpu.with_memory_space_constraint(a, hbm)
            for a in (h, norm_gain.reshape(1, depth), w, q, temperature.reshape(1, seqs))))

        lcol, ncol, small, zend = pl.pallas_call(
            functools.partial(verify_kernel, (tp, rows, draft_rows, seqs, vocab, start)),
            out_shape=(pltpu.VMEM((draft_rows, LANES), F32), pltpu.VMEM((draft_rows, LANES), F32),
                       pltpu.VMEM((16, LANES), F32), pltpu.VMEM((rows, width), F32)),
            in_specs=[spec(vmem)] * 9,
            out_specs=(spec(vmem),) * 4,
            scratch_shapes=[
                pltpu.VMEM((draft_rows, LANES), F32), pltpu.VMEM((4, LANES), F32),
                pltpu.VMEM((draft_rows, start + width), F32), pltpu.VMEM((draft_rows, LANES), F32),
                pltpu.VMEM((tp, 4, LANES), F32), pltpu.VMEM((tp, 4, LANES), F32), pltpu.VMEM((tp, 8, LANES), F32),
                pltpu.VMEM((4, LANES), F32), pltpu.VMEM((8, LANES), F32),
                pltpu.VMEM((draft_rows, LANES), F32), pltpu.VMEM((2, draft_rows, LANES), F32),
                pltpu.VMEM((draft_rows, LANES), F32),
            ] + [pltpu.SemaphoreType.DMA((tp,))] * 6,
            compiler_params=pltpu.CompilerParams(vmem_limit_bytes=17 * MIB, collective_id=0, has_side_effects=True),
        )(s, qv, scale, x, wend, m, sm, bonus, dt)

        block = 16
        stages = draft_rows // block
        res, acc, norm, bonus = pl.pallas_call(
            functools.partial(residual_kernel, (draft_rows, seqs, vocab, block, stages, start)),
            out_shape=(jax.ShapeDtypeStruct((draft_rows, vocab), F32), jax.ShapeDtypeStruct((drafts, seqs), F32),
                       jax.ShapeDtypeStruct((drafts, seqs), F32), jax.ShapeDtypeStruct((1, seqs), F32)),
            in_specs=[spec(vmem)] * 7,
            out_specs=(spec(hbm),) * 4,
            scratch_shapes=[
                pltpu.VMEM((drafts, seqs), F32), pltpu.VMEM((drafts, seqs), F32), pltpu.VMEM((1, seqs), F32),
                pltpu.VMEM((stages, block, vocab), F32), pltpu.SemaphoreType.DMA((stages,)),
                pltpu.SemaphoreType.DMA((3,)),
            ],
            compiler_params=pltpu.CompilerParams(vmem_limit_bytes=16 * MIB),
        )(s, zend, qv, lcol, ncol, scale, small)
        res = res.reshape(drafts, seqs, vocab).transpose(1, 0, 2)
        return acc.T, norm.T, res, bonus.reshape(seqs)

    return jax.shard_map(
        local_step,
        mesh=mesh,
        in_specs=(P('dp', None, None), P(), P(None, 'tp'), P('dp', None, 'tp'), P('dp', None), P('dp')),
        out_specs=(P('dp', None), P('dp', None), P('dp', None, 'tp'), P('dp')),
        check_vma=False,
    )
```

```python
import functools

import jax
import jax.numpy as jnp
from jax import lax
from jax.experimental import pallas as pl
from jax.experimental.pallas import tpu as pltpu
from jax.sharding import PartitionSpec as P

F32 = jnp.float32
LANES = 128
NEG = -3.0e38
LOG2E = 1.4426950408889634
MIB = 1024 * 1024


def eye():
    rows = lax.broadcasted_iota(jnp.int32, (LANES, LANES), 0)
    return rows == lax.broadcasted_iota(jnp.int32, (LANES, LANES), 1)


def to_lanes(column):
    return jnp.sum(jnp.where(eye(), column, 0.0), axis=0, keepdims=True)


def to_column(row):
    col = jnp.sum(jnp.where(eye(), jnp.broadcast_to(row, (LANES, LANES)), 0.0), axis=1, keepdims=True)
    return jnp.broadcast_to(col, (LANES, LANES))


def head_kernel(dims, h_ref, g_ref, w_ref, t_ref, s_ref, scale_ref, x, wend, m, sm, bonus,
                hbuf, gbuf, tbuf, wbuf, rinv, hsem, gsem, fsem, wsem, esem):
    rows, draft_rows, seqs, depth, vocab, chunk, slots = dims
    n = pl.cdiv(vocab, chunk)
    tail = vocab - (n - 1) * chunk
    half = chunk // 2
    ktiles = depth // half
    groups = rows // 16
    copy = pltpu.make_async_copy

    def wcopy(i):
        slot = lax.rem(i, slots)
        at = pl.ds(pl.multiple_of(i * chunk, chunk), chunk)
        return copy(w_ref.at[at], wbuf.at[slot], wsem.at[slot])

    def wfirst(p):
        cols = slice(p * depth // 4, (p + 1) * depth // 4)
        return copy(w_ref.at[0:chunk, cols], wbuf.at[0, :, cols], fsem.at[p])

    def wlast():
        fill = wend.shape[0] - tail
        return [copy(w_ref.at[vocab - tail:vocab], wend.at[0:tail], esem.at[0]),
                copy(w_ref.at[0:fill], wend.at[tail:tail + fill], esem.at[1])]

    def wwait(i):
        slot = lax.rem(i, slots)
        copy(w_ref.at[0:chunk], wbuf.at[slot], wsem.at[slot]).wait()

    def hcopy(i):
        at = pl.ds(pl.multiple_of(i * seqs, seqs), seqs)
        return copy(h_ref.at[at], hbuf.at[at], hsem.at[i])

    small = [copy(src, dst, gsem.at[i])
             for i, (src, dst) in enumerate(((g_ref, gbuf), (t_ref, tbuf)))]
    for c in small:
        c.start()
    for i in range(rows // seqs):
        hcopy(i).start()
    wfirst(0).start()
    wfirst(1).start()

    m[...] = jnp.full(m.shape, NEG, F32)
    sm[...] = jnp.zeros(sm.shape, F32)
    for c in small:
        c.wait()
    lane = lax.broadcasted_iota(jnp.int32, (8, LANES), 1)
    t = tbuf[...]
    spread = jnp.where(eye(), jnp.broadcast_to(jnp.concatenate([t, t], axis=1), (LANES, LANES)), 0.0)
    tcol = jnp.sum(spread, axis=1, keepdims=True)
    scale_ref[...] = jnp.broadcast_to(LOG2E / tcol[:seqs], (seqs, LANES))

    for i in range(rows // seqs):
        hcopy(i).wait()
        if i == 0:
            wfirst(2).start()
            wfirst(3).start()
        if i == 3:
            wcopy(1).start()
        for b in range(i * seqs, (i + 1) * seqs, 16):
            h = hbuf[b:b + 16, :].astype(F32)
            r = lax.rsqrt(jnp.mean(h * h, axis=1, keepdims=True) + 1e-5)
            rinv[b:b + 16, :] = jnp.broadcast_to(r, (16, LANES))

    def normalise(k):
        for b in range(0, rows, 16):
            r = rinv[b:b + 16, :]
            for c in range(k * half, (k + 1) * half, LANES):
                h = hbuf[b:b + 16, c:c + LANES].astype(F32)
                x[b // 16, c // LANES] = (h * r * gbuf[:, c:c + LANES]).astype(jnp.bfloat16)

    def push(i, k):
        slot = lax.rem(i, slots)
        cols = slice(k * half, (k + 1) * half)
        for u in range(2):
            pltpu.matmul_push_rhs(wbuf[slot, u * half:(u + 1) * half, cols], k % 2, u, transpose=True)

    def run(*refs):
        accs = [[refs[(2 * u + v) * groups:(2 * u + v + 1) * groups] for v in range(2)] for u in range(2)]

        def stats(i, side, b, size=chunk, valid=chunk):
            base = pl.multiple_of(i * chunk, chunk)
            zs = [pltpu.matmul_pop(accs[u][side][b]) for u in range(2)]
            for o in (0, 8):
                row = b * 16 + o
                r8 = slice(row, row + 8)
                scale = scale_ref[row % seqs:row % seqs + 8, :]
                parts = []
                for c in range(0, size, LANES):
                    z = zs[c // half][o:o + 8, c % half:c % half + LANES]
                    if c + LANES > valid:
                        z = jnp.where(lane < valid - c, z, NEG)
                    parts.append(z)
                    if row < draft_rows:
                        s_ref[r8, pl.ds(base + c, LANES)] = z
                old = m[r8, :]
                new = old
                for z in parts:
                    new = jnp.maximum(new, z)
                tot = sm[r8, :] * jnp.exp2((old - new) * scale)
                for z in parts:
                    tot = tot + jnp.exp2((z - new) * scale)
                m[r8, :] = new
                sm[r8, :] = tot

        def matmul(i, side, last=False, first=False):
            for k in range(ktiles):
                if first:
                    normalise(k)
                    if k == 6:
                        wcopy(3).start()
                if k + 1 < ktiles:
                    if first and (k + 1) % (ktiles // 4) == 0:
                        wfirst((k + 1) // (ktiles // 4)).wait()
                    push(i, k + 1)
                elif not last:
                    wwait(i + 1)
                    push(i + 1, 0)
                for b in range(groups):
                    lhs = jnp.concatenate([x[b, k * half // LANES + c] for c in range(half // LANES)], axis=1)
                    for u in range(2):
                        pltpu.matmul_acc_lhs(accs[u][side][b], lhs, load_staged_rhs=k % 2 if b == 0 else None)
                    done = k * groups + b
                    if not first and done % ktiles == ktiles - 1:
                        stats(i - 1, 1 - side, done // ktiles)

        pairs = (n - 2) // 2
        wfirst(0).wait()
        push(0, 0)
        wcopy(2).start()
        matmul(0, 0, first=True)

        @pl.loop(0, pairs - 1)
        def _(k):
            i = 2 * k + 1
            wcopy(i + 3).start()
            matmul(i, 1)

            @pl.when(k < pairs - 2)
            def _():
                wcopy(i + 4).start()

            @pl.when(k == pairs - 2)
            def _():
                for c in wlast():
                    c.start()

            matmul(i + 1, 0)

        matmul(n - 3, 1)
        matmul(n - 2, 0, True)
        for b in range(groups):
            zs = [pltpu.matmul_pop(accs[u][0][b]) for u in range(2)]
            for u in range(2):
                if b * 16 < draft_rows:
                    s_ref[b * 16:b * 16 + 16, (n - 2) * chunk + u * half:(n - 2) * chunk + (u + 1) * half] = zs[u]
                else:
                    bonus[b * 16 - draft_rows:b * 16 - draft_rows + 16, u * half:(u + 1) * half] = zs[u]
        for c in wlast():
            c.wait()

    pl.run_scoped(run, *(pltpu.ACC(u)((16, half), F32) for u in range(2) for _ in range(2 * groups)))


def verify_kernel(dims, s_ref, qh_ref, scale_ref, x_ref, wend_ref, m_ref, sm_ref, bonus_ref, dt_ref,
                  lcol_ref, ncol_ref, out_ref, zend, q_ref,
                  mrow_ref, lse_ref, e_ref, ccol_ref, g1, g2, g3, msg2, msg3, acc, at_ref, tok, send1, recv1, send2, recv2, send3, recv3, qsem):
    tp, rows, draft_rows, seqs, vocab, start, qrows = dims
    blocks = draft_rows // LANES
    me = lax.axis_index("tp")
    full = vocab // LANES * LANES
    rest = vocab - full

    barrier = pltpu.get_barrier_semaphore()
    for d in range(1, tp):
        pl.semaphore_signal(barrier, inc=1, device_id={"tp": lax.rem(me + d, tp)},
                            device_id_type=pl.DeviceIdType.MESH)
    def qcopy(i):
        at = pl.ds(pl.multiple_of(i * qrows, qrows), qrows)
        return pltpu.make_async_copy(qh_ref.at[at], q_ref.at[at], qsem.at[i])

    @pl.loop(0, draft_rows // qrows)
    def _(i):
        qcopy(i).start()

    width = wend_ref.shape[0]
    pieces = x_ref.shape[1]

    lhs = jnp.concatenate([
        jnp.concatenate([x_ref[b, p] for p in range(pieces)], axis=1) for b in range(rows // 16)], axis=0)
    zend[...] = lax.dot_general(lhs, wend_ref[...], (((1,), (1,)), ((), ())), preferred_element_type=F32)

    lse_ref[...] = jnp.zeros(lse_ref.shape, F32)
    for i in range(pl.cdiv(rows, LANES)):
        size = min(LANES, rows - i * LANES)
        r = slice(i * LANES, i * LANES + size)
        scale = jnp.concatenate([scale_ref[...]] * (size // seqs), axis=0)
        parts = [zend[r, c:c + LANES] for c in range(0, width, LANES)]
        lanes = lax.broadcasted_iota(jnp.int32, (size, LANES), 1)
        parts[-1] = jnp.where(lanes < vocab - start - width + LANES, parts[-1], NEG)
        for c in range(0, bonus_ref.shape[1], LANES):
            if i * LANES < draft_rows:
                at = start - bonus_ref.shape[1] + c
                parts.append(s_ref[r, at:at + LANES])
            else:
                parts.append(bonus_ref[:, c:c + LANES])
        ml = m_ref[r, :]
        top = ml
        for z in parts:
            top = jnp.maximum(top, z)
        mrow = jnp.max(top, axis=1, keepdims=True)
        tot = sm_ref[r, :] * jnp.exp2((ml - mrow) * scale)
        for z in parts:
            tot = tot + jnp.exp2((z - mrow) * scale)
        srow = jnp.sum(tot, axis=1, keepdims=True)
        lse = mrow * (scale * (1.0 / LOG2E)) + jnp.log(srow)
        if i * LANES < draft_rows:
            mrow_ref[r, :] = jnp.broadcast_to(mrow, (size, LANES))
        mask = eye()[:size]
        lse_ref[i:i + 1, :] = jnp.sum(jnp.where(mask, lse, 0.0), axis=0, keepdims=True)

    pl.semaphore_wait(barrier, tp - 1)

    def exchange(src, gather, send, recv):
        def copy(slot, sem, d):
            return pltpu.make_async_remote_copy(
                src_ref=src, dst_ref=gather.at[slot], send_sem=send.at[d], recv_sem=recv.at[sem],
                device_id={"tp": lax.rem(me + d, tp)}, device_id_type=pl.DeviceIdType.MESH)

        def start():
            for d in range(1, tp):
                copy(me, me, d).start()
            gather[me] = src[...]

        def wait():
            for d in range(1, tp):
                peer = lax.rem(me + d, tp)
                copy(peer, peer, d).wait_recv()

        def drain():
            for d in range(1, tp):
                copy(me, me, d).wait_send()

        return start, wait, drain

    start1, wait1, drain1 = exchange(lse_ref, g1, send1, recv1)
    start2, wait2, drain2 = exchange(msg2, g2, send2, recv2)
    start3, wait3, drain3 = exchange(msg3, g3, send3, recv3)
    start1()

    offset = me * vocab
    for i in range(blocks):
        ids = jnp.concatenate([dt_ref[2 * i:2 * i + 1, :], dt_ref[2 * i + 1:2 * i + 2, :]], axis=1)
        tok[i * LANES:(i + 1) * LANES, :] = to_column((ids - offset).astype(F32))
    lane = lax.broadcasted_iota(jnp.int32, (8, LANES), 1).astype(F32)
    acc[...] = jnp.zeros(acc.shape, F32)
    at_ref[...] = jnp.zeros(at_ref.shape, F32)

    @pl.loop(0, draft_rows // 8)
    def _(b):
        @pl.when(lax.rem(b, qrows // 8) == 0)
        def _():
            qcopy(b // (qrows // 8)).wait()

        r8 = pl.ds(pl.multiple_of(b * 8, 8), 8)
        mr = mrow_ref[r8, :]
        scale = scale_ref[pl.ds(pl.multiple_of(lax.rem(b * 8, seqs), 8), 8), :]
        away = tok[r8, :] - lane
        zr = zend[r8, full - start:full - start + rest]
        e_ref[r8, full:full + rest] = jnp.exp2((zr - mr[:, :rest]) * scale[:, :rest])
        hit = away[:, :rest] == float(full)
        at_ref[0, r8, 0:rest] = jnp.where(hit, zr, 0.0)
        at_ref[1, r8, 0:rest] = jnp.where(hit, q_ref[r8, full:full + rest], 0.0)
        az, aq = at_ref[0, r8, :], at_ref[1, r8, :]
        for c in range(0, full, LANES):
            z = s_ref[r8, c:c + LANES] if c < start else zend[r8, c - start:c - start + LANES]
            e_ref[r8, c:c + LANES] = jnp.exp2((z - mr) * scale)
            hit = away == float(c)
            az = jnp.where(hit, z, az)
            aq = jnp.where(hit, q_ref[r8, c:c + LANES], aq)
        at_ref[0, r8, :] = az
        at_ref[1, r8, :] = aq

    msg3[...] = jnp.zeros(msg3.shape, F32)
    for i in range(blocks):
        r = slice(i * LANES, (i + 1) * LANES)
        for part in range(2):
            value = jnp.sum(at_ref[part, r, :], axis=1, keepdims=True)
            msg3[4 * part + i:4 * part + i + 1, :] = to_lanes(jnp.broadcast_to(value, (LANES, LANES)))
    start3()
    wait1()
    parts = g1[...]
    top = jnp.max(parts, axis=0)
    lse = top + jnp.log(jnp.sum(jnp.exp(parts - top[None]), axis=0))
    out_ref[...] = jnp.zeros(out_ref.shape, F32)
    out_ref[0:4, :] = lse
    for i in range(blocks):
        r = slice(i * LANES, (i + 1) * LANES)
        scale = jnp.concatenate([scale_ref[...]] * (LANES // seqs), axis=0)
        lcol = to_column(lse[i:i + 1, :]) * (LOG2E / scale)
        lcol_ref[r, :] = lcol
        ccol_ref[r, :] = jnp.exp2((mrow_ref[r, :] - lcol) * scale)

    @pl.loop(0, draft_rows // 8)
    def _(b):
        r8 = pl.ds(pl.multiple_of(b * 8, 8), 8)
        cc = ccol_ref[r8, :]
        er = e_ref[r8, full:full + rest]
        acc[r8, 0:rest] = jnp.maximum(er * cc[:, :rest] - q_ref[r8, full:full + rest], 0.0)
        sums = [acc[r8, :]] + [jnp.zeros((8, LANES), F32)] * 3
        for k, c in enumerate(range(0, full, LANES)):
            sums[k % 4] += jnp.maximum(e_ref[r8, c:c + LANES] * cc - q_ref[r8, c:c + LANES], 0.0)
        acc[r8, :] = (sums[0] + sums[1]) + (sums[2] + sums[3])

    msg2[...] = jnp.zeros(msg2.shape, F32)
    for i in range(blocks):
        total = jnp.sum(acc[i * LANES:(i + 1) * LANES, :], axis=1, keepdims=True)
        msg2[i:i + 1, :] = to_lanes(jnp.broadcast_to(total, (LANES, LANES)))
    start2()
    wait3()
    at = jnp.sum(g3[...], axis=0)
    column = jnp.concatenate([scale_ref[...]] * (LANES // seqs), axis=0)
    scale = to_lanes(column)
    p = jnp.exp2((at[0:4] - lse * (LOG2E / scale)) * scale)
    out_ref[8:12, :] = jnp.minimum(1.0, p / at[4:8])
    drain1()
    drain3()
    drain2()
    wait2()
    sums = jnp.sum(g2[...], axis=0)
    out_ref[4:8, :] = sums
    for i in range(blocks):
        ncol_ref[i * LANES:(i + 1) * LANES, :] = to_column(1.0 / sums[i:i + 1, :])


def residual_kernel(dims, s_ref, zend_ref, q_ref, lcol_ref, ncol_ref, scale_ref, small_ref, res_ref, *refs):
    draft_rows, seqs, vocab, block, slots, start = dims
    outs, (acc_ref, norm_ref, bonus_ref, stage, sem, small_sem) = refs[:3], refs[3:]
    n = draft_rows // block
    full = vocab // LANES * LANES
    rest = vocab - full

    def copy(i):
        slot = lax.rem(i, slots)
        return pltpu.make_async_copy(stage.at[slot], res_ref.at[pl.ds(pl.multiple_of(i * block, block), block)],
                                     sem.at[slot])

    for j in range(draft_rows // seqs):
        i, off = j // 2, (j % 2) * seqs
        norm_ref[j:j + 1, :] = small_ref[4 + i:5 + i, off:off + seqs]
        acc_ref[j:j + 1, :] = small_ref[8 + i:9 + i, off:off + seqs]
    bonus_ref[...] = small_ref[3:4, 0:seqs]
    small_copies = [pltpu.make_async_copy(src, dst, small_sem.at[i])
                    for i, (src, dst) in enumerate(zip((acc_ref, norm_ref, bonus_ref), outs))]
    for c in small_copies:
        c.start()

    @pl.loop(0, n)
    def _(i):
        slot = lax.rem(i, slots)

        for b in range(block // 8):
            src = pl.ds(pl.multiple_of(i * block + b * 8, 8), 8)
            dst = slice(b * 8, b * 8 + 8)
            lc, inv = lcol_ref[src, :], ncol_ref[src, :]
            scale = scale_ref[pl.ds(pl.multiple_of(lax.rem(i * block + b * 8, seqs), 8), 8), :]
            for c in range(0, full, LANES):
                z = s_ref[src, c:c + LANES] if c < start else zend_ref[src, c - start:c - start + LANES]
                stage[slot, dst, c:c + LANES] = (
                    jnp.maximum(jnp.exp2((z - lc) * scale) - q_ref[src, c:c + LANES], 0.0) * inv)
            stage[slot, dst, full:full + rest] = (
                jnp.maximum(jnp.exp2((zend_ref[src, full - start:full - start + rest] - lc[:, :rest]) * scale[:, :rest])
                            - q_ref[src, full:full + rest], 0.0)
                * inv[:, :rest])
        copy(i).start()

    for c in small_copies:
        c.wait()
    for i in range(n - slots, n):
        copy(i).wait()


def solution(mesh):
    tp = mesh.shape["tp"]
    vmem, hbm = pltpu.VMEM, pltpu.HBM

    def spec(space):
        return pl.BlockSpec(memory_space=space)

    def local_step(hidden, norm_gain, w_head, draft_probs, draft_tokens, temperature):
        seqs, positions, depth = hidden.shape
        drafts, vocab = draft_probs.shape[1:]
        rows, draft_rows = seqs * positions, seqs * drafts
        h = hidden.transpose(1, 0, 2).reshape(rows, depth)
        w = w_head.T
        q = draft_probs.transpose(1, 0, 2).reshape(draft_rows, vocab)
        dt = draft_tokens.T
        chunk, slots, qrows = 512, 4, 32
        start = (pl.cdiv(vocab, chunk) - 1) * chunk
        width = pl.cdiv(vocab - start, LANES) * LANES
        stat = pltpu.VMEM((rows, LANES), F32)
        dims = (rows, draft_rows, seqs, depth, vocab, chunk, slots)
        s, scale, x, wend, m, sm, bonus = pl.pallas_call(
            functools.partial(head_kernel, dims),
            out_shape=(pltpu.VMEM((draft_rows, start), F32),
                       pltpu.VMEM((seqs, LANES), F32), pltpu.VMEM((rows // 16, depth // LANES, 16, LANES), jnp.bfloat16),
                       pltpu.VMEM((width, depth), jnp.bfloat16), stat, stat,
                       pltpu.VMEM((rows - draft_rows, chunk), F32)),
            in_specs=[spec(hbm)] * 4,
            out_specs=(spec(vmem),) * 7,
            scratch_shapes=[
                pltpu.VMEM((rows, depth), jnp.bfloat16), pltpu.VMEM((1, depth), F32), pltpu.VMEM((1, seqs), F32),
                pltpu.VMEM((slots, chunk, depth), jnp.bfloat16),
                pltpu.VMEM((rows, LANES), F32),
                pltpu.SemaphoreType.DMA((positions,)), pltpu.SemaphoreType.DMA((2,)), pltpu.SemaphoreType.DMA((4,)),
                pltpu.SemaphoreType.DMA((slots,)), pltpu.SemaphoreType.DMA((2,)),
            ],
            compiler_params=pltpu.CompilerParams(vmem_limit_bytes=18 * MIB),
        )(*(pltpu.with_memory_space_constraint(a, hbm)
            for a in (h, norm_gain.reshape(1, depth), w, temperature.reshape(1, seqs))))

        lcol, ncol, small, zend, qv = pl.pallas_call(
            functools.partial(verify_kernel, (tp, rows, draft_rows, seqs, vocab, start, qrows)),
            out_shape=(pltpu.VMEM((draft_rows, LANES), F32), pltpu.VMEM((draft_rows, LANES), F32),
                       pltpu.VMEM((16, LANES), F32), pltpu.VMEM((rows, width), F32),
                       pltpu.VMEM((draft_rows, vocab), F32)),
            in_specs=[spec(vmem), spec(hbm)] + [spec(vmem)] * 7,
            out_specs=(spec(vmem),) * 5,
            scratch_shapes=[
                pltpu.VMEM((draft_rows, LANES), F32), pltpu.VMEM((4, LANES), F32),
                pltpu.VMEM((draft_rows, start + width), F32), pltpu.VMEM((draft_rows, LANES), F32),
                pltpu.VMEM((tp, 4, LANES), F32), pltpu.VMEM((tp, 4, LANES), F32), pltpu.VMEM((tp, 8, LANES), F32),
                pltpu.VMEM((4, LANES), F32), pltpu.VMEM((8, LANES), F32),
                pltpu.VMEM((draft_rows, LANES), F32), pltpu.VMEM((2, draft_rows, LANES), F32),
                pltpu.VMEM((draft_rows, LANES), F32),
            ] + [pltpu.SemaphoreType.DMA((tp,))] * 6 + [pltpu.SemaphoreType.DMA((draft_rows // qrows,))],
            compiler_params=pltpu.CompilerParams(vmem_limit_bytes=17 * MIB, collective_id=0, has_side_effects=True),
        )(s, pltpu.with_memory_space_constraint(q, hbm), scale, x, wend, m, sm, bonus, dt)

        block = 16
        stages = draft_rows // block
        res, acc, norm, bonus = pl.pallas_call(
            functools.partial(residual_kernel, (draft_rows, seqs, vocab, block, stages, start)),
            out_shape=(jax.ShapeDtypeStruct((draft_rows, vocab), F32), jax.ShapeDtypeStruct((drafts, seqs), F32),
                       jax.ShapeDtypeStruct((drafts, seqs), F32), jax.ShapeDtypeStruct((1, seqs), F32)),
            in_specs=[spec(vmem)] * 7,
            out_specs=(spec(hbm),) * 4,
            scratch_shapes=[
                pltpu.VMEM((drafts, seqs), F32), pltpu.VMEM((drafts, seqs), F32), pltpu.VMEM((1, seqs), F32),
                pltpu.VMEM((stages, block, vocab), F32), pltpu.SemaphoreType.DMA((stages,)),
                pltpu.SemaphoreType.DMA((3,)),
            ],
            compiler_params=pltpu.CompilerParams(vmem_limit_bytes=16 * MIB),
        )(s, zend, qv, lcol, ncol, scale, small)
        res = res.reshape(drafts, seqs, vocab).transpose(1, 0, 2)
        return acc.T, norm.T, res, bonus.reshape(seqs)

    return jax.shard_map(
        local_step,
        mesh=mesh,
        in_specs=(P('dp', None, None), P(), P(None, 'tp'), P('dp', None, 'tp'), P('dp', None), P('dp')),
        out_specs=(P('dp', None), P('dp', None), P('dp', None, 'tp'), P('dp')),
        check_vma=False,
    )
```
